16 devices in a mesh: dp: 2 (over y, z), sp: 8 (over x, core).
Axes of the slice: x: 4, y: 2, z: 1, core: 2. Of those that a mesh axis runs over, the one named last changes fastest.
The devices are a block of a 4x4x8 slice.
Arguments:
- tokens: bfloat16 [32768, 512], P(('dp', 'sp')), parts along dimension 0
- grad_out: bfloat16 [32768, 512], P(('dp', 'sp')), parts along dimension 0
- ln_gain: float32 [512], replicated
- ln_bias: float32 [512], replicated
- w_qkv: bfloat16 [512, 1536], replicated
- w_out: bfloat16 [512, 512], replicated
- temperature: float32 [8], replicated
Outputs:
- output 1: bfloat16 [32768, 512], P(('dp', 'sp')), parts along dimension 0
- output 2: bfloat16 [32768, 512], P(('dp', 'sp')), parts along dimension 0
- output 3: float32 [1024, 1536], P(('dp', 'sp')), parts along dimension 0
- output 4: float32 [1024, 512], P(('dp', 'sp')), parts along dimension 0
- output 5: float32 [1024], P('dp'), parts along dimension 0
- output 6: float32 [1024], P('dp'), parts along dimension 0
- output 7: float32 [16], P('dp'), parts along dimension 0
There are 2 independent parts. The reference program is written for one: setup_inputs(seed, part) draws one part's arguments, and reference() takes and returns one part's arrays. A program takes and returns all parts, laid end to end along the dimension named above; an argument that names none is the same for every part.
All inputs are finite; a program needn't handle non-finite values.
Results may differ from the reference program's by a relative error of at most 0.00113883.
Values are sent between devices in bfloat16 or wider.
A program may use at most 768 MiB of HBM per device.

```python
import jax
import jax.numpy as jnp
from jax import lax

SEQ_LEN = 16384
MODEL_DIM = 512
NUM_HEADS = 8

HEAD_DIM = MODEL_DIM // NUM_HEADS


def setup_inputs(seed: int = 0, part: int = 0) -> dict:
    part_keys = jax.random.split(jax.random.fold_in(jax.random.key(seed), part), 4)
    shared_keys = jax.random.split(jax.random.key(seed + 1), 5)
    position = (jnp.arange(SEQ_LEN, dtype=jnp.float32) + 0.5) / SEQ_LEN
    wave_basis = jnp.cos(jnp.pi * position[:, None] * jnp.arange(1, 5, dtype=jnp.float32)[None, :])
    x_pattern = jnp.dot(wave_basis, jax.random.normal(part_keys[0], (4, MODEL_DIM), jnp.float32))
    tokens = jax.random.normal(part_keys[1], (SEQ_LEN, MODEL_DIM), jnp.float32) + x_pattern
    dy_pattern = jnp.dot(wave_basis, jax.random.normal(part_keys[2], (4, MODEL_DIM), jnp.float32))
    grad_out = jax.random.normal(part_keys[3], (SEQ_LEN, MODEL_DIM), jnp.float32) + 0.5 * dy_pattern
    w_scale = MODEL_DIM ** -0.5
    return {
        'tokens': tokens.astype(jnp.bfloat16),
        'grad_out': grad_out.astype(jnp.bfloat16),
        'ln_gain': 1.0 + 0.3 * jax.random.normal(shared_keys[0], (MODEL_DIM,), jnp.float32),
        'ln_bias': 0.3 * jax.random.normal(shared_keys[1], (MODEL_DIM,), jnp.float32),
        'w_qkv': (w_scale * jax.random.normal(shared_keys[2], (MODEL_DIM, 3 * MODEL_DIM), jnp.float32)).astype(jnp.bfloat16),
        'w_out': (w_scale * jax.random.normal(shared_keys[3], (MODEL_DIM, MODEL_DIM), jnp.float32)).astype(jnp.bfloat16),
        'temperature': jax.random.uniform(shared_keys[4], (NUM_HEADS,), jnp.float32, 2.5, 6.5),
    }


def layer_norm(x_f32, ln_gain, ln_bias):
    row_mean = jnp.mean(x_f32, axis=-1, keepdims=True)
    centered = x_f32 - row_mean
    row_var = jnp.mean(centered * centered, axis=-1, keepdims=True)
    return centered * lax.rsqrt(row_var + 1e-6) * ln_gain + ln_bias


def attn_probs(gram_sum, q_sq, k_sq, temperature):
    cosine = gram_sum / (jnp.sqrt(q_sq)[..., :, None] * jnp.sqrt(k_sq)[..., None, :])
    return jax.nn.softmax(temperature[..., None, None] * cosine, axis=-1)


def reference(tokens, grad_out, ln_gain, ln_bias, w_qkv, w_out, temperature):
    x_f32 = tokens.astype(jnp.float32)
    ln_value, ln_vjp = jax.vjp(layer_norm, x_f32, ln_gain, ln_bias)
    normed = ln_value.astype(jnp.bfloat16)
    qkv_act = jnp.dot(normed, w_qkv, preferred_element_type=jnp.float32).astype(jnp.bfloat16)
    qkv_heads = qkv_act.astype(jnp.float32).reshape(SEQ_LEN, 3, NUM_HEADS, HEAD_DIM)
    q_heads = qkv_heads[:, 0]
    k_heads = qkv_heads[:, 1]
    v_heads = qkv_heads[:, 2]
    gram_sum = jnp.einsum('nhi,nhj->hij', q_heads, k_heads)
    q_sq = jnp.sum(q_heads * q_heads, axis=0)
    k_sq = jnp.sum(k_heads * k_heads, axis=0)
    attn_f32, probs_vjp = jax.vjp(attn_probs, gram_sum, q_sq, k_sq, temperature)
    attn_weights = attn_f32.astype(jnp.bfloat16).astype(jnp.float32)
    attn_out = jnp.einsum('nhj,hij->nhi', v_heads, attn_weights).astype(jnp.bfloat16).reshape(SEQ_LEN, MODEL_DIM)
    out_tokens = (x_f32 + jnp.dot(attn_out, w_out, preferred_element_type=jnp.float32)).astype(jnp.bfloat16)

    grad_w_out = jnp.dot(attn_out.T, grad_out, preferred_element_type=jnp.float32)
    d_attn = jnp.dot(grad_out, w_out.T, preferred_element_type=jnp.float32).astype(jnp.bfloat16)
    d_heads = d_attn.astype(jnp.float32).reshape(SEQ_LEN, NUM_HEADS, HEAD_DIM)
    d_probs = jnp.einsum('nhi,nhj->hij', d_heads, v_heads)
    d_gram, d_qsq, d_ksq, grad_temperature = probs_vjp(d_probs)
    d_gram_bf = d_gram.astype(jnp.bfloat16).astype(jnp.float32)
    d_q = jnp.einsum('hij,nhj->nhi', d_gram_bf, k_heads) + 2.0 * q_heads * d_qsq
    d_k = jnp.einsum('hij,nhi->nhj', d_gram_bf, q_heads) + 2.0 * k_heads * d_ksq
    d_v = jnp.einsum('hij,nhi->nhj', attn_weights, d_heads)
    d_qkv = jnp.stack([d_q, d_k, d_v], axis=1).astype(jnp.bfloat16).reshape(SEQ_LEN, 3 * MODEL_DIM)
    grad_w_qkv = jnp.dot(normed.T, d_qkv, preferred_element_type=jnp.float32)
    d_normed = jnp.dot(d_qkv, w_qkv.T, preferred_element_type=jnp.float32)
    d_x, grad_gain, grad_bias = ln_vjp(d_normed)
    grad_tokens = (grad_out.astype(jnp.float32) + d_x).astype(jnp.bfloat16)
    return (out_tokens, grad_tokens, grad_w_qkv, grad_w_out, grad_gain, grad_bias, grad_temperature)
```

```python
import functools

import jax
import jax.numpy as jnp
from jax import lax
from jax.experimental import pallas as pl
from jax.experimental.pallas import tpu as pltpu
from jax.sharding import PartitionSpec as P

F32 = jnp.float32
BF16 = jnp.bfloat16
NN = (((1,), (0,)), ((), ()))
NT = (((1,), (1,)), ((), ()))
TN = (((0,), (0,)), ((), ()))
EPS = 1e-6


def mm(a, b, dims=NN):
    return lax.dot_general(a, b, dims, preferred_element_type=F32)


def kernel(ns, rows, width, heads, tile,
           x_hbm, dy_hbm, gain_hbm, bias_hbm, wqkv_hbm, wout_hbm, temp_ref,
           out_hbm, gtok_hbm, gwqkv_hbm, gwout_hbm, ggain_ref, gbias_ref, gtemp_ref,
           x_v, dy_v, gain_v, bias_v, wqkv_v, wout_v,
           u_v, q_v, k_v, v_v, do_v, o_v, dqkv_v, xhat_v, rstd_v,
           gacc, dacc, sqacc, skacc, gsend, grecv, dsend, drecv, a_all, e_all, st_all, bd_a, bd_g,
           gw, pre, opp, nrr, rlr, gwst, gbacc, gb_all,
           in_sem, out_sem, small_s, small_r, pre_s, pre_r, x2_s, x2_r):
    me = lax.axis_index('sp')
    nt = rows // tile
    hd = width // heads
    core = lax.rem(me, 2)
    chip = me // 2
    nchip = ns // 2
    partner = me + 1 - 2 * core
    right = lax.rem(me + 2, ns)
    left = lax.rem(me + ns - 2, ns)
    c_r = lax.rem(chip + 1, nchip)
    c_l = lax.rem(chip + nchip - 1, nchip)
    c_o = lax.rem(chip + 2, nchip)

    def remote(src, dst, ssem, rsem, dev):
        return pltpu.make_async_remote_copy(src_ref=src, dst_ref=dst, send_sem=ssem, recv_sem=rsem,
                                            device_id={'sp': dev}, device_id_type=pl.DeviceIdType.MESH)

    barrier = pltpu.get_barrier_semaphore()
    for r in range(1, ns):
        pl.semaphore_signal(barrier, inc=1, device_id={'sp': lax.rem(me + r, ns)},
                            device_id_type=pl.DeviceIdType.MESH)

    def ld(i, src, dst):
        return pltpu.make_async_copy(src, dst, in_sem.at[i])

    def tile_of(i):
        return pl.ds(pl.multiple_of(i * tile, tile), tile)

    def x_copy(i):
        return ld(i, x_hbm.at[tile_of(i)], x_v.at[tile_of(i)])

    def dy_copy(i):
        return ld(nt + i, dy_hbm.at[tile_of(i)], dy_v.at[tile_of(i)])

    gain_copy = ld(2 * nt, gain_hbm, gain_v)
    bias_copy = ld(2 * nt + 1, bias_hbm, bias_v)
    wqk_copy = ld(2 * nt + 2, wqkv_hbm.at[:, 0:2 * width], wqkv_v.at[:, 0:2 * width])
    wv_copy = ld(2 * nt + 3, wqkv_hbm.at[:, 2 * width:3 * width], wqkv_v.at[:, 2 * width:3 * width])
    wout_copy = ld(2 * nt + 4, wout_hbm, wout_v)
    gain_copy.start()
    bias_copy.start()
    x_copy(0).start()
    wqk_copy.start()
    for i in range(1, nt):
        x_copy(i).start()
    wv_copy.start()
    wout_copy.start()
    for i in range(nt):
        dy_copy(i).start()

    gacc[...] = jnp.zeros_like(gacc)
    dacc[...] = jnp.zeros_like(dacc)
    sqacc[...] = jnp.zeros_like(sqacc)
    skacc[...] = jnp.zeros_like(skacc)
    gbacc[...] = jnp.zeros_like(gbacc)
    bd_a[...] = jnp.zeros_like(bd_a)
    bd_g[...] = jnp.zeros_like(bd_g)
    gain_copy.wait()
    bias_copy.wait()
    wqk_copy.wait()

    ngrp = width // 256
    hpg = heads // ngrp

    def c1(i, carry):
        x_copy(i).wait()
        t = tile_of(i)
        x = x_v[t, :].astype(F32)
        mean = jnp.mean(x, axis=1, keepdims=True)
        cent = x - mean
        var = jnp.mean(cent * cent, axis=1, keepdims=True)
        rstd = lax.rsqrt(var + EPS)
        xhat = cent * rstd
        xhat_v[t, :] = xhat
        rstd_v[t, :] = rstd
        u = (xhat * gain_v[...] + bias_v[...]).astype(BF16)
        u_v[t, :] = u
        q = mm(u, wqkv_v[:, 0:width]).astype(BF16)
        q_v[t, :] = q
        k = mm(u, wqkv_v[:, width:2 * width]).astype(BF16)
        k_v[t, :] = k
        for g in range(ngrp):
            c = slice(256 * g, 256 * g + 256)
            gacc[g] += mm(q[:, c], k[:, c], TN)
        q32 = q.astype(F32)
        k32 = k.astype(F32)
        sqacc[...] += jnp.sum((q32 * q32).reshape(tile // 8, 8, width), axis=0)
        skacc[...] += jnp.sum((k32 * k32).reshape(tile // 8, 8, width), axis=0)
        return carry

    lax.fori_loop(0, nt, c1, 0)

    lane32 = lax.broadcasted_iota(jnp.int32, (hd // 2, 2 * hd), 1)

    def pack(acc, h):
        g, hh = h // hpg, h % hpg
        blk = acc[g, hh * hd:hh * hd + hd, (hh // 2) * 128:(hh // 2) * 128 + 128]
        top, bot = blk[0:hd // 2], blk[hd // 2:hd]
        if h % 2 == 0:
            bot = pltpu.roll(bot, hd, axis=1)
        else:
            top = pltpu.roll(top, hd, axis=1)
        return jnp.where(lane32 < hd, top, bot)

    sq_row = jnp.sum(sqacc[...], axis=0, keepdims=True)
    sk_row = jnp.sum(skacc[...], axis=0, keepdims=True)
    for h in range(heads):
        gsend[h, 0:hd // 2, :] = pack(gacc, h)
        c = slice((h // 2) * 128, (h // 2) * 128 + 128)
        gsend[h, hd // 2:hd // 2 + 1, :] = sq_row[:, c]
        gsend[h, hd // 2 + 1:hd // 2 + 2, :] = sk_row[:, c]

    def to_owner(kind, src, dst, r):
        dst_dev = lax.rem(me + r, ns)
        return remote(src.at[dst_dev], dst.at[r], small_s.at[kind, r], small_r.at[kind, r], dst_dev)

    def to_all(kind, buf, r):
        return remote(buf.at[me], buf.at[me], small_s.at[kind, r], small_r.at[kind, r], lax.rem(me + r, ns))

    pl.semaphore_wait(barrier, ns - 1)
    for r in range(1, ns):
        to_owner(0, gsend, grecv, r).start()

    wv_copy.wait()
    wout_copy.wait()

    def c2(i, carry):
        dy_copy(i).wait()
        t = tile_of(i)
        v = mm(u_v[t, :], wqkv_v[:, 2 * width:3 * width]).astype(BF16)
        v_v[t, :] = v
        do = mm(dy_v[t, :], wout_v[...], NT).astype(BF16)
        do_v[t, :] = do
        for g in range(ngrp):
            c = slice(256 * g, 256 * g + 256)
            dacc[g] += mm(do[:, c], v[:, c], TN)
        return carry

    lax.fori_loop(0, nt, c2, 0)
    for h in range(heads):
        dsend[h] = pack(dacc, h)
    for r in range(1, ns):
        to_owner(1, dsend, drecv, r).start()

    row = lax.broadcasted_iota(jnp.int32, (hd, 2 * hd), 0)
    lanep = lax.broadcasted_iota(jnp.int32, (hd, 2 * hd), 1) - hd * core
    half = (lanep >= 0) & (lanep < hd)
    diag = lanep == row
    half1 = half[0:1]

    def unpack(p):
        rolled = pltpu.roll(p, hd, axis=1)
        even = core == 0
        full = jnp.concatenate([jnp.where(even, p, rolled), jnp.where(even, rolled, p)], axis=0)
        return jnp.where(half, full, 0.0)

    for r in range(1, ns):
        to_owner(0, gsend, grecv, r).wait_recv()
    tot = gsend[me, 0:hd // 2 + 2]
    for r in range(1, ns):
        tot = tot + grecv[r, 0:hd // 2 + 2]
    gram = unpack(tot[0:hd // 2])
    sq_r = tot[hd // 2:hd // 2 + 1]
    sk_r = jnp.where(half1, tot[hd // 2 + 1:hd // 2 + 2], 1.0)
    sq_c = jnp.sum(jnp.where(diag, sq_r, 0.0), axis=1, keepdims=True)
    den = jnp.sqrt(sq_c) * jnp.sqrt(sk_r)
    cosine = gram / den
    temp = temp_ref[me]
    logits = jnp.where(half, temp * cosine, -jnp.inf)
    ex = jnp.exp(logits - jnp.max(logits, axis=1, keepdims=True))
    attn = ex / jnp.sum(ex, axis=1, keepdims=True)
    a_all[me] = attn.astype(BF16)
    for r in range(1, ns):
        to_all(2, a_all, r).start()

    for r in range(1, ns):
        to_owner(1, dsend, drecv, r).wait_recv()
    dtot = dsend[me]
    for r in range(1, ns):
        dtot = dtot + drecv[r]
    d_a = unpack(dtot)
    inner = jnp.sum(d_a * attn, axis=1, keepdims=True)
    d_s = attn * (d_a - inner)
    d_cos = temp * d_s
    d_t = jnp.sum(jnp.sum(d_s * cosine, axis=1, keepdims=True), axis=0, keepdims=True)
    e_all[me] = (d_cos / den).astype(BF16)
    ec = d_cos * cosine
    dsq_c = -0.5 * jnp.sum(ec, axis=1, keepdims=True) / sq_c
    dsk_r = -0.5 * jnp.sum(ec, axis=0, keepdims=True) / sk_r
    dsq_r = jnp.sum(jnp.where(diag, dsq_c, 0.0), axis=0, keepdims=True)
    st_all[me, 0:1, :] = dsq_r
    st_all[me, 1:2, :] = dsk_r
    st_all[me, 2:3, :] = jnp.broadcast_to(d_t, (1, 2 * hd))
    for r in range(1, ns):
        to_all(3, e_all, r).start()
    for r in range(1, ns):
        to_all(4, st_all, r).start()

    def fill(bd, blocks):
        for g in range(ngrp):
            for j in range(2):
                s = slice(128 * j, 128 * j + 128)
                h = g * hpg + 2 * j
                bd[g, s, s] = blocks[h:h + 2].reshape(128, 128)

    def pre_copy(pc):
        return remote(gw.at[pc, :, 1 - core], pre.at[pc], pre_s.at[pc], pre_r.at[pc], partner)

    hr = gw.shape[3] // 2
    lo, hi = slice(0, hr), slice(hr, 2 * hr)

    def first_copies(pc):
        return [remote(pre.at[pc, c_o, lo], opp.at[pc, 0], x2_s.at[pc, 0], x2_r.at[pc, 0], right),
                remote(pre.at[pc, c_o, hi], opp.at[pc, 1], x2_s.at[pc, 1], x2_r.at[pc, 1], left),
                remote(pre.at[pc, c_r, hi], nrr.at[pc, 0], x2_s.at[pc, 2], x2_r.at[pc, 2], right),
                remote(pre.at[pc, c_l, lo], nrr.at[pc, 1], x2_s.at[pc, 3], x2_r.at[pc, 3], left)]

    def relay_copies(pc):
        return [remote(pre.at[pc, c_r, lo], rlr.at[pc, 0], x2_s.at[pc, 4], x2_r.at[pc, 4], right),
                remote(pre.at[pc, c_l, hi], rlr.at[pc, 1], x2_s.at[pc, 5], x2_r.at[pc, 5], left)]

    def rs_pre(pc):
        pre_copy(pc).start()

    def rs_first(pc):
        pre_copy(pc).wait_recv()
        pre[pc] = pre[pc] + gw[pc, :, core]
        for cp in first_copies(pc):
            cp.start()

    def rs_relay(pc):
        first, second = first_copies(pc), relay_copies(pc)
        first[0].wait_recv()
        pre[pc, c_r, lo] = pre[pc, c_r, lo] + opp[pc, 0]
        second[0].start()
        first[1].wait_recv()
        pre[pc, c_l, hi] = pre[pc, c_l, hi] + opp[pc, 1]
        second[1].start()

    def rs_final(pc):
        first, second = first_copies(pc), relay_copies(pc)
        first[2].wait_recv()
        first[3].wait_recv()
        second[0].wait_recv()
        second[1].wait_recv()
        gwst[pc, lo] = pre[pc, chip, lo] + rlr[pc, 0] + nrr[pc, 1]
        gwst[pc, hi] = pre[pc, chip, hi] + nrr[pc, 0] + rlr[pc, 1]

    for r in range(1, ns):
        to_all(2, a_all, r).wait_recv()
    fill(bd_a, a_all)

    def c3(i, carry):
        t = tile_of(i)
        for g in range(ngrp):
            c = slice(256 * g, 256 * g + 256)
            o_v[t, c] = mm(v_v[t, c], bd_a[g], NT).astype(BF16)
        return carry

    lax.fori_loop(0, nt, c3, 0)
    gw[0] = mm(o_v[...], dy_v[...], TN).reshape(gw.shape[1:])
    rs_pre(0)

    def c4(i, carry):
        t = tile_of(i)
        for g in range(ngrp):
            c = slice(256 * g, 256 * g + 256)
            dqkv_v[t, 2 * width + 256 * g:2 * width + 256 * g + 256] = mm(do_v[t, c], bd_a[g]).astype(BF16)
        return carry

    lax.fori_loop(0, nt, c4, 0)
    gw[1] = mm(u_v[...], dqkv_v[:, 2 * width:3 * width], TN).reshape(gw.shape[1:])
    rs_pre(1)
    rs_first(0)

    for r in range(1, ns):
        to_all(3, e_all, r).wait_recv()
    for r in range(1, ns):
        to_all(4, st_all, r).wait_recv()
    fill(bd_g, e_all)
    pair = [st_all[2 * j, 0:2, :] + st_all[2 * j + 1, 0:2, :] for j in range(heads // 2)]
    dsq2 = jnp.concatenate([2.0 * p[0:1] for p in pair], axis=1)
    dsk2 = jnp.concatenate([2.0 * p[1:2] for p in pair], axis=1)
    lane1 = lax.broadcasted_iota(jnp.int32, (1, 2 * hd), 1)
    gt = jnp.zeros((1, 2 * hd), F32)
    for h in range(heads):
        gt = jnp.where(lane1 == h, st_all[h, 2:3, :], gt)
    gtemp_ref[...] = gt[:, 0:heads]

    def c5(i, carry):
        t = tile_of(i)
        for g in range(ngrp):
            c = slice(256 * g, 256 * g + 256)
            dqkv_v[t, c] = (mm(k_v[t, c], bd_g[g], NT) + q_v[t, c].astype(F32) * dsq2[:, c]).astype(BF16)
        return carry

    lax.fori_loop(0, nt, c5, 0)
    gw[2] = mm(u_v[...], dqkv_v[:, 0:width], TN).reshape(gw.shape[1:])
    rs_pre(2)
    rs_first(1)
    rs_relay(0)

    def c6(i, carry):
        t = tile_of(i)
        for g in range(ngrp):
            c = slice(256 * g, 256 * g + 256)
            dqkv_v[t, width + 256 * g:width + 256 * g + 256] = (
                mm(q_v[t, c], bd_g[g]) + k_v[t, c].astype(F32) * dsk2[:, c]).astype(BF16)
        return carry

    lax.fori_loop(0, nt, c6, 0)
    gw[3] = mm(u_v[...], dqkv_v[:, width:2 * width], TN).reshape(gw.shape[1:])
    rs_pre(3)
    rs_first(2)
    rs_relay(1)

    def out_copy(i):
        return pltpu.make_async_copy(x_v.at[tile_of(i)], out_hbm.at[tile_of(i)], out_sem.at[i])

    def gtok_copy(i):
        return pltpu.make_async_copy(dy_v.at[tile_of(i)], gtok_hbm.at[tile_of(i)], out_sem.at[nt + i])

    def c7(i, carry):
        t = tile_of(i)
        x_v[t, :] = (x_v[t, :].astype(F32) + mm(o_v[t, :], wout_v[...])).astype(BF16)
        out_copy(i).start()
        return carry

    def c8(i, carry):
        t = tile_of(i)
        du = mm(dqkv_v[t, :], wqkv_v[...], NT)
        xhat = xhat_v[t, :]
        p = du * xhat
        gbacc[0] += jnp.sum(p.reshape(tile // 8, 8, width), axis=0)
        gbacc[1] += jnp.sum(du.reshape(tile // 8, 8, width), axis=0)
        dxh = du * gain_v[...]
        m1 = jnp.mean(dxh, axis=1, keepdims=True)
        m2 = jnp.mean(p * gain_v[...], axis=1, keepdims=True)
        dx = rstd_v[t, :] * (dxh - m1 - xhat * m2)
        dy_v[t, :] = (dy_v[t, :].astype(F32) + dx).astype(BF16)
        gtok_copy(i).start()
        return carry

    lax.fori_loop(0, nt // 2, c8, 0)
    rs_first(3)
    rs_relay(2)
    lax.fori_loop(nt // 2, nt, c8, 0)

    gb_all[me, 0:1, :] = jnp.sum(gbacc[0], axis=0, keepdims=True)
    gb_all[me, 1:2, :] = jnp.sum(gbacc[1], axis=0, keepdims=True)
    for r in range(1, ns):
        to_all(5, gb_all, r).start()
    rs_relay(3)
    lax.fori_loop(0, nt, c7, 0)

    def gw_copy(pc):
        dst = gwout_hbm if pc == 0 else gwqkv_hbm.at[:, pl.ds({1: 2, 2: 0, 3: 1}[pc] * width, width)]
        return pltpu.make_async_copy(gwst.at[pc], dst, out_sem.at[2 * nt + pc])

    for pc in range(4):
        rs_final(pc)
        gw_copy(pc).start()

    for r in range(1, ns):
        to_all(5, gb_all, r).wait_recv()
    gb = gb_all[0, 0:2]
    for d in range(1, ns):
        gb = gb + gb_all[d, 0:2]
    ggain_ref[...] = gb[0:1]
    gbias_ref[...] = gb[1:2]

    for r in range(1, ns):
        to_owner(0, gsend, grecv, r).wait_send()
        to_owner(1, dsend, drecv, r).wait_send()
        to_all(2, a_all, r).wait_send()
        to_all(3, e_all, r).wait_send()
        to_all(4, st_all, r).wait_send()
        to_all(5, gb_all, r).wait_send()
    for pc in range(4):
        pre_copy(pc).wait_send()
        for cp in first_copies(pc) + relay_copies(pc):
            cp.wait_send()
        gw_copy(pc).wait()
    for i in range(nt):
        out_copy(i).wait()
        gtok_copy(i).wait()


def solution(mesh):
    ns = mesh.shape['sp']
    row_spec = P(('dp', 'sp'), None)
    part_spec = P('dp')

    def local_step(x, dy, gain, bias, w_qkv, w_out, temp):
        rows, width = x.shape
        heads = temp.shape[0]
        hd = width // heads
        tile = 512
        nt = rows // tile
        share = width // ns
        nchip = ns // 2
        ngrp = width // 256
        hbm = pl.BlockSpec(memory_space=pl.ANY)
        vmem = pl.BlockSpec(memory_space=pltpu.VMEM)
        tok = lambda: pltpu.VMEM((rows, width), BF16)
        outs = pl.pallas_call(
            functools.partial(kernel, ns, rows, width, heads, tile),
            out_shape=[jax.ShapeDtypeStruct((rows, width), BF16),
                       jax.ShapeDtypeStruct((rows, width), BF16),
                       jax.ShapeDtypeStruct((share, 3 * width), F32),
                       jax.ShapeDtypeStruct((share, width), F32),
                       jax.ShapeDtypeStruct((1, width), F32),
                       jax.ShapeDtypeStruct((1, width), F32),
                       jax.ShapeDtypeStruct((1, heads), F32)],
            in_specs=[hbm] * 6 + [pl.BlockSpec(memory_space=pltpu.SMEM)],
            out_specs=[hbm] * 4 + [vmem] * 3,
            scratch_shapes=[
                tok(), tok(), pltpu.VMEM((1, width), F32), pltpu.VMEM((1, width), F32),
                pltpu.VMEM((width, 3 * width), BF16), pltpu.VMEM((width, width), BF16),
                tok(), tok(), tok(), tok(), tok(), tok(), pltpu.VMEM((rows, 3 * width), BF16),
                pltpu.VMEM((rows, width), F32), pltpu.VMEM((rows, 1), F32),
                pltpu.VMEM((ngrp, 256, 256), F32), pltpu.VMEM((ngrp, 256, 256), F32),
                pltpu.VMEM((8, width), F32), pltpu.VMEM((8, width), F32),
                pltpu.VMEM((heads, hd // 2 + 8, 2 * hd), F32), pltpu.VMEM((ns, hd // 2 + 8, 2 * hd), F32),
                pltpu.VMEM((heads, hd // 2, 2 * hd), F32), pltpu.VMEM((ns, hd // 2, 2 * hd), F32),
                pltpu.VMEM((heads, hd, 2 * hd), BF16), pltpu.VMEM((heads, hd, 2 * hd), BF16),
                pltpu.VMEM((heads, 8, 2 * hd), F32),
                pltpu.VMEM((ngrp, 256, 256), BF16), pltpu.VMEM((ngrp, 256, 256), BF16),
                pltpu.VMEM((4, nchip, 2, share, width), F32), pltpu.VMEM((4, nchip, share, width), F32),
                pltpu.VMEM((4, 2, share // 2, width), F32), pltpu.VMEM((4, 2, share // 2, width), F32),
                pltpu.VMEM((4, 2, share // 2, width), F32), pltpu.VMEM((4, share, width), F32),
                pltpu.VMEM((2, 8, width), F32), pltpu.VMEM((ns, 8, width), F32),
                pltpu.SemaphoreType.DMA((2 * nt + 5,)), pltpu.SemaphoreType.DMA((2 * nt + 4,)),
                pltpu.SemaphoreType.DMA((6, ns)), pltpu.SemaphoreType.DMA((6, ns)),
                pltpu.SemaphoreType.DMA((4,)), pltpu.SemaphoreType.DMA((4,)),
                pltpu.SemaphoreType.DMA((4, 6)), pltpu.SemaphoreType.DMA((4, 6)),
            ],
            compiler_params=pltpu.CompilerParams(collective_id=0, has_side_effects=True,
                                                 vmem_limit_bytes=60 * 1024 * 1024),
        )(x, dy, gain.reshape(1, -1), bias.reshape(1, -1), w_qkv, w_out, temp)
        out, gtok, gwqkv, gwout, ggain, gbias, gtemp = outs
        return out, gtok, gwqkv, gwout, ggain.reshape(-1), gbias.reshape(-1), gtemp.reshape(-1)

    full = P()
    return jax.shard_map(local_step, mesh=mesh,
                         in_specs=(row_spec, row_spec, full, full, full, full, full),
                         out_specs=(row_spec, row_spec, row_spec, row_spec, part_spec, part_spec, part_spec),
                         check_vma=False)
```

```python
import functools

import jax
import jax.numpy as jnp
from jax import lax
from jax.experimental import pallas as pl
from jax.experimental.pallas import tpu as pltpu
from jax.sharding import PartitionSpec as P

F32 = jnp.float32
BF16 = jnp.bfloat16
NN = (((1,), (0,)), ((), ()))
NT = (((1,), (1,)), ((), ()))
TN = (((0,), (0,)), ((), ()))
EPS = 1e-6


def mm(a, b, dims=NN):
    return lax.dot_general(a, b, dims, preferred_element_type=F32)


def kernel(ns, rows, width, heads, tile,
           x_hbm, dy_hbm, gain_hbm, bias_hbm, wqkv_hbm, wout_hbm, temp_ref,
           out_v, gtok_v, gwst, ggain_ref, gbias_ref, gtemp_ref,
           x_v, dy_v, gain_v, bias_v, wqkv_v, wout_v,
           u_v, q_v, k_v, v_v, do_v, o_v, dqkv_v, xhat_v, rstd_v,
           gacc, dacc, sqacc, skacc, gsend, grecv, dsend, drecv, a_all, e_all, st_all, bd_a, bd_g,
           gw, pre, opp, nrr, rlr, gbacc, gb_all,
           in_sem, small_s, small_r, pre_s, pre_r, x2_s, x2_r):
    me = lax.axis_index('sp')
    nt = rows // tile
    hd = width // heads
    core = lax.rem(me, 2)
    chip = me // 2
    nchip = ns // 2
    partner = me + 1 - 2 * core
    right = lax.rem(me + 2, ns)
    left = lax.rem(me + ns - 2, ns)
    c_r = lax.rem(chip + 1, nchip)
    c_l = lax.rem(chip + nchip - 1, nchip)
    c_o = lax.rem(chip + 2, nchip)

    def remote(src, dst, ssem, rsem, dev):
        return pltpu.make_async_remote_copy(src_ref=src, dst_ref=dst, send_sem=ssem, recv_sem=rsem,
                                            device_id={'sp': dev}, device_id_type=pl.DeviceIdType.MESH)

    barrier = pltpu.get_barrier_semaphore()
    for r in range(1, ns):
        pl.semaphore_signal(barrier, inc=1, device_id={'sp': lax.rem(me + r, ns)},
                            device_id_type=pl.DeviceIdType.MESH)

    def ld(i, src, dst):
        return pltpu.make_async_copy(src, dst, in_sem.at[i])

    def tile_of(i):
        return pl.ds(pl.multiple_of(i * tile, tile), tile)

    def x_copy(i):
        return ld(i, x_hbm.at[tile_of(i)], x_v.at[tile_of(i)])

    def dy_copy(i):
        return ld(nt + i, dy_hbm.at[tile_of(i)], dy_v.at[tile_of(i)])

    gain_copy = ld(2 * nt, gain_hbm, gain_v)
    bias_copy = ld(2 * nt + 1, bias_hbm, bias_v)
    wqk_copy = ld(2 * nt + 2, wqkv_hbm.at[:, 0:2 * width], wqkv_v.at[:, 0:2 * width])
    wv_copy = ld(2 * nt + 3, wqkv_hbm.at[:, 2 * width:3 * width], wqkv_v.at[:, 2 * width:3 * width])
    wout_copy = ld(2 * nt + 4, wout_hbm, wout_v)
    gain_copy.start()
    bias_copy.start()
    x_copy(0).start()
    wqk_copy.start()
    for i in range(1, nt):
        x_copy(i).start()
    wv_copy.start()
    wout_copy.start()
    for i in range(nt):
        dy_copy(i).start()

    with jax.named_scope("init"):
        gacc[...] = jnp.zeros_like(gacc)
        dacc[...] = jnp.zeros_like(dacc)
        sqacc[...] = jnp.zeros_like(sqacc)
        skacc[...] = jnp.zeros_like(skacc)
        gbacc[...] = jnp.zeros_like(gbacc)
        bd_a[...] = jnp.zeros_like(bd_a)
        bd_g[...] = jnp.zeros_like(bd_g)
        gain_copy.wait()
        bias_copy.wait()
        wqk_copy.wait()

    ngrp = width // 256
    hpg = heads // ngrp

    def c1(i, carry):
        x_copy(i).wait()
        t = tile_of(i)
        x = x_v[t, :].astype(F32)
        mean = jnp.mean(x, axis=1, keepdims=True)
        cent = x - mean
        var = jnp.mean(cent * cent, axis=1, keepdims=True)
        rstd = lax.rsqrt(var + EPS)
        xhat = cent * rstd
        xhat_v[t, :] = xhat
        rstd_v[t, :] = rstd
        u = (xhat * gain_v[...] + bias_v[...]).astype(BF16)
        u_v[t, :] = u
        q = mm(u, wqkv_v[:, 0:width]).astype(BF16)
        q_v[t, :] = q
        k = mm(u, wqkv_v[:, width:2 * width]).astype(BF16)
        k_v[t, :] = k
        for g in range(ngrp):
            c = slice(256 * g, 256 * g + 256)
            gacc[g] += mm(q[:, c], k[:, c], TN)
        q32 = q.astype(F32)
        k32 = k.astype(F32)
        sqacc[...] += jnp.sum((q32 * q32).reshape(tile // 8, 8, width), axis=0)
        skacc[...] += jnp.sum((k32 * k32).reshape(tile // 8, 8, width), axis=0)
        return carry

    with jax.named_scope("c1"):
        lax.fori_loop(0, nt, c1, 0)

    lane32 = lax.broadcasted_iota(jnp.int32, (hd // 2, 2 * hd), 1)

    def pack(acc, h):
        g, hh = h // hpg, h % hpg
        blk = acc[g, hh * hd:hh * hd + hd, (hh // 2) * 128:(hh // 2) * 128 + 128]
        top, bot = blk[0:hd // 2], blk[hd // 2:hd]
        if h % 2 == 0:
            bot = pltpu.roll(bot, hd, axis=1)
        else:
            top = pltpu.roll(top, hd, axis=1)
        return jnp.where(lane32 < hd, top, bot)

    with jax.named_scope("packg"):
        sq_row = jnp.sum(sqacc[...], axis=0, keepdims=True)
        sk_row = jnp.sum(skacc[...], axis=0, keepdims=True)
        for h in range(heads):
            gsend[h, 0:hd // 2, :] = pack(gacc, h)
            c = slice((h // 2) * 128, (h // 2) * 128 + 128)
            gsend[h, hd // 2:hd // 2 + 1, :] = sq_row[:, c]
            gsend[h, hd // 2 + 1:hd // 2 + 2, :] = sk_row[:, c]

    def to_owner(kind, src, dst, r):
        dst_dev = lax.rem(me + r, ns)
        return remote(src.at[dst_dev], dst.at[r], small_s.at[kind, r], small_r.at[kind, r], dst_dev)

    def to_all(kind, buf, r):
        return remote(buf.at[me], buf.at[me], small_s.at[kind, r], small_r.at[kind, r], lax.rem(me + r, ns))

    with jax.named_scope("sendg"):
        pl.semaphore_wait(barrier, ns - 1)
        for r in range(1, ns):
            to_owner(0, gsend, grecv, r).start()

    wv_copy.wait()
    wout_copy.wait()

    def c2(i, carry):
        dy_copy(i).wait()
        t = tile_of(i)
        v = mm(u_v[t, :], wqkv_v[:, 2 * width:3 * width]).astype(BF16)
        v_v[t, :] = v
        do = mm(dy_v[t, :], wout_v[...], NT).astype(BF16)
        do_v[t, :] = do
        for g in range(ngrp):
            c = slice(256 * g, 256 * g + 256)
            dacc[g] += mm(do[:, c], v[:, c], TN)
        return carry

    with jax.named_scope("c2"):
        lax.fori_loop(0, nt, c2, 0)
    with jax.named_scope("sendd"):
        for h in range(heads):
            dsend[h] = pack(dacc, h)
        for r in range(1, ns):
            to_owner(1, dsend, drecv, r).start()

    row = lax.broadcasted_iota(jnp.int32, (hd, 2 * hd), 0)
    lanep = lax.broadcasted_iota(jnp.int32, (hd, 2 * hd), 1) - hd * core
    half = (lanep >= 0) & (lanep < hd)
    diag = lanep == row
    half1 = half[0:1]

    def unpack(p):
        rolled = pltpu.roll(p, hd, axis=1)
        even = core == 0
        full = jnp.concatenate([jnp.where(even, p, rolled), jnp.where(even, rolled, p)], axis=0)
        return jnp.where(half, full, 0.0)

    with jax.named_scope("waitg"):
        for r in range(1, ns):
            to_owner(0, gsend, grecv, r).wait_recv()
    with jax.named_scope("soft"):
        tot = gsend[me, 0:hd // 2 + 2]
        for r in range(1, ns):
            tot = tot + grecv[r, 0:hd // 2 + 2]
        gram = unpack(tot[0:hd // 2])
        sq_r = tot[hd // 2:hd // 2 + 1]
        sk_r = jnp.where(half1, tot[hd // 2 + 1:hd // 2 + 2], 1.0)
        sq_c = jnp.sum(jnp.where(diag, sq_r, 0.0), axis=1, keepdims=True)
        den = jnp.sqrt(sq_c) * jnp.sqrt(sk_r)
        cosine = gram / den
        temp = temp_ref[me]
        logits = jnp.where(half, temp * cosine, -jnp.inf)
        ex = jnp.exp(logits - jnp.max(logits, axis=1, keepdims=True))
        attn = ex / jnp.sum(ex, axis=1, keepdims=True)
        a_all[me] = attn.astype(BF16)
        for r in range(1, ns):
            to_all(2, a_all, r).start()

    with jax.named_scope("waitd"):
        for r in range(1, ns):
            to_owner(1, dsend, drecv, r).wait_recv()
    with jax.named_scope("vjp"):
        dtot = dsend[me]
        for r in range(1, ns):
            dtot = dtot + drecv[r]
        d_a = unpack(dtot)
        inner = jnp.sum(d_a * attn, axis=1, keepdims=True)
        d_s = attn * (d_a - inner)
        d_cos = temp * d_s
        d_t = jnp.sum(jnp.sum(d_s * cosine, axis=1, keepdims=True), axis=0, keepdims=True)
        e_all[me] = (d_cos / den).astype(BF16)
        ec = d_cos * cosine
        dsq_c = -0.5 * jnp.sum(ec, axis=1, keepdims=True) / sq_c
        dsk_r = -0.5 * jnp.sum(ec, axis=0, keepdims=True) / sk_r
        dsq_r = jnp.sum(jnp.where(diag, dsq_c, 0.0), axis=0, keepdims=True)
        st_all[me, 0:1, :] = dsq_r
        st_all[me, 1:2, :] = dsk_r
        st_all[me, 2:3, :] = jnp.broadcast_to(d_t, (1, 2 * hd))
        for r in range(1, ns):
            to_all(3, e_all, r).start()
        for r in range(1, ns):
            to_all(4, st_all, r).start()

    def fill(bd, blocks):
        for g in range(ngrp):
            for j in range(2):
                s = slice(128 * j, 128 * j + 128)
                h = g * hpg + 2 * j
                bd[g, s, s] = blocks[h:h + 2].reshape(128, 128)

    def pre_copy(pc):
        return remote(gw.at[pc, :, 1 - core], pre.at[pc], pre_s.at[pc], pre_r.at[pc], partner)

    hr = gw.shape[3] // 2
    lo, hi = slice(0, hr), slice(hr, 2 * hr)

    def first_copies(pc):
        return [remote(pre.at[pc, c_o, lo], opp.at[pc, 0], x2_s.at[pc, 0], x2_r.at[pc, 0], right),
                remote(pre.at[pc, c_o, hi], opp.at[pc, 1], x2_s.at[pc, 1], x2_r.at[pc, 1], left),
                remote(pre.at[pc, c_r, hi], nrr.at[pc, 0], x2_s.at[pc, 2], x2_r.at[pc, 2], right),
                remote(pre.at[pc, c_l, lo], nrr.at[pc, 1], x2_s.at[pc, 3], x2_r.at[pc, 3], left)]

    def relay_copies(pc):
        return [remote(pre.at[pc, c_r, lo], rlr.at[pc, 0], x2_s.at[pc, 4], x2_r.at[pc, 4], right),
                remote(pre.at[pc, c_l, hi], rlr.at[pc, 1], x2_s.at[pc, 5], x2_r.at[pc, 5], left)]

    def rs_pre(pc):
        pre_copy(pc).start()

    def rs_first(pc):
        pre_copy(pc).wait_recv()
        pre[pc] = pre[pc] + gw[pc, :, core]
        for cp in first_copies(pc):
            cp.start()

    def rs_relay(pc):
        first, second = first_copies(pc), relay_copies(pc)
        first[0].wait_recv()
        pre[pc, c_r, lo] = pre[pc, c_r, lo] + opp[pc, 0]
        second[0].start()
        first[1].wait_recv()
        pre[pc, c_l, hi] = pre[pc, c_l, hi] + opp[pc, 1]
        second[1].start()

    def rs_final(pc):
        first, second = first_copies(pc), relay_copies(pc)
        first[2].wait_recv()
        first[3].wait_recv()
        second[0].wait_recv()
        second[1].wait_recv()
        gwst[pc, lo] = pre[pc, chip, lo] + rlr[pc, 0] + nrr[pc, 1]
        gwst[pc, hi] = pre[pc, chip, hi] + nrr[pc, 0] + rlr[pc, 1]

    with jax.named_scope("waita"):
        for r in range(1, ns):
            to_all(2, a_all, r).wait_recv()
    fill(bd_a, a_all)

    def c3(i, carry):
        t = tile_of(i)
        for g in range(ngrp):
            c = slice(256 * g, 256 * g + 256)
            o_v[t, c] = mm(v_v[t, c], bd_a[g], NT).astype(BF16)
        return carry

    with jax.named_scope("c3"):
        lax.fori_loop(0, nt, c3, 0)
    with jax.named_scope("gw0"):
        gw[0] = mm(o_v[...], dy_v[...], TN).reshape(gw.shape[1:])
        rs_pre(0)

    def c4(i, carry):
        t = tile_of(i)
        for g in range(ngrp):
            c = slice(256 * g, 256 * g + 256)
            dqkv_v[t, 2 * width + 256 * g:2 * width + 256 * g + 256] = mm(do_v[t, c], bd_a[g]).astype(BF16)
        return carry

    with jax.named_scope("c4"):
        lax.fori_loop(0, nt, c4, 0)
    with jax.named_scope("gw1"):
        gw[1] = mm(u_v[...], dqkv_v[:, 2 * width:3 * width], TN).reshape(gw.shape[1:])
        rs_pre(1)
    with jax.named_scope("first0"):
        rs_first(0)

    with jax.named_scope("waite"):
        for r in range(1, ns):
            to_all(3, e_all, r).wait_recv()
        for r in range(1, ns):
            to_all(4, st_all, r).wait_recv()
    fill(bd_g, e_all)
    pair = [st_all[2 * j, 0:2, :] + st_all[2 * j + 1, 0:2, :] for j in range(heads // 2)]
    dsq2 = jnp.concatenate([2.0 * p[0:1] for p in pair], axis=1)
    dsk2 = jnp.concatenate([2.0 * p[1:2] for p in pair], axis=1)
    lane1 = lax.broadcasted_iota(jnp.int32, (1, 2 * hd), 1)
    gt = jnp.zeros((1, 2 * hd), F32)
    for h in range(heads):
        gt = jnp.where(lane1 == h, st_all[h, 2:3, :], gt)
    gtemp_ref[...] = gt[:, 0:heads]

    def c5(i, carry):
        t = tile_of(i)
        for g in range(ngrp):
            c = slice(256 * g, 256 * g + 256)
            dqkv_v[t, c] = (mm(k_v[t, c], bd_g[g], NT) + q_v[t, c].astype(F32) * dsq2[:, c]).astype(BF16)
        return carry

    with jax.named_scope("c5"):
        lax.fori_loop(0, nt, c5, 0)
    with jax.named_scope("gw2"):
        gw[2] = mm(u_v[...], dqkv_v[:, 0:width], TN).reshape(gw.shape[1:])
        rs_pre(2)
    with jax.named_scope("first1relay0"):
        rs_first(1)
        rs_relay(0)

    def c6(i, carry):
        t = tile_of(i)
        for g in range(ngrp):
            c = slice(256 * g, 256 * g + 256)
            dqkv_v[t, width + 256 * g:width + 256 * g + 256] = (
                mm(q_v[t, c], bd_g[g]) + k_v[t, c].astype(F32) * dsk2[:, c]).astype(BF16)
        return carry

    with jax.named_scope("c6"):
        lax.fori_loop(0, nt, c6, 0)
    with jax.named_scope("gw3"):
        gw[3] = mm(u_v[...], dqkv_v[:, width:2 * width], TN).reshape(gw.shape[1:])
        rs_pre(3)
    with jax.named_scope("first2relay1"):
        rs_first(2)
        rs_relay(1)

    def c7(i, carry):
        t = tile_of(i)
        out_v[t, :] = (x_v[t, :].astype(F32) + mm(o_v[t, :], wout_v[...])).astype(BF16)
        return carry

    def c8(i, carry):
        t = tile_of(i)
        du = mm(dqkv_v[t, :], wqkv_v[...], NT)
        xhat = xhat_v[t, :]
        p = du * xhat
        gbacc[0] += jnp.sum(p.reshape(tile // 8, 8, width), axis=0)
        gbacc[1] += jnp.sum(du.reshape(tile // 8, 8, width), axis=0)
        dxh = du * gain_v[...]
        m1 = jnp.mean(dxh, axis=1, keepdims=True)
        m2 = jnp.mean(p * gain_v[...], axis=1, keepdims=True)
        dx = rstd_v[t, :] * (dxh - m1 - xhat * m2)
        gtok_v[t, :] = (dy_v[t, :].astype(F32) + dx).astype(BF16)
        return carry

    with jax.named_scope("c8a"):
        lax.fori_loop(0, nt // 2, c8, 0)
    with jax.named_scope("first3relay2"):
        rs_first(3)
        rs_relay(2)
    with jax.named_scope("c8b"):
        lax.fori_loop(nt // 2, nt, c8, 0)

    gb_all[me, 0:1, :] = jnp.sum(gbacc[0], axis=0, keepdims=True)
    gb_all[me, 1:2, :] = jnp.sum(gbacc[1], axis=0, keepdims=True)
    for r in range(1, ns):
        to_all(5, gb_all, r).start()
    with jax.named_scope("relay3"):
        rs_relay(3)
    with jax.named_scope("c7"):
        lax.fori_loop(0, nt, c7, 0)

    with jax.named_scope("final"):
        for pc in range(4):
            rs_final(pc)

    with jax.named_scope("gb"):
        for r in range(1, ns):
            to_all(5, gb_all, r).wait_recv()
        gb = gb_all[0, 0:2]
        for d in range(1, ns):
            gb = gb + gb_all[d, 0:2]
        ggain_ref[...] = gb[0:1]
        gbias_ref[...] = gb[1:2]

    with jax.named_scope("drain"):
        for r in range(1, ns):
            to_owner(0, gsend, grecv, r).wait_send()
            to_owner(1, dsend, drecv, r).wait_send()
            to_all(2, a_all, r).wait_send()
            to_all(3, e_all, r).wait_send()
            to_all(4, st_all, r).wait_send()
            to_all(5, gb_all, r).wait_send()
        for pc in range(4):
            pre_copy(pc).wait_send()
            for cp in first_copies(pc) + relay_copies(pc):
                cp.wait_send()


def writer(width, out_v, gtok_v, gwst, gg_v, gb_v, gt_v, out_hbm, gtok_hbm, gwqkv_hbm, gwout_hbm, gg_hbm, gb_hbm, gt_hbm, sem):
    copies = [(out_v, out_hbm), (gtok_v, gtok_hbm), (gwst.at[0], gwout_hbm), (gg_v, gg_hbm), (gb_v, gb_hbm), (gt_v, gt_hbm)]
    copies += [(gwst.at[pc], gwqkv_hbm.at[:, pl.ds(c * width, width)]) for pc, c in ((1, 2), (2, 0), (3, 1))]
    for i, (src, dst) in enumerate(copies):
        pltpu.make_async_copy(src, dst, sem.at[i]).start()
    for i, (src, dst) in enumerate(copies):
        pltpu.make_async_copy(src, dst, sem.at[i]).wait()


def solution(mesh):
    ns = mesh.shape['sp']
    row_spec = P(('dp', 'sp'), None)
    part_spec = P('dp')

    def local_step(x, dy, gain, bias, w_qkv, w_out, temp):
        rows, width = x.shape
        heads = temp.shape[0]
        hd = width // heads
        tile = 512
        nt = rows // tile
        share = width // ns
        nchip = ns // 2
        ngrp = width // 256
        hbm = pl.BlockSpec(memory_space=pl.ANY)
        vmem = pl.BlockSpec(memory_space=pltpu.VMEM)
        tok = lambda: pltpu.VMEM((rows, width), BF16)
        outs = pl.pallas_call(
            functools.partial(kernel, ns, rows, width, heads, tile),
            out_shape=[pltpu.VMEM((rows, width), BF16), pltpu.VMEM((rows, width), BF16),
                       pltpu.VMEM((4, share, width), F32), pltpu.VMEM((1, width), F32),
                       pltpu.VMEM((1, width), F32), pltpu.VMEM((1, heads), F32)],
            in_specs=[hbm] * 6 + [pl.BlockSpec(memory_space=pltpu.SMEM)],
            out_specs=[vmem] * 6,
            scratch_shapes=[
                tok(), tok(), pltpu.VMEM((1, width), F32), pltpu.VMEM((1, width), F32),
                pltpu.VMEM((width, 3 * width), BF16), pltpu.VMEM((width, width), BF16),
                tok(), tok(), tok(), tok(), tok(), tok(), pltpu.VMEM((rows, 3 * width), BF16),
                pltpu.VMEM((rows, width), F32), pltpu.VMEM((rows, 1), F32),
                pltpu.VMEM((ngrp, 256, 256), F32), pltpu.VMEM((ngrp, 256, 256), F32),
                pltpu.VMEM((8, width), F32), pltpu.VMEM((8, width), F32),
                pltpu.VMEM((heads, hd // 2 + 8, 2 * hd), F32), pltpu.VMEM((ns, hd // 2 + 8, 2 * hd), F32),
                pltpu.VMEM((heads, hd // 2, 2 * hd), F32), pltpu.VMEM((ns, hd // 2, 2 * hd), F32),
                pltpu.VMEM((heads, hd, 2 * hd), BF16), pltpu.VMEM((heads, hd, 2 * hd), BF16),
                pltpu.VMEM((heads, 8, 2 * hd), F32),
                pltpu.VMEM((ngrp, 256, 256), BF16), pltpu.VMEM((ngrp, 256, 256), BF16),
                pltpu.VMEM((4, nchip, 2, share, width), F32), pltpu.VMEM((4, nchip, share, width), F32),
                pltpu.VMEM((4, 2, share // 2, width), F32), pltpu.VMEM((4, 2, share // 2, width), F32),
                pltpu.VMEM((4, 2, share // 2, width), F32),
                pltpu.VMEM((2, 8, width), F32), pltpu.VMEM((ns, 8, width), F32),
                pltpu.SemaphoreType.DMA((2 * nt + 5,)),
                pltpu.SemaphoreType.DMA((6, ns)), pltpu.SemaphoreType.DMA((6, ns)),
                pltpu.SemaphoreType.DMA((4,)), pltpu.SemaphoreType.DMA((4,)),
                pltpu.SemaphoreType.DMA((4, 6)), pltpu.SemaphoreType.DMA((4, 6)),
            ],
            compiler_params=pltpu.CompilerParams(collective_id=0, has_side_effects=True,
                                                 vmem_limit_bytes=52 * 1024 * 1024),
        )(x, dy, gain.reshape(1, -1), bias.reshape(1, -1), w_qkv, w_out, temp)
        out, gtok, gwqkv, gwout, ggain, gbias, gtemp = pl.pallas_call(
            functools.partial(writer, width),
            out_shape=[jax.ShapeDtypeStruct((rows, width), BF16),
                       jax.ShapeDtypeStruct((rows, width), BF16),
                       jax.ShapeDtypeStruct((share, 3 * width), F32),
                       jax.ShapeDtypeStruct((share, width), F32),
                       jax.ShapeDtypeStruct((1, width), F32),
                       jax.ShapeDtypeStruct((1, width), F32),
                       jax.ShapeDtypeStruct((1, heads), F32)],
            in_specs=[vmem] * 6,
            out_specs=[hbm] * 7,
            scratch_shapes=[pltpu.SemaphoreType.DMA((9,))],
            compiler_params=pltpu.CompilerParams(vmem_limit_bytes=1024 * 1024),
        )(*outs)
        return out, gtok, gwqkv, gwout, ggain.reshape(-1), gbias.reshape(-1), gtemp.reshape(-1)

    full = P()
    return jax.shard_map(local_step, mesh=mesh,
                         in_specs=(row_spec, row_spec, full, full, full, full, full),
                         out_specs=(row_spec, row_spec, row_spec, row_spec, part_spec, part_spec, part_spec),
                         check_vma=False)
```

```python
import functools

import jax
import jax.numpy as jnp
from jax import lax
from jax.experimental import pallas as pl
from jax.experimental.pallas import tpu as pltpu
from jax.sharding import PartitionSpec as P

F32 = jnp.float32
BF16 = jnp.bfloat16
NN = (((1,), (0,)), ((), ()))
NT = (((1,), (1,)), ((), ()))
TN = (((0,), (0,)), ((), ()))
EPS = 1e-6


def mm(a, b, dims=NN):
    return lax.dot_general(a, b, dims, preferred_element_type=F32)


def kernel(ns, rows, width, heads, tile,
           x_hbm, dy_hbm, gain_hbm, bias_hbm, wqkv_hbm, wout_hbm, temp_ref,
           out_v, gtok_v, gwst, ggain_ref, gbias_ref, gtemp_ref,
           x_v, dy_v, gain_v, bias_v, wqkv_v, wout_v,
           u_v, q_v, k_v, v_v, do_v, o_v, dqkv_v, mean_v, rstd_v,
           gacc, dacc, sqacc, skacc, gsend, gpre, grecv, dsend, dpre, drecv, a_all, e_all, st_all, bd_a, bd_g,
           gw, pre, opp, fin, gbacc, gb_all,
           in_sem, own_s, own_r, all_s, all_r, pre_s, pre_r, opp_s, opp_r, fin_s, fin_r):
    me = lax.axis_index('sp')
    nt = rows // tile
    hd = width // heads
    core = lax.rem(me, 2)
    chip = me // 2
    nchip = ns // 2
    partner = me + 1 - 2 * core
    right = lax.rem(me + 2, ns)
    left = lax.rem(me + ns - 2, ns)
    c_r = lax.rem(chip + 1, nchip)
    c_l = lax.rem(chip + nchip - 1, nchip)
    c_o = lax.rem(chip + 2, nchip)
    scope = jax.named_scope

    def remote(src, dst, ssem, rsem, dev):
        return lambda: pltpu.make_async_remote_copy(src_ref=src, dst_ref=dst, send_sem=ssem, recv_sem=rsem,
                                                    device_id={'sp': dev}, device_id_type=pl.DeviceIdType.MESH)

    def wait_bytes(ref, sem):
        pltpu.make_async_copy(ref, ref, sem).wait()

    far_first = sorted(range(1, nchip), key=lambda s: -min(s, nchip - s))
    peers = [2 * lax.rem(chip + s, nchip) + c for s in far_first for c in (core, 1 - core)] + [partner]

    barrier = pltpu.get_barrier_semaphore()
    for dev in peers:
        pl.semaphore_signal(barrier, inc=1, device_id={'sp': dev}, device_id_type=pl.DeviceIdType.MESH)

    def ld(i, src, dst):
        return lambda: pltpu.make_async_copy(src, dst, in_sem.at[i])

    def tile_of(i):
        return slice(i * tile, (i + 1) * tile)

    def x_copy(i):
        return ld(i, x_hbm.at[tile_of(i)], x_v.at[tile_of(i)])

    dy_copy = ld(nt, dy_hbm, dy_v)
    gain_copy = ld(nt + 1, gain_hbm, gain_v)
    bias_copy = ld(nt + 2, bias_hbm, bias_v)
    wqk_copy = ld(nt + 3, wqkv_hbm.at[:, 0:2 * width], wqkv_v.at[:, 0:2 * width])
    wv_copy = ld(nt + 4, wqkv_hbm.at[:, 2 * width:3 * width], wqkv_v.at[:, 2 * width:3 * width])
    wout_copy = ld(nt + 5, wout_hbm, wout_v)
    gain_copy().start()
    bias_copy().start()
    x_copy(0)().start()
    wqk_copy().start()
    for i in range(1, nt):
        x_copy(i)().start()
    wv_copy().start()
    wout_copy().start()
    dy_copy().start()

    with scope('init'):
        bd_a[...] = jnp.zeros_like(bd_a)
        bd_g[...] = jnp.zeros_like(bd_g)
        gain_copy().wait()
        bias_copy().wait()

    ngrp = width // 256
    hpg = heads // ngrp

    def cols(g):
        return slice(256 * g, 256 * g + 256)

    def ln(t):
        x = x_v[t, :].astype(F32)
        mean = jnp.mean(x, axis=1, keepdims=True)
        cent = x - mean
        var = jnp.mean(cent * cent, axis=1, keepdims=True)
        rstd = lax.rsqrt(var + EPS)
        mean_v[t, :] = mean
        rstd_v[t, :] = rstd
        u_v[t, :] = (cent * rstd * gain_v[...] + bias_v[...]).astype(BF16)

    def accumulate(ref, idx, val, first):
        if first:
            ref[idx] = val
        else:
            ref[idx] += val

    def square_sum(ref, c, val, first):
        v32 = val.astype(F32)
        part = jnp.sum((v32 * v32).reshape(tile // 8, 8, 256), axis=0)
        ref[:, c] = part if first else ref[:, c] + part

    nsub = 2 * ngrp
    sub = tile // nsub

    def ln_sub(i, j):
        if i < nt:
            ln(slice(i * tile + j * sub, i * tile + (j + 1) * sub))

    with scope('c1'):
        x_copy(0)().wait()
        for j in range(nsub):
            ln_sub(0, j)
        wqk_copy().wait()
        for i in range(1, nt):
            x_copy(i)().wait()
        for i in range(nt):
            t = tile_of(i)
            for g in range(ngrp):
                c = cols(g)
                q = mm(u_v[t, :], wqkv_v[:, c]).astype(BF16)
                q_v[t, c] = q
                square_sum(sqacc, c, q, i == 0)
                ln_sub(i + 1, 2 * g)
                k = mm(u_v[t, :], wqkv_v[:, width + 256 * g:width + 256 * g + 256]).astype(BF16)
                k_v[t, c] = k
                square_sum(skacc, c, k, i == 0)
                ln_sub(i + 1, 2 * g + 1)
                accumulate(gacc, g, mm(q, k, TN), i == 0)

    lane32 = lax.broadcasted_iota(jnp.int32, (hd // 2, 2 * hd), 1)

    def pack_block(blk, odd):
        top, bot = blk[0:hd // 2], blk[hd // 2:hd]
        if odd:
            top = pltpu.roll(top, hd, axis=1)
        else:
            bot = pltpu.roll(bot, hd, axis=1)
        return jnp.where(lane32 < hd, top, bot)

    def pack(acc, h):
        g, hh = h // hpg, h % hpg
        return pack_block(acc[g, hh * hd:hh * hd + hd, (hh // 2) * 128:(hh // 2) * 128 + 128], h % 2 == 1)

    with scope('packg'):
        sq_row = jnp.sum(sqacc[...], axis=0, keepdims=True)
        sk_row = jnp.sum(skacc[...], axis=0, keepdims=True)
        for h in range(heads):
            gsend[h // 2, h % 2, 0:hd // 2, :] = pack(gacc, h)
            c = slice((h // 2) * 128, (h // 2) * 128 + 128)
            gsend[h // 2, h % 2, hd // 2:hd // 2 + 1, :] = sq_row[:, c]
            gsend[h // 2, h % 2, hd // 2 + 1:hd // 2 + 2, :] = sk_row[:, c]

    def to_partner(kind, src, dst):
        return remote(src.at[:, 1 - core], dst, own_s.at[kind, 0], own_r.at[kind, 0], partner)

    def chip_sum(kind, src, mid, dst):
        wait_bytes(mid, own_r.at[kind, 0])
        n = mid.shape[1] if kind else hd // 2 + 2
        for c in range(nchip):
            mid[c, 0:n] = mid[c, 0:n] + src[c, core, 0:n]
        for s in far_first:
            c = lax.rem(chip + s, nchip)
            remote(mid.at[c], dst.at[s], own_s.at[kind, 1], own_r.at[kind, 1], 2 * c + core)().start()

    def image_sum(kind, mid, dst):
        n = mid.shape[1] if kind else hd // 2 + 2
        wait_bytes(dst.at[1:nchip], own_r.at[kind, 1])
        tot = mid[chip, 0:n]
        for s in range(1, nchip):
            tot = tot + dst[s, 0:n]
        return tot

    def to_all(kind, buf):
        for dev in peers:
            remote(buf.at[me], buf.at[me], all_s.at[kind], all_r.at[kind], dev)().start()

    def from_all(kind, buf):
        wait_bytes(buf.at[0:ns - 1], all_r.at[kind])

    with scope('sendg'):
        pl.semaphore_wait(barrier, ns - 1)
        to_partner(0, gsend, gpre)().start()

    def c2(i):
        t = tile_of(i)
        v = mm(u_v[t, :], wqkv_v[:, 2 * width:3 * width]).astype(BF16)
        v_v[t, :] = v
        do = mm(dy_v[t, :], wout_v[...], NT).astype(BF16)
        do_v[t, :] = do
        for g in range(ngrp):
            accumulate(dacc, g, mm(do[:, cols(g)], v[:, cols(g)], TN), i == 0)

    with scope('c2a'):
        wv_copy().wait()
        wout_copy().wait()
        dy_copy().wait()
        c2(0)
    with scope('chipg'):
        chip_sum(0, gsend, gpre, grecv)
    with scope('c2b'):
        for i in range(1, nt):
            c2(i)
    with scope('sendd'):
        for h in range(heads):
            dsend[h // 2, h % 2] = pack(dacc, h)
        to_partner(1, dsend, dpre)().start()

    row = lax.broadcasted_iota(jnp.int32, (hd, 2 * hd), 0)
    lanep = lax.broadcasted_iota(jnp.int32, (hd, 2 * hd), 1) - hd * core
    half = (lanep >= 0) & (lanep < hd)
    diag = lanep == row
    half1 = half[0:1]
    even = core == 0

    def unpack(p):
        rolled = pltpu.roll(p, hd, axis=1)
        full = jnp.concatenate([jnp.where(even, p, rolled), jnp.where(even, rolled, p)], axis=0)
        return jnp.where(half, full, 0.0)

    def pack_mine(blk):
        rolled = pltpu.roll(blk, hd, axis=1)
        low, high = jnp.where(even, blk, rolled), jnp.where(even, rolled, blk)
        return jnp.where(lane32 < hd, low[0:hd // 2], high[hd // 2:hd])

    with scope('waitg'):
        tot = image_sum(0, gpre, grecv)
    with scope('soft'):
        gram = unpack(tot[0:hd // 2])
        sq_r = tot[hd // 2:hd // 2 + 1]
        sk_r = jnp.where(half1, tot[hd // 2 + 1:hd // 2 + 2], 1.0)
        sq_c = jnp.sum(jnp.where(diag, sq_r, 0.0), axis=1, keepdims=True)
        den = jnp.sqrt(sq_c) * jnp.sqrt(sk_r)
        cosine = gram / den
        temp = temp_ref[me]
        logits = jnp.where(half, temp * cosine, -jnp.inf)
        ex = jnp.exp(logits - jnp.max(logits, axis=1, keepdims=True))
        attn = ex / jnp.sum(ex, axis=1, keepdims=True)
        a_all[me] = pack_mine(attn).astype(BF16)
        to_all(0, a_all)
    with scope('chipd'):
        chip_sum(1, dsend, dpre, drecv)

    with scope('waitd'):
        d_a = unpack(image_sum(1, dpre, drecv))
    with scope('vjp'):
        inner = jnp.sum(d_a * attn, axis=1, keepdims=True)
        d_s = attn * (d_a - inner)
        d_cos = temp * d_s
        d_t = jnp.sum(jnp.sum(d_s * cosine, axis=1, keepdims=True), axis=0, keepdims=True)
        e_all[me] = pack_mine(d_cos / den).astype(BF16)
        ec = d_cos * cosine
        dsq_c = -0.5 * jnp.sum(ec, axis=1, keepdims=True) / sq_c
        dsk_r = -0.5 * jnp.sum(ec, axis=0, keepdims=True) / sk_r
        st_all[me, 0:1, :] = jnp.sum(jnp.where(diag, dsq_c, 0.0), axis=0, keepdims=True)
        st_all[me, 1:2, :] = dsk_r
        st_all[me, 2:3, :] = jnp.broadcast_to(d_t, (1, 2 * hd))
        to_all(1, e_all)
        to_all(2, st_all)

    def fill(bd, blocks):
        for h in range(heads):
            g, hh = h // hpg, h % hpg
            p = blocks[h].astype(F32)
            rolled = pltpu.roll(p, hd, axis=1)
            mine = (lane32 < hd) if h % 2 == 0 else (lane32 >= hd)
            top, bot = (p, rolled) if h % 2 == 0 else (rolled, p)
            c = slice((hh // 2) * 128, (hh // 2) * 128 + 128)
            bd[g, hh * hd:hh * hd + hd // 2, c] = jnp.where(mine, top, 0.0).astype(BF16)
            bd[g, hh * hd + hd // 2:hh * hd + hd, c] = jnp.where(mine, bot, 0.0).astype(BF16)

    hr = gw.shape[3] // 2
    lo, hi = slice(0, hr), slice(hr, 2 * hr)
    npc = gw.shape[0]

    def put_rows(pc, c, val, sem):
        gw[pc, c] = val.reshape(gw.shape[2:])
        remote(gw.at[pc, c, 1 - core], pre.at[pc, c], pre_s.at[0], pre_r.at[sem], partner)().start()

    def put(pc, val):
        gw[pc] = val.reshape(gw.shape[1:])
        remote(gw.at[pc, :, 1 - core], pre.at[pc], pre_s.at[0], pre_r.at[pc], partner)().start()

    def add_rows(pc, c):
        pre[pc, c] = pre[pc, c] + gw[pc, c, core]

    def send_far(pc):
        add_rows(pc, c_o)
        remote(pre.at[pc, c_o, lo], opp.at[pc, 0], opp_s.at[0], opp_r.at[pc], right)().start()
        remote(pre.at[pc, c_o, hi], opp.at[pc, 1], opp_s.at[0], opp_r.at[pc], left)().start()

    def send_near(pc):
        add_rows(pc, c_r)
        remote(pre.at[pc, c_r, hi], fin.at[pc, 0], fin_s.at[0], fin_r.at[pc], right)().start()
        add_rows(pc, c_l)
        remote(pre.at[pc, c_l, lo], fin.at[pc, 1], fin_s.at[0], fin_r.at[pc], left)().start()
        add_rows(pc, chip)

    def rs_first(pc):
        with scope('first%d' % pc):
            wait_bytes(pre.at[pc], pre_r.at[pc])
            send_far(pc)
            send_near(pc)

    def rs_relay(pc):
        with scope('relay%d' % pc):
            wait_bytes(opp.at[pc], opp_r.at[pc])
            pre[pc, c_r, lo] = pre[pc, c_r, lo] + opp[pc, 0]
            remote(pre.at[pc, c_r, lo], fin.at[pc, 2], fin_s.at[0], fin_r.at[pc], right)().start()
            pre[pc, c_l, hi] = pre[pc, c_l, hi] + opp[pc, 1]
            remote(pre.at[pc, c_l, hi], fin.at[pc, 3], fin_s.at[0], fin_r.at[pc], left)().start()

    def rs_final(pc):
        with scope('final%d' % pc):
            wait_bytes(fin.at[pc], fin_r.at[pc])
            gwst[pc, lo] = pre[pc, chip, lo] + fin[pc, 2] + fin[pc, 1]
            gwst[pc, hi] = pre[pc, chip, hi] + fin[pc, 0] + fin[pc, 3]

    def c3(i):
        t = tile_of(i)
        for g in range(ngrp):
            o_v[t, cols(g)] = mm(v_v[t, cols(g)], bd_a[g], NT).astype(BF16)

    def c4(i):
        t = tile_of(i)
        for g in range(ngrp):
            dqkv_v[t, 2 * width + 256 * g:2 * width + 256 * g + 256] = mm(do_v[t, cols(g)], bd_a[g]).astype(BF16)

    with scope('waita'):
        from_all(0, a_all)
    with scope('c3'):
        fill(bd_a, a_all)
        for i in range(nt):
            c3(i)
    rows_of = 2 * gw.shape[3]

    def gw_rows(c):
        return mm(o_v[:, pl.ds(pl.multiple_of(c * rows_of, rows_of), rows_of)], dy_v[...], TN)

    with scope('gw0a'):
        put_rows(0, c_o, gw_rows(c_o), 0)
    with scope('gw0b'):
        for c in (c_r, c_l, chip):
            put_rows(0, c, gw_rows(c), npc)
    with scope('far0'):
        wait_bytes(pre.at[0, 0], pre_r.at[0])
        send_far(0)

    with scope('c4'):
        for i in range(nt):
            c4(i)
    with scope('near0'):
        wait_bytes(pre.at[0, 1:nchip], pre_r.at[npc])
        send_near(0)

    def gw_piece(p, c):
        with scope('gw%d' % p):
            put(p, mm(u_v[...], dqkv_v[:, c * width:(c + 1) * width], TN))

    gw_piece(1, 2)

    with scope('waite'):
        from_all(1, e_all)
        from_all(2, st_all)
    with scope('fillg'):
        fill(bd_g, e_all)
        pair = [st_all[2 * j, 0:2, :] + st_all[2 * j + 1, 0:2, :] for j in range(heads // 2)]
        dsq2 = jnp.concatenate([2.0 * p[0:1] for p in pair], axis=1)
        dsk2 = jnp.concatenate([2.0 * p[1:2] for p in pair], axis=1)
        lane1 = lax.broadcasted_iota(jnp.int32, (1, 2 * hd), 1)
        gt = jnp.zeros((1, 2 * hd), F32)
        for h in range(heads):
            gt = jnp.where(lane1 == h, st_all[h, 2:3, :], gt)
        gtemp_ref[...] = gt[:, 0:heads]

    def c5(i):
        t = tile_of(i)
        for g in range(ngrp):
            c = cols(g)
            dqkv_v[t, c] = (mm(k_v[t, c], bd_g[g], NT) + q_v[t, c].astype(F32) * dsq2[:, c]).astype(BF16)

    def c6(i):
        t = tile_of(i)
        for g in range(ngrp):
            c = cols(g)
            dqkv_v[t, width + 256 * g:width + 256 * g + 256] = (
                mm(q_v[t, c], bd_g[g]) + k_v[t, c].astype(F32) * dsk2[:, c]).astype(BF16)

    with scope('c5a'):
        for i in range(nt // 2):
            c5(i)
    rs_relay(0)
    with scope('c5b'):
        for i in range(nt // 2, nt):
            c5(i)
    gw_piece(2, 0)
    rs_first(1)
    with scope('c6'):
        for i in range(nt):
            c6(i)
    gw_piece(3, 1)
    rs_first(2)

    def c7(i):
        t = tile_of(i)
        out_v[t, :] = (x_v[t, :].astype(F32) + mm(o_v[t, :], wout_v[...])).astype(BF16)

    def c8(i):
        t = tile_of(i)
        du = mm(dqkv_v[t, :], wqkv_v[...], NT)
        rstd = rstd_v[t, :]
        xhat = (x_v[t, :].astype(F32) - mean_v[t, :]) * rstd
        p = du * xhat
        accumulate(gbacc, 0, jnp.sum(p.reshape(tile // 8, 8, width), axis=0), i == 0)
        accumulate(gbacc, 1, jnp.sum(du.reshape(tile // 8, 8, width), axis=0), i == 0)
        dxh = du * gain_v[...]
        m1 = jnp.mean(dxh, axis=1, keepdims=True)
        m2 = jnp.mean(p * gain_v[...], axis=1, keepdims=True)
        dx = rstd * (dxh - m1 - xhat * m2)
        gtok_v[t, :] = (dy_v[t, :].astype(F32) + dx).astype(BF16)

    with scope('c8a'):
        c8(0)
    rs_relay(1)
    rs_first(3)
    with scope('c8b'):
        c8(1)
    with scope('c8c'):
        c8(2)
    rs_relay(2)
    with scope('c8d'):
        c8(3)
        for n in range(2):
            row_sum = jnp.sum(gbacc[n], axis=0, keepdims=True)
            for j in range(width // 128):
                gb_all[me, 4 * n + j:4 * n + j + 1, :] = row_sum[:, 128 * j:128 * j + 128]
        to_all(3, gb_all)
    with scope('c7a'):
        for i in range(nt // 2):
            c7(i)
    rs_relay(3)
    with scope('c7b'):
        for i in range(nt // 2, nt):
            c7(i)
    for pc in range(npc):
        rs_final(pc)

    with scope('gb'):
        from_all(3, gb_all)
        gb = gb_all[0]
        for d in range(1, ns):
            gb = gb + gb_all[d]
        for j in range(width // 128):
            ggain_ref[:, 128 * j:128 * j + 128] = gb[j:j + 1]
            gbias_ref[:, 128 * j:128 * j + 128] = gb[4 + j:5 + j]

    with scope('drain'):
        for kind, mid in enumerate((gpre, dpre)):
            wait_bytes(mid, own_s.at[kind, 0])
            wait_bytes(mid.at[1:nchip], own_s.at[kind, 1])
        for kind, buf in enumerate((a_all, e_all, st_all, gb_all)):
            wait_bytes(buf.at[0:ns - 1], all_s.at[kind])
        wait_bytes(pre, pre_s.at[0])
        wait_bytes(opp, opp_s.at[0])
        wait_bytes(fin, fin_s.at[0])


def writer(width, out_v, gtok_v, gwst, gg_v, gb_v, gt_v, out_hbm, gtok_hbm, gwqkv_hbm, gwout_hbm, gg_hbm, gb_hbm, gt_hbm, sem):
    copies = [(out_v, out_hbm), (gtok_v, gtok_hbm), (gg_v, gg_hbm), (gb_v, gb_hbm), (gt_v, gt_hbm), (gwst.at[0], gwout_hbm)]
    copies += [(gwst.at[pc], gwqkv_hbm.at[:, pl.ds(c * width, width)]) for pc, c in ((1, 2), (2, 0), (3, 1))]
    for i, (src, dst) in enumerate(copies):
        pltpu.make_async_copy(src, dst, sem.at[i]).start()
    for i, (src, dst) in enumerate(copies):
        pltpu.make_async_copy(src, dst, sem.at[i]).wait()


def solution(mesh):
    ns = mesh.shape['sp']
    row_spec = P(('dp', 'sp'), None)
    part_spec = P('dp')

    def local_step(x, dy, gain, bias, w_qkv, w_out, temp):
        rows, width = x.shape
        heads = temp.shape[0]
        hd = width // heads
        tile = 512
        nt = rows // tile
        share = width // ns
        nchip = ns // 2
        ngrp = width // 256
        hbm = pl.BlockSpec(memory_space=pl.ANY)
        vmem = pl.BlockSpec(memory_space=pltpu.VMEM)
        tok = lambda: pltpu.VMEM((rows, width), BF16)
        outs = pl.pallas_call(
            functools.partial(kernel, ns, rows, width, heads, tile),
            out_shape=[pltpu.VMEM((rows, width), BF16), pltpu.VMEM((rows, width), BF16),
                       pltpu.VMEM((4, share, width), F32), pltpu.VMEM((1, width), F32),
                       pltpu.VMEM((1, width), F32), pltpu.VMEM((1, heads), F32)],
            in_specs=[hbm] * 6 + [pl.BlockSpec(memory_space=pltpu.SMEM)],
            out_specs=[vmem] * 6,
            scratch_shapes=[
                tok(), tok(), pltpu.VMEM((1, width), F32), pltpu.VMEM((1, width), F32),
                pltpu.VMEM((width, 3 * width), BF16), pltpu.VMEM((width, width), BF16),
                tok(), tok(), tok(), tok(), tok(), tok(), pltpu.VMEM((rows, 3 * width), BF16),
                pltpu.VMEM((rows, 1), F32), pltpu.VMEM((rows, 1), F32),
                pltpu.VMEM((ngrp, 256, 256), F32), pltpu.VMEM((ngrp, 256, 256), F32),
                pltpu.VMEM((8, width), F32), pltpu.VMEM((8, width), F32),
                pltpu.VMEM((nchip, 2, hd // 2 + 8, 2 * hd), F32), pltpu.VMEM((nchip, hd // 2 + 8, 2 * hd), F32),
                pltpu.VMEM((nchip, hd // 2 + 8, 2 * hd), F32),
                pltpu.VMEM((nchip, 2, hd // 2, 2 * hd), F32), pltpu.VMEM((nchip, hd // 2, 2 * hd), F32),
                pltpu.VMEM((nchip, hd // 2, 2 * hd), F32),
                pltpu.VMEM((heads, hd // 2, 2 * hd), BF16), pltpu.VMEM((heads, hd // 2, 2 * hd), BF16),
                pltpu.VMEM((heads, 8, 2 * hd), F32),
                pltpu.VMEM((ngrp, 256, 256), BF16), pltpu.VMEM((ngrp, 256, 256), BF16),
                pltpu.VMEM((4, nchip, 2, share, width), F32), pltpu.VMEM((4, nchip, share, width), F32),
                pltpu.VMEM((4, 2, share // 2, width), F32), pltpu.VMEM((4, 4, share // 2, width), F32),
                pltpu.VMEM((2, 8, width), F32), pltpu.VMEM((ns, 8, 128), F32),
                pltpu.SemaphoreType.DMA((nt + 6,)),
                pltpu.SemaphoreType.DMA((2, 2)), pltpu.SemaphoreType.DMA((2, 2)),
                pltpu.SemaphoreType.DMA((4,)), pltpu.SemaphoreType.DMA((4,)),
                pltpu.SemaphoreType.DMA((1,)), pltpu.SemaphoreType.DMA((5,)),
                pltpu.SemaphoreType.DMA((1,)), pltpu.SemaphoreType.DMA((4,)),
                pltpu.SemaphoreType.DMA((1,)), pltpu.SemaphoreType.DMA((4,)),
            ],
            compiler_params=pltpu.CompilerParams(collective_id=0, has_side_effects=True,
                                                 vmem_limit_bytes=52 * 1024 * 1024),
        )(x, dy, gain.reshape(1, -1), bias.reshape(1, -1), w_qkv, w_out, temp)
        out, gtok, gwqkv, gwout, ggain, gbias, gtemp = pl.pallas_call(
            functools.partial(writer, width),
            out_shape=[jax.ShapeDtypeStruct((rows, width), BF16),
                       jax.ShapeDtypeStruct((rows, width), BF16),
                       jax.ShapeDtypeStruct((share, 3 * width), F32),
                       jax.ShapeDtypeStruct((share, width), F32),
                       jax.ShapeDtypeStruct((1, width), F32),
                       jax.ShapeDtypeStruct((1, width), F32),
                       jax.ShapeDtypeStruct((1, heads), F32)],
            in_specs=[vmem] * 6,
            out_specs=[hbm] * 7,
            scratch_shapes=[pltpu.SemaphoreType.DMA((9,))],
            compiler_params=pltpu.CompilerParams(vmem_limit_bytes=1024 * 1024),
        )(*outs)
        return out, gtok, gwqkv, gwout, ggain.reshape(-1), gbias.reshape(-1), gtemp.reshape(-1)

    full = P()
    return jax.shard_map(local_step, mesh=mesh,
                         in_specs=(row_spec, row_spec, full, full, full, full, full),
                         out_specs=(row_spec, row_spec, row_spec, row_spec, part_spec, part_spec, part_spec),
                         check_vma=False)
```

```python
import functools

import jax
import jax.numpy as jnp
from jax import lax
from jax.experimental import pallas as pl
from jax.experimental.pallas import tpu as pltpu
from jax.sharding import PartitionSpec as P

F32 = jnp.float32
BF16 = jnp.bfloat16
NN = (((1,), (0,)), ((), ()))
NT = (((1,), (1,)), ((), ()))
TN = (((0,), (0,)), ((), ()))
EPS = 1e-6


def mm(a, b, dims=NN):
    return lax.dot_general(a, b, dims, preferred_element_type=F32)


def kernel(ns, rows, width, heads, tile,
           x_hbm, dy_hbm, gain_hbm, bias_hbm, wqkv_hbm, wout_hbm, temp_hbm,
           out_v, gtok_v, gwst, ggain_ref, gbias_ref, gtemp_ref,
           x_v, dy_v, gain_v, bias_v, wqkv_v, wout_v, temp_ref,
           u_v, q_v, k_v, v_v, do_v, ut_v, vt_v, ot_v, dqkv_v, mean_v, rstd_v,
           gacc, dacc, sqacc, skacc, gsend, gpre, grecv, dsend, dpre, drecv, a_all, e_all, st_all, bd_a, bd_g,
           gw, pre, opp, fin, gbacc, gb_all,
           in_sem, own_s, own_r, all_s, all_r, pre_s, pre_r, opp_s, opp_r, fin_s, fin_r):
    me = lax.axis_index('sp')
    nt = rows // tile
    hd = width // heads
    core = lax.rem(me, 2)
    chip = me // 2
    nchip = ns // 2
    partner = me + 1 - 2 * core
    right = lax.rem(me + 2, ns)
    left = lax.rem(me + ns - 2, ns)
    c_r = lax.rem(chip + 1, nchip)
    c_l = lax.rem(chip + nchip - 1, nchip)
    c_o = lax.rem(chip + 2, nchip)
    scope = jax.named_scope

    def remote(src, dst, ssem, rsem, dev):
        return lambda: pltpu.make_async_remote_copy(src_ref=src, dst_ref=dst, send_sem=ssem, recv_sem=rsem,
                                                    device_id={'sp': dev}, device_id_type=pl.DeviceIdType.MESH)

    def wait_bytes(ref, sem):
        pltpu.make_async_copy(ref, ref, sem).wait()

    far_first = sorted(range(1, nchip), key=lambda s: -min(s, nchip - s))
    peers = [2 * lax.rem(chip + s, nchip) + c for s in far_first for c in (core, 1 - core)] + [partner]

    barrier = pltpu.get_barrier_semaphore()
    def ld(i, src, dst):
        return lambda: pltpu.make_async_copy(src, dst, in_sem.at[i])

    def tile_of(i):
        return slice(i * tile, (i + 1) * tile)

    def x_copy(i):
        return ld(i, x_hbm.at[tile_of(i)], x_v.at[tile_of(i)])

    dy_copy = ld(nt, dy_hbm, dy_v)
    gain_copy = ld(nt + 1, gain_hbm, gain_v)
    bias_copy = ld(nt + 2, bias_hbm, bias_v)
    wqk_copy = ld(nt + 3, wqkv_hbm.at[:, 0:2 * width], wqkv_v.at[:, 0:2 * width])
    wv_copy = ld(nt + 4, wqkv_hbm.at[:, 2 * width:3 * width], wqkv_v.at[:, 2 * width:3 * width])
    wout_copy = ld(nt + 5, wout_hbm, wout_v)
    temp_copy = ld(nt + 6, temp_hbm, temp_ref)
    x_copy(0)().start()
    gain_copy().start()
    bias_copy().start()
    wqk_copy().start()
    x_copy(1)().start()
    for dev in peers:
        pl.semaphore_signal(barrier, inc=1, device_id={'sp': dev}, device_id_type=pl.DeviceIdType.MESH)

    with scope('init'):
        bd_a[...] = jnp.zeros_like(bd_a)
        bd_g[...] = jnp.zeros_like(bd_g)

    ngrp = width // 256
    hpg = heads // ngrp

    def cols(g):
        return slice(256 * g, 256 * g + 256)

    def ln(t):
        x = x_v[t, :].astype(F32)
        mean = jnp.mean(x, axis=1, keepdims=True)
        cent = x - mean
        var = jnp.mean(cent * cent, axis=1, keepdims=True)
        rstd = lax.rsqrt(var + EPS)
        mean_v[t, :] = mean
        rstd_v[t, :] = rstd
        u_v[t, :] = (cent * rstd * gain_v[...] + bias_v[...]).astype(BF16)

    def accumulate(ref, idx, val, first):
        if first:
            ref[idx] = val
        else:
            ref[idx] += val

    def square_sum(ref, c, val, first):
        v32 = val.astype(F32)
        part = jnp.sum((v32 * v32).reshape(tile // 8, 8, 256), axis=0)
        ref[:, c] = part if first else ref[:, c] + part

    with scope('wx0'):
        x_copy(0)().wait()
        for i in range(2, nt):
            x_copy(i)().start()
        gain_copy().wait()
        bias_copy().wait()
    with scope('ln0'):
        ln(tile_of(0))
    with scope('ww'):
        wqk_copy().wait()
        x_copy(1)().wait()
        wv_copy().start()
        wout_copy().start()
        dy_copy().start()
        temp_copy().start()
    with scope('c1'):
        for i in range(nt):
            t = tile_of(i)
            if i == 1:
                for j in range(2, nt):
                    x_copy(j)().wait()
            if i + 1 < nt:
                ln(tile_of(i + 1))
            q = mm(u_v[t, :], wqkv_v[:, 0:width]).astype(BF16)
            q_v[t, :] = q
            k = mm(u_v[t, :], wqkv_v[:, width:2 * width]).astype(BF16)
            k_v[t, :] = k
            for g in range(ngrp):
                c = cols(g)
                square_sum(sqacc, c, q[:, c], i == 0)
                square_sum(skacc, c, k[:, c], i == 0)
                accumulate(gacc, g, mm(q[:, c], k[:, c], TN), i == 0)

    lane32 = lax.broadcasted_iota(jnp.int32, (hd // 2, 2 * hd), 1)

    def pack_block(blk, odd):
        top, bot = blk[0:hd // 2], blk[hd // 2:hd]
        if odd:
            top = pltpu.roll(top, hd, axis=1)
        else:
            bot = pltpu.roll(bot, hd, axis=1)
        return jnp.where(lane32 < hd, top, bot)

    def pack(acc, h):
        g, hh = h // hpg, h % hpg
        return pack_block(acc[g, hh * hd:hh * hd + hd, (hh // 2) * 128:(hh // 2) * 128 + 128], h % 2 == 1)

    with scope('packg'):
        sq_row = jnp.sum(sqacc[...], axis=0, keepdims=True)
        sk_row = jnp.sum(skacc[...], axis=0, keepdims=True)
        for h in range(heads):
            gsend[h // 2, h % 2, 0:hd // 2, :] = pack(gacc, h)
            c = slice((h // 2) * 128, (h // 2) * 128 + 128)
            gsend[h // 2, h % 2, hd // 2:hd // 2 + 1, :] = sq_row[:, c]
            gsend[h // 2, h % 2, hd // 2 + 1:hd // 2 + 2, :] = sk_row[:, c]

    def to_partner(kind, src, dst):
        return remote(src.at[:, 1 - core], dst, own_s.at[kind, 0], own_r.at[kind, 0], partner)

    def chip_sum(kind, src, mid, dst):
        wait_bytes(mid, own_r.at[kind, 0])
        n = mid.shape[1] if kind else hd // 2 + 2
        for c in range(nchip):
            mid[c, 0:n] = mid[c, 0:n] + src[c, core, 0:n]
        for s in far_first:
            c = lax.rem(chip + s, nchip)
            remote(mid.at[c], dst.at[s], own_s.at[kind, 1], own_r.at[kind, 1], 2 * c + core)().start()

    def image_sum(kind, mid, dst):
        n = mid.shape[1] if kind else hd // 2 + 2
        wait_bytes(dst.at[1:nchip], own_r.at[kind, 1])
        tot = mid[chip, 0:n]
        for s in range(1, nchip):
            tot = tot + dst[s, 0:n]
        return tot

    def to_all(kind, buf):
        for dev in peers:
            remote(buf.at[me], buf.at[me], all_s.at[kind], all_r.at[kind], dev)().start()

    def from_all(kind, buf):
        wait_bytes(buf.at[0:ns - 1], all_r.at[kind])

    with scope('sendg'):
        pl.semaphore_wait(barrier, ns - 1)
        to_partner(0, gsend, gpre)().start()

    def c2(i):
        t = tile_of(i)
        v = mm(u_v[t, :], wqkv_v[:, 2 * width:3 * width]).astype(BF16)
        v_v[t, :] = v
        do = mm(dy_v[t, :], wout_v[...], NT).astype(BF16)
        do_v[t, :] = do
        for g in range(ngrp):
            accumulate(dacc, g, mm(do[:, cols(g)], v[:, cols(g)], TN), i == 0)

    with scope('c2a'):
        wv_copy().wait()
        wout_copy().wait()
        dy_copy().wait()
        c2(0)
    with scope('chipg'):
        chip_sum(0, gsend, gpre, grecv)
    with scope('c2b'):
        for i in range(1, nt):
            c2(i)
    with scope('sendd'):
        for h in range(heads):
            dsend[h // 2, h % 2] = pack(dacc, h)
        to_partner(1, dsend, dpre)().start()

    row = lax.broadcasted_iota(jnp.int32, (hd, 2 * hd), 0)
    lanep = lax.broadcasted_iota(jnp.int32, (hd, 2 * hd), 1) - hd * core
    half = (lanep >= 0) & (lanep < hd)
    diag = lanep == row
    half1 = half[0:1]
    even = core == 0

    def unpack(p):
        rolled = pltpu.roll(p, hd, axis=1)
        full = jnp.concatenate([jnp.where(even, p, rolled), jnp.where(even, rolled, p)], axis=0)
        return jnp.where(half, full, 0.0)

    def pack_mine(blk):
        rolled = pltpu.roll(blk, hd, axis=1)
        low, high = jnp.where(even, blk, rolled), jnp.where(even, rolled, blk)
        return jnp.where(lane32 < hd, low[0:hd // 2], high[hd // 2:hd])

    with scope('waitg'):
        tot = image_sum(0, gpre, grecv)
    with scope('soft'):
        gram = unpack(tot[0:hd // 2])
        sq_r = tot[hd // 2:hd // 2 + 1]
        sk_r = jnp.where(half1, tot[hd // 2 + 1:hd // 2 + 2], 1.0)
        sq_c = jnp.sum(jnp.where(diag, sq_r, 0.0), axis=1, keepdims=True)
        den = jnp.sqrt(sq_c) * jnp.sqrt(sk_r)
        cosine = gram / den
        temp_copy().wait()
        temp = temp_ref[me]
        logits = jnp.where(half, temp * cosine, -jnp.inf)
        ex = jnp.exp(logits - jnp.max(logits, axis=1, keepdims=True))
        attn = ex / jnp.sum(ex, axis=1, keepdims=True)
        a_all[me] = pack_mine(attn).astype(BF16)
        to_all(0, a_all)
    with scope('chipd'):
        chip_sum(1, dsend, dpre, drecv)

    def head_vjp():
        with scope('waitd'):
            d_a = unpack(image_sum(1, dpre, drecv))
        with scope('vjp'):
            inner = jnp.sum(d_a * attn, axis=1, keepdims=True)
            d_s = attn * (d_a - inner)
            d_cos = temp * d_s
            d_t = jnp.sum(jnp.sum(d_s * cosine, axis=1, keepdims=True), axis=0, keepdims=True)
            e_all[me] = pack_mine(d_cos / den).astype(BF16)
            ec = d_cos * cosine
            dsq_c = -0.5 * jnp.sum(ec, axis=1, keepdims=True) / sq_c
            dsk_r = -0.5 * jnp.sum(ec, axis=0, keepdims=True) / sk_r
            st_all[me, 0:1, :] = jnp.sum(jnp.where(diag, dsq_c, 0.0), axis=0, keepdims=True)
            st_all[me, 1:2, :] = dsk_r
            st_all[me, 2:3, :] = jnp.broadcast_to(d_t, (1, 2 * hd))
            to_all(1, e_all)
            to_all(2, st_all)

    def fill(bd, blocks):
        for h in range(heads):
            g, hh = h // hpg, h % hpg
            p = blocks[h].astype(F32)
            rolled = pltpu.roll(p, hd, axis=1)
            mine = (lane32 < hd) if h % 2 == 0 else (lane32 >= hd)
            top, bot = (p, rolled) if h % 2 == 0 else (rolled, p)
            c = slice((hh // 2) * 128, (hh // 2) * 128 + 128)
            bd[g, hh * hd:hh * hd + hd // 2, c] = jnp.where(mine, top, 0.0).astype(BF16)
            bd[g, hh * hd + hd // 2:hh * hd + hd, c] = jnp.where(mine, bot, 0.0).astype(BF16)

    hr = gw.shape[3] // 2
    lo, hi = slice(0, hr), slice(hr, 2 * hr)
    npc = gw.shape[0]

    nhalf = nchip // 2
    half_rows = nhalf * 2 * gw.shape[3]
    near_half = lax.rem(c_o // nhalf + 1, 2)
    far_half = 1 - near_half

    def put(pc, n, lhs, rhs):
        first = (far_half, near_half)[n]
        val = mm(lhs[pl.ds(pl.multiple_of(first * half_rows, half_rows), half_rows), :], rhs)
        c = pl.ds(first * nhalf, nhalf)
        gw[pc, c] = val.reshape(nhalf, *gw.shape[2:])
        remote(gw.at[pc, c, 1 - core], pre.at[pc, c], pre_s.at[0], pre_r.at[pc, n], partner)().start()

    def add_half(pc, n):
        wait_bytes(pre.at[pc, 0:nhalf], pre_r.at[pc, n])
        c = pl.ds((far_half, near_half)[n] * nhalf, nhalf)
        pre[pc, c] = pre[pc, c] + gw[pc, c, core]

    def rs_far(pc):
        with scope('far%d' % pc):
            add_half(pc, 0)
            remote(pre.at[pc, c_o, lo], opp.at[pc, 0], opp_s.at[0], opp_r.at[pc], right)().start()
            remote(pre.at[pc, c_o, hi], opp.at[pc, 1], opp_s.at[0], opp_r.at[pc], left)().start()

    def rs_near(pc):
        with scope('near%d' % pc):
            add_half(pc, 1)
            remote(pre.at[pc, c_r, hi], fin.at[pc, 0], fin_s.at[0], fin_r.at[pc], right)().start()
            remote(pre.at[pc, c_l, lo], fin.at[pc, 1], fin_s.at[0], fin_r.at[pc], left)().start()

    def rs_relay(pc):
        with scope('relay%d' % pc):
            wait_bytes(opp.at[pc], opp_r.at[pc])
            pre[pc, c_r, lo] = pre[pc, c_r, lo] + opp[pc, 0]
            remote(pre.at[pc, c_r, lo], fin.at[pc, 2], fin_s.at[0], fin_r.at[pc], right)().start()
            pre[pc, c_l, hi] = pre[pc, c_l, hi] + opp[pc, 1]
            remote(pre.at[pc, c_l, hi], fin.at[pc, 3], fin_s.at[0], fin_r.at[pc], left)().start()

    def rs_final(pc):
        with scope('final%d' % pc):
            wait_bytes(fin.at[pc], fin_r.at[pc])
            gwst[pc, lo] = pre[pc, chip, lo] + fin[pc, 2] + fin[pc, 1]
            gwst[pc, hi] = pre[pc, chip, hi] + fin[pc, 0] + fin[pc, 3]

    def c3(g):
        with scope('c3'):
            c = pl.ds(pl.multiple_of(g * 256, 256), 256)
            for i in range(nt):
                t = tile_of(i)
                ot_v[c, t] = mm(bd_a[g], vt_v[c, t]).astype(BF16)

    def c4(i):
        t = tile_of(i)
        for g in range(ngrp):
            dqkv_v[t, 2 * width + 256 * g:2 * width + 256 * g + 256] = mm(do_v[t, cols(g)], bd_a[g]).astype(BF16)

    with scope('transpose'):
        for i in range(nt):
            t = tile_of(i)
            ut_v[:, t] = u_v[t, :].T
            vt_v[:, t] = v_v[t, :].T
    with scope('waita'):
        from_all(0, a_all)
    with scope('filla'):
        fill(bd_a, a_all)
    def gw_piece(pc, n, lhs, rhs):
        with scope('gw%d%s' % (pc, 'ab'[n])):
            put(pc, n, lhs, rhs)

    def dcols(c):
        return dqkv_v[:, c * width:(c + 1) * width]

    def c7(i):
        t = tile_of(i)
        out_v[t, :] = (x_v[t, :].astype(F32) + mm(ot_v[:, t], wout_v[...], TN)).astype(BF16)

    c3(far_half)
    gw_piece(0, 0, ot_v, dy_v[...])
    c3(near_half)
    gw_piece(0, 1, ot_v, dy_v[...])
    head_vjp()
    rs_far(0)

    with scope('c4'):
        for i in range(nt):
            c4(i)
    rs_near(0)
    gw_piece(1, 0, ut_v, dcols(2))
    gw_piece(1, 1, ut_v, dcols(2))
    with scope('c7a'):
        for i in range(nt // 2):
            c7(i)
    rs_far(1)
    with scope('c7b'):
        for i in range(nt // 2, nt):
            c7(i)
    rs_near(1)

    with scope('waite'):
        from_all(1, e_all)
        from_all(2, st_all)
    with scope('fillg'):
        fill(bd_g, e_all)
        pair = [st_all[2 * j, 0:2, :] + st_all[2 * j + 1, 0:2, :] for j in range(heads // 2)]
        dsq2 = jnp.concatenate([2.0 * p[0:1] for p in pair], axis=1)
        dsk2 = jnp.concatenate([2.0 * p[1:2] for p in pair], axis=1)
        lane1 = lax.broadcasted_iota(jnp.int32, (1, 2 * hd), 1)
        gt = jnp.zeros((1, 2 * hd), F32)
        for h in range(heads):
            gt = jnp.where(lane1 == h, st_all[h, 2:3, :], gt)
        gtemp_ref[...] = gt[:, 0:heads]

    def c5(i):
        t = tile_of(i)
        for g in range(ngrp):
            c = cols(g)
            dqkv_v[t, c] = (mm(k_v[t, c], bd_g[g], NT) + q_v[t, c].astype(F32) * dsq2[:, c]).astype(BF16)

    def c6(i):
        t = tile_of(i)
        for g in range(ngrp):
            c = cols(g)
            dqkv_v[t, width + 256 * g:width + 256 * g + 256] = (
                mm(q_v[t, c], bd_g[g]) + k_v[t, c].astype(F32) * dsk2[:, c]).astype(BF16)

    with scope('c5'):
        for i in range(nt):
            c5(i)
    rs_relay(0)
    gw_piece(2, 0, ut_v, dcols(0))
    gw_piece(2, 1, ut_v, dcols(0))
    with scope('c6'):
        for i in range(nt):
            c6(i)
    rs_far(2)
    gw_piece(3, 0, ut_v, dcols(1))
    rs_near(2)
    gw_piece(3, 1, ut_v, dcols(1))
    rs_relay(1)

    def c8(i):
        t = tile_of(i)
        du = mm(dqkv_v[t, :], wqkv_v[...], NT)
        rstd = rstd_v[t, :]
        xhat = (x_v[t, :].astype(F32) - mean_v[t, :]) * rstd
        p = du * xhat
        accumulate(gbacc, 0, jnp.sum(p.reshape(tile // 8, 8, width), axis=0), i == 0)
        accumulate(gbacc, 1, jnp.sum(du.reshape(tile // 8, 8, width), axis=0), i == 0)
        dxh = du * gain_v[...]
        m1 = jnp.mean(dxh, axis=1, keepdims=True)
        m2 = jnp.mean(p * gain_v[...], axis=1, keepdims=True)
        dx = rstd * (dxh - m1 - xhat * m2)
        gtok_v[t, :] = (dy_v[t, :].astype(F32) + dx).astype(BF16)

    with scope('c8a'):
        c8(0)
    rs_far(3)
    rs_near(3)
    with scope('c8b'):
        c8(1)
    rs_relay(2)
    with scope('c8c'):
        c8(2)
    with scope('c8d'):
        c8(3)
        for n in range(2):
            row_sum = jnp.sum(gbacc[n], axis=0, keepdims=True)
            for j in range(width // 128):
                gb_all[me, 4 * n + j:4 * n + j + 1, :] = row_sum[:, 128 * j:128 * j + 128]
        to_all(3, gb_all)
    rs_relay(3)
    for pc in range(npc):
        rs_final(pc)

    with scope('gb'):
        from_all(3, gb_all)
        gb = gb_all[0]
        for d in range(1, ns):
            gb = gb + gb_all[d]
        for j in range(width // 128):
            ggain_ref[:, 128 * j:128 * j + 128] = gb[j:j + 1]
            gbias_ref[:, 128 * j:128 * j + 128] = gb[4 + j:5 + j]

    with scope('drain'):
        for kind, mid in enumerate((gpre, dpre)):
            wait_bytes(mid, own_s.at[kind, 0])
            wait_bytes(mid.at[1:nchip], own_s.at[kind, 1])
        for kind, buf in enumerate((a_all, e_all, st_all, gb_all)):
            wait_bytes(buf.at[0:ns - 1], all_s.at[kind])
        wait_bytes(pre, pre_s.at[0])
        wait_bytes(opp, opp_s.at[0])
        wait_bytes(fin, fin_s.at[0])


def writer(width, out_v, gtok_v, gwst, gg_v, gb_v, gt_v, out_hbm, gtok_hbm, gwqkv_hbm, gwout_hbm, gg_hbm, gb_hbm, gt_hbm, sem):
    copies = [(gg_v, gg_hbm), (gb_v, gb_hbm), (gt_v, gt_hbm), (gwst.at[0], gwout_hbm)]
    copies += [(gwst.at[pc], gwqkv_hbm.at[:, pl.ds(c * width, width)]) for pc, c in ((1, 2), (2, 0), (3, 1))]
    copies += [(out_v, out_hbm), (gtok_v, gtok_hbm)]
    for i, (src, dst) in enumerate(copies):
        pltpu.make_async_copy(src, dst, sem.at[i]).start()
    for i, (src, dst) in enumerate(copies):
        pltpu.make_async_copy(src, dst, sem.at[i]).wait()


def solution(mesh):
    ns = mesh.shape['sp']
    row_spec = P(('dp', 'sp'), None)
    part_spec = P('dp')

    def local_step(x, dy, gain, bias, w_qkv, w_out, temp):
        rows, width = x.shape
        heads = temp.shape[0]
        hd = width // heads
        tile = 512
        nt = rows // tile
        share = width // ns
        nchip = ns // 2
        ngrp = width // 256
        hbm = pl.BlockSpec(memory_space=pl.ANY)
        vmem = pl.BlockSpec(memory_space=pltpu.VMEM)
        tok = lambda: pltpu.VMEM((rows, width), BF16)
        tok_t = lambda: pltpu.VMEM((width, rows), BF16)
        outs = pl.pallas_call(
            functools.partial(kernel, ns, rows, width, heads, tile),
            out_shape=[pltpu.VMEM((rows, width), BF16), pltpu.VMEM((rows, width), BF16),
                       pltpu.VMEM((4, share, width), F32), pltpu.VMEM((1, width), F32),
                       pltpu.VMEM((1, width), F32), pltpu.VMEM((1, heads), F32)],
            in_specs=[hbm] * 7,
            out_specs=[vmem] * 6,
            scratch_shapes=[
                tok(), tok(), pltpu.VMEM((1, width), F32), pltpu.VMEM((1, width), F32),
                pltpu.VMEM((width, 3 * width), BF16), pltpu.VMEM((width, width), BF16), pltpu.SMEM((heads,), F32),
                tok(), tok(), tok(), tok(), tok(), tok_t(), tok_t(), tok_t(), pltpu.VMEM((rows, 3 * width), BF16),
                pltpu.VMEM((rows, 1), F32), pltpu.VMEM((rows, 1), F32),
                pltpu.VMEM((ngrp, 256, 256), F32), pltpu.VMEM((ngrp, 256, 256), F32),
                pltpu.VMEM((8, width), F32), pltpu.VMEM((8, width), F32),
                pltpu.VMEM((nchip, 2, hd // 2 + 8, 2 * hd), F32), pltpu.VMEM((nchip, hd // 2 + 8, 2 * hd), F32),
                pltpu.VMEM((nchip, hd // 2 + 8, 2 * hd), F32),
                pltpu.VMEM((nchip, 2, hd // 2, 2 * hd), F32), pltpu.VMEM((nchip, hd // 2, 2 * hd), F32),
                pltpu.VMEM((nchip, hd // 2, 2 * hd), F32),
                pltpu.VMEM((heads, hd // 2, 2 * hd), BF16), pltpu.VMEM((heads, hd // 2, 2 * hd), BF16),
                pltpu.VMEM((heads, 8, 2 * hd), F32),
                pltpu.VMEM((ngrp, 256, 256), BF16), pltpu.VMEM((ngrp, 256, 256), BF16),
                pltpu.VMEM((4, nchip, 2, share, width), F32), pltpu.VMEM((4, nchip, share, width), F32),
                pltpu.VMEM((4, 2, share // 2, width), F32), pltpu.VMEM((4, 4, share // 2, width), F32),
                pltpu.VMEM((2, 8, width), F32), pltpu.VMEM((ns, 8, 128), F32),
                pltpu.SemaphoreType.DMA((nt + 7,)),
                pltpu.SemaphoreType.DMA((2, 2)), pltpu.SemaphoreType.DMA((2, 2)),
                pltpu.SemaphoreType.DMA((4,)), pltpu.SemaphoreType.DMA((4,)),
                pltpu.SemaphoreType.DMA((1,)), pltpu.SemaphoreType.DMA((4, 2)),
                pltpu.SemaphoreType.DMA((1,)), pltpu.SemaphoreType.DMA((4,)),
                pltpu.SemaphoreType.DMA((1,)), pltpu.SemaphoreType.DMA((4,)),
            ],
            compiler_params=pltpu.CompilerParams(collective_id=0, has_side_effects=True,
                                                 vmem_limit_bytes=52 * 1024 * 1024),
        )(x, dy, gain.reshape(1, -1), bias.reshape(1, -1), w_qkv, w_out, temp)
        out, gtok, gwqkv, gwout, ggain, gbias, gtemp = pl.pallas_call(
            functools.partial(writer, width),
            out_shape=[jax.ShapeDtypeStruct((rows, width), BF16),
                       jax.ShapeDtypeStruct((rows, width), BF16),
                       jax.ShapeDtypeStruct((share, 3 * width), F32),
                       jax.ShapeDtypeStruct((share, width), F32),
                       jax.ShapeDtypeStruct((1, width), F32),
                       jax.ShapeDtypeStruct((1, width), F32),
                       jax.ShapeDtypeStruct((1, heads), F32)],
            in_specs=[vmem] * 6,
            out_specs=[hbm] * 7,
            scratch_shapes=[pltpu.SemaphoreType.DMA((9,))],
            compiler_params=pltpu.CompilerParams(vmem_limit_bytes=1024 * 1024),
        )(*outs)
        return out, gtok, gwqkv, gwout, ggain.reshape(-1), gbias.reshape(-1), gtemp.reshape(-1)

    full = P()
    return jax.shard_map(local_step, mesh=mesh,
                         in_specs=(row_spec, row_spec, full, full, full, full, full),
                         out_specs=(row_spec, row_spec, row_spec, row_spec, part_spec, part_spec, part_spec),
                         check_vma=False)
```

```python
import functools

import jax
import jax.numpy as jnp
from jax import lax
from jax.experimental import pallas as pl
from jax.experimental.pallas import tpu as pltpu
from jax.sharding import PartitionSpec as P

F32 = jnp.float32
BF16 = jnp.bfloat16
NN = (((1,), (0,)), ((), ()))
NT = (((1,), (1,)), ((), ()))
TN = (((0,), (0,)), ((), ()))
EPS = 1e-6


def mm(a, b, dims=NN):
    return lax.dot_general(a, b, dims, preferred_element_type=F32)


def kernel(ns, rows, width, heads, tile,
           x_hbm, dy_hbm, gain_hbm, bias_hbm, wqkv_hbm, wout_hbm, temp_hbm,
           out_v, gtok_v, gwst, ggain_ref, gbias_ref, gtemp_ref,
           x_v, dy_v, gain_v, bias_v, wqkv_v, wout_v, temp_ref,
           u_v, q_v, k_v, v_v, do_v, ut_v, vt_v, ot_v, dqkv_v, mean_v, rstd_v,
           gacc, dacc, sqacc, skacc, gsend, gpre, grecv, dsend, dpre, drecv, a_all, e_all, st_all, bd_a, bd_g,
           gw, pre, opp, fin, gbacc, gb_all,
           in_sem, own_s, own_r, all_s, all_r, pre_s, pre_r, opp_s, opp_r, fin_s, fin_r):
    me = lax.axis_index('sp')
    nt = rows // tile
    hd = width // heads
    core = lax.rem(me, 2)
    chip = me // 2
    nchip = ns // 2
    partner = me + 1 - 2 * core
    right = lax.rem(me + 2, ns)
    left = lax.rem(me + ns - 2, ns)
    c_r = lax.rem(chip + 1, nchip)
    c_l = lax.rem(chip + nchip - 1, nchip)
    c_o = lax.rem(chip + 2, nchip)
    scope = jax.named_scope

    def remote(src, dst, ssem, rsem, dev):
        return lambda: pltpu.make_async_remote_copy(src_ref=src, dst_ref=dst, send_sem=ssem, recv_sem=rsem,
                                                    device_id={'sp': dev}, device_id_type=pl.DeviceIdType.MESH)

    def wait_bytes(ref, sem):
        pltpu.make_async_copy(ref, ref, sem).wait()

    far_first = sorted(range(1, nchip), key=lambda s: -min(s, nchip - s))
    peers = [2 * lax.rem(chip + s, nchip) + c for s in far_first for c in (core, 1 - core)] + [partner]

    barrier = pltpu.get_barrier_semaphore()
    def ld(i, src, dst):
        return lambda: pltpu.make_async_copy(src, dst, in_sem.at[i])

    def tile_of(i):
        return slice(i * tile, (i + 1) * tile)

    def x_copy(i):
        return ld(i, x_hbm.at[tile_of(i)], x_v.at[tile_of(i)])

    dy_copy = ld(nt, dy_hbm, dy_v)
    gain_copy = ld(nt + 1, gain_hbm, gain_v)
    bias_copy = ld(nt + 2, bias_hbm, bias_v)
    wq_copy = ld(nt + 3, wqkv_hbm.at[:, 0:width], wqkv_v.at[:, 0:width])
    wk_copy = ld(nt + 7, wqkv_hbm.at[:, width:2 * width], wqkv_v.at[:, width:2 * width])
    wv_copy = ld(nt + 4, wqkv_hbm.at[:, 2 * width:3 * width], wqkv_v.at[:, 2 * width:3 * width])
    wout_copy = ld(nt + 5, wout_hbm, wout_v)
    temp_copy = ld(nt + 6, temp_hbm, temp_ref)
    head = slice(0, tile // 2)
    rest = slice(tile // 2, tile)
    x_head = ld(0, x_hbm.at[head], x_v.at[head])
    x_rest = ld(nt + 8, x_hbm.at[rest], x_v.at[rest])
    x_head().start()
    gain_copy().start()
    bias_copy().start()
    wq_copy().start()
    x_rest().start()
    wk_copy().start()
    x_copy(1)().start()
    for dev in peers:
        pl.semaphore_signal(barrier, inc=1, device_id={'sp': dev}, device_id_type=pl.DeviceIdType.MESH)

    with scope('init'):
        bd_a[...] = jnp.zeros_like(bd_a)
        bd_g[...] = jnp.zeros_like(bd_g)

    ngrp = width // 256
    hpg = heads // ngrp

    def cols(g):
        return slice(256 * g, 256 * g + 256)

    def ln(t):
        x = x_v[t, :].astype(F32)
        mean = jnp.mean(x, axis=1, keepdims=True)
        cent = x - mean
        var = jnp.mean(cent * cent, axis=1, keepdims=True)
        rstd = lax.rsqrt(var + EPS)
        mean_v[t, :] = mean
        rstd_v[t, :] = rstd
        u_v[t, :] = (cent * rstd * gain_v[...] + bias_v[...]).astype(BF16)

    def accumulate(ref, idx, val, first):
        if first:
            ref[idx] = val
        else:
            ref[idx] += val

    def square_sum(ref, c, val, first):
        v32 = val.astype(F32)
        part = jnp.sum((v32 * v32).reshape(tile // 8, 8, 256), axis=0)
        ref[:, c] = part if first else ref[:, c] + part

    with scope('wx0'):
        x_head().wait()
        for i in range(2, nt):
            x_copy(i)().start()
        gain_copy().wait()
        bias_copy().wait()
    with scope('ln0'):
        ln(head)
    with scope('ww'):
        wq_copy().wait()
        x_rest().wait()
    with scope('c1h'):
        ln(rest)
        q_v[head, :] = mm(u_v[head, :], wqkv_v[:, 0:width]).astype(BF16)
    with scope('ww2'):
        wk_copy().wait()
        x_copy(1)().wait()
        wv_copy().start()
        wout_copy().start()
        dy_copy().start()
        temp_copy().start()
    with scope('c1'):
        for i in range(nt):
            t = tile_of(i)
            if i == 1:
                for j in range(2, nt):
                    x_copy(j)().wait()
            if i + 1 < nt:
                ln(tile_of(i + 1))
            if i == 0:
                q_v[rest, :] = mm(u_v[rest, :], wqkv_v[:, 0:width]).astype(BF16)
                q = q_v[t, :]
            else:
                q = mm(u_v[t, :], wqkv_v[:, 0:width]).astype(BF16)
                q_v[t, :] = q
            k = mm(u_v[t, :], wqkv_v[:, width:2 * width]).astype(BF16)
            k_v[t, :] = k
            for g in range(ngrp):
                c = cols(g)
                square_sum(sqacc, c, q[:, c], i == 0)
                square_sum(skacc, c, k[:, c], i == 0)
                accumulate(gacc, g, mm(q[:, c], k[:, c], TN), i == 0)

    lane32 = lax.broadcasted_iota(jnp.int32, (hd // 2, 2 * hd), 1)

    def pack_block(blk, odd):
        top, bot = blk[0:hd // 2], blk[hd // 2:hd]
        if odd:
            top = pltpu.roll(top, hd, axis=1)
        else:
            bot = pltpu.roll(bot, hd, axis=1)
        return jnp.where(lane32 < hd, top, bot)

    def pack(acc, h):
        g, hh = h // hpg, h % hpg
        return pack_block(acc[g, hh * hd:hh * hd + hd, (hh // 2) * 128:(hh // 2) * 128 + 128], h % 2 == 1)

    with scope('packg'):
        sq_row = jnp.sum(sqacc[...], axis=0, keepdims=True)
        sk_row = jnp.sum(skacc[...], axis=0, keepdims=True)
        for h in range(heads):
            gsend[h // 2, h % 2, 0:hd // 2, :] = pack(gacc, h)
            c = slice((h // 2) * 128, (h // 2) * 128 + 128)
            gsend[h // 2, h % 2, hd // 2:hd // 2 + 1, :] = sq_row[:, c]
            gsend[h // 2, h % 2, hd // 2 + 1:hd // 2 + 2, :] = sk_row[:, c]

    def to_partner(kind, src, dst):
        return remote(src.at[:, 1 - core], dst, own_s.at[kind, 0], own_r.at[kind, 0], partner)

    def chip_sum(kind, src, mid, dst):
        wait_bytes(mid, own_r.at[kind, 0])
        n = mid.shape[1] if kind else hd // 2 + 2
        for c in range(nchip):
            mid[c, 0:n] = mid[c, 0:n] + src[c, core, 0:n]
        for s in far_first:
            c = lax.rem(chip + s, nchip)
            remote(mid.at[c], dst.at[s], own_s.at[kind, 1], own_r.at[kind, 1], 2 * c + core)().start()

    def image_sum(kind, mid, dst):
        n = mid.shape[1] if kind else hd // 2 + 2
        wait_bytes(dst.at[1:nchip], own_r.at[kind, 1])
        tot = mid[chip, 0:n]
        for s in range(1, nchip):
            tot = tot + dst[s, 0:n]
        return tot

    def to_all(kind, buf):
        for dev in peers:
            remote(buf.at[me], buf.at[me], all_s.at[kind], all_r.at[kind], dev)().start()

    def from_all(kind, buf):
        wait_bytes(buf.at[0:ns - 1], all_r.at[kind])

    with scope('sendg'):
        pl.semaphore_wait(barrier, ns - 1)
        to_partner(0, gsend, gpre)().start()

    def v_rows(t):
        v_v[t, :] = mm(u_v[t, :], wqkv_v[:, 2 * width:3 * width]).astype(BF16)

    cut = rows - tile
    with scope('c2a'):
        wv_copy().wait()
        v_rows(slice(0, cut))
    with scope('chipg'):
        chip_sum(0, gsend, gpre, grecv)
    with scope('c2b'):
        wout_copy().wait()
        dy_copy().wait()
        v_rows(slice(cut, rows))
        for i in range(nt):
            t = tile_of(i)
            do_v[t, :] = mm(dy_v[t, :], wout_v[...], NT).astype(BF16)
        for g in range(ngrp):
            dacc[g] = mm(do_v[:, cols(g)], v_v[:, cols(g)], TN)
    with scope('sendd'):
        for h in range(heads):
            dsend[h // 2, h % 2] = pack(dacc, h)
        to_partner(1, dsend, dpre)().start()

    row = lax.broadcasted_iota(jnp.int32, (hd, 2 * hd), 0)
    lanep = lax.broadcasted_iota(jnp.int32, (hd, 2 * hd), 1) - hd * core
    half = (lanep >= 0) & (lanep < hd)
    diag = lanep == row
    half1 = half[0:1]
    even = core == 0

    def unpack(p):
        rolled = pltpu.roll(p, hd, axis=1)
        full = jnp.concatenate([jnp.where(even, p, rolled), jnp.where(even, rolled, p)], axis=0)
        return jnp.where(half, full, 0.0)

    def pack_mine(blk):
        rolled = pltpu.roll(blk, hd, axis=1)
        low, high = jnp.where(even, blk, rolled), jnp.where(even, rolled, blk)
        return jnp.where(lane32 < hd, low[0:hd // 2], high[hd // 2:hd])

    with scope('waitg'):
        tot = image_sum(0, gpre, grecv)
    with scope('soft'):
        gram = unpack(tot[0:hd // 2])
        sq_r = tot[hd // 2:hd // 2 + 1]
        sk_r = jnp.where(half1, tot[hd // 2 + 1:hd // 2 + 2], 1.0)
        sq_c = jnp.sum(jnp.where(diag, sq_r, 0.0), axis=1, keepdims=True)
        den = jnp.sqrt(sq_c) * jnp.sqrt(sk_r)
        cosine = gram / den
        temp_copy().wait()
        temp = temp_ref[me]
        logits = jnp.where(half, temp * cosine, -jnp.inf)
        ex = jnp.exp(logits - jnp.max(logits, axis=1, keepdims=True))
        attn = ex / jnp.sum(ex, axis=1, keepdims=True)
        a_all[me] = pack_mine(attn).astype(BF16)
        to_all(0, a_all)
    with scope('chipd'):
        chip_sum(1, dsend, dpre, drecv)

    def vjp_gram():
        d_a = unpack(image_sum(1, dpre, drecv))
        inner = jnp.sum(d_a * attn, axis=1, keepdims=True)
        d_s = attn * (d_a - inner)
        d_cos = temp * d_s
        e_all[me] = pack_mine(d_cos / den).astype(BF16)
        return d_s, d_cos * cosine

    def vjp_rest(d_s, ec):
        d_t = jnp.sum(jnp.sum(d_s * cosine, axis=1, keepdims=True), axis=0, keepdims=True)
        dsq_c = -0.5 * jnp.sum(ec, axis=1, keepdims=True) / sq_c
        dsk_r = -0.5 * jnp.sum(ec, axis=0, keepdims=True) / sk_r
        st_all[me, 0:1, :] = jnp.sum(jnp.where(diag, dsq_c, 0.0), axis=0, keepdims=True)
        st_all[me, 1:2, :] = dsk_r
        st_all[me, 2:3, :] = jnp.broadcast_to(d_t, (1, 2 * hd))

    def fill(bd, blocks):
        for h in range(heads):
            g, hh = h // hpg, h % hpg
            p = blocks[h].astype(F32)
            rolled = pltpu.roll(p, hd, axis=1)
            mine = (lane32 < hd) if h % 2 == 0 else (lane32 >= hd)
            top, bot = (p, rolled) if h % 2 == 0 else (rolled, p)
            c = slice((hh // 2) * 128, (hh // 2) * 128 + 128)
            bd[g, hh * hd:hh * hd + hd // 2, c] = jnp.where(mine, top, 0.0).astype(BF16)
            bd[g, hh * hd + hd // 2:hh * hd + hd, c] = jnp.where(mine, bot, 0.0).astype(BF16)

    hr = gw.shape[3] // 2
    lo, hi = slice(0, hr), slice(hr, 2 * hr)
    npc = gw.shape[0]

    nhalf = nchip // 2
    half_rows = nhalf * 2 * gw.shape[3]
    near_half = lax.rem(c_o // nhalf + 1, 2)
    far_half = 1 - near_half

    def put(pc, n, lhs, rhs):
        first = (far_half, near_half)[n]
        val = mm(lhs[pl.ds(pl.multiple_of(first * half_rows, half_rows), half_rows), :], rhs)
        c = pl.ds(first * nhalf, nhalf)
        gw[pc, c] = val.reshape(nhalf, *gw.shape[2:])
        remote(gw.at[pc, c, 1 - core], pre.at[pc, c], pre_s.at[0], pre_r.at[pc, n], partner)().start()

    def add_half(pc, n):
        wait_bytes(pre.at[pc, 0:nhalf], pre_r.at[pc, n])
        c = pl.ds((far_half, near_half)[n] * nhalf, nhalf)
        pre[pc, c] = pre[pc, c] + gw[pc, c, core]

    def rs_far(pc):
        with scope('far%d' % pc):
            add_half(pc, 0)
            remote(pre.at[pc, c_o, lo], opp.at[pc, 0], opp_s.at[0], opp_r.at[pc], right)().start()
            remote(pre.at[pc, c_o, hi], opp.at[pc, 1], opp_s.at[0], opp_r.at[pc], left)().start()

    def rs_near(pc):
        with scope('near%d' % pc):
            add_half(pc, 1)
            remote(pre.at[pc, c_r, hi], fin.at[pc, 0], fin_s.at[0], fin_r.at[pc], right)().start()
            remote(pre.at[pc, c_l, lo], fin.at[pc, 1], fin_s.at[0], fin_r.at[pc], left)().start()

    def rs_relay(pc):
        with scope('relay%d' % pc):
            wait_bytes(opp.at[pc], opp_r.at[pc])
            pre[pc, c_r, lo] = pre[pc, c_r, lo] + opp[pc, 0]
            remote(pre.at[pc, c_r, lo], fin.at[pc, 2], fin_s.at[0], fin_r.at[pc], right)().start()
            pre[pc, c_l, hi] = pre[pc, c_l, hi] + opp[pc, 1]
            remote(pre.at[pc, c_l, hi], fin.at[pc, 3], fin_s.at[0], fin_r.at[pc], left)().start()

    def rs_final(pc):
        with scope('final%d' % pc):
            wait_bytes(fin.at[pc], fin_r.at[pc])
            gwst[pc, lo] = pre[pc, chip, lo] + fin[pc, 2] + fin[pc, 1]
            gwst[pc, hi] = pre[pc, chip, hi] + fin[pc, 0] + fin[pc, 3]

    def c3(g):
        with scope('c3'):
            c = pl.ds(pl.multiple_of(g * 256, 256), 256)
            ot_v[c, :] = mm(bd_a[g], vt_v[c, :]).astype(BF16)

    def c4(i):
        t = tile_of(i)
        for g in range(ngrp):
            dqkv_v[t, 2 * width + 256 * g:2 * width + 256 * g + 256] = mm(do_v[t, cols(g)], bd_a[g]).astype(BF16)

    with scope('transpose'):
        for i in range(nt):
            t = tile_of(i)
            ut_v[:, t] = u_v[t, :].T
            vt_v[:, t] = v_v[t, :].T
    with scope('waita'):
        from_all(0, a_all)
    with scope('filla'):
        fill(bd_a, a_all)
    def gw_piece(pc, n, lhs, rhs):
        with scope('gw%d%s' % (pc, 'ab'[n])):
            put(pc, n, lhs, rhs)

    def dcols(c):
        return dqkv_v[:, c * width:(c + 1) * width]

    def c7(i):
        t = tile_of(i)
        out_v[t, :] = (x_v[t, :].astype(F32) + mm(ot_v[:, t], wout_v[...], TN)).astype(BF16)

    c3(far_half)
    with scope('gw0a'):
        vjp_rest(*vjp_gram())
        put(0, 0, ot_v, dy_v[...])
        to_all(1, e_all)
        to_all(2, st_all)
    c3(near_half)
    gw_piece(0, 1, ot_v, dy_v[...])
    rs_far(0)

    with scope('c4'):
        for i in range(nt):
            c4(i)
    gw_piece(1, 0, ut_v, dcols(2))
    rs_near(0)
    gw_piece(1, 1, ut_v, dcols(2))
    with scope('c7a'):
        for i in range(nt // 2):
            c7(i)
    rs_far(1)

    with scope('waite'):
        from_all(1, e_all)
        from_all(2, st_all)
    with scope('fillg'):
        fill(bd_g, e_all)
        pair = [st_all[2 * j, 0:2, :] + st_all[2 * j + 1, 0:2, :] for j in range(heads // 2)]
        dsq2 = jnp.concatenate([2.0 * p[0:1] for p in pair], axis=1)
        dsk2 = jnp.concatenate([2.0 * p[1:2] for p in pair], axis=1)
        lane1 = lax.broadcasted_iota(jnp.int32, (1, 2 * hd), 1)
        gt = jnp.zeros((1, 2 * hd), F32)
        for h in range(heads):
            gt = jnp.where(lane1 == h, st_all[h, 2:3, :], gt)
        gtemp_ref[...] = gt[:, 0:heads]

    def c5(i):
        t = tile_of(i)
        for g in range(ngrp):
            c = cols(g)
            dqkv_v[t, c] = (mm(k_v[t, c], bd_g[g], NT) + q_v[t, c].astype(F32) * dsq2[:, c]).astype(BF16)

    def c6(i):
        t = tile_of(i)
        for g in range(ngrp):
            c = cols(g)
            dqkv_v[t, width + 256 * g:width + 256 * g + 256] = (
                mm(q_v[t, c], bd_g[g]) + k_v[t, c].astype(F32) * dsk2[:, c]).astype(BF16)

    with scope('c5'):
        for i in range(nt):
            c5(i)
    rs_near(1)
    gw_piece(2, 0, ut_v, dcols(0))
    rs_relay(0)
    with scope('c6'):
        for i in range(nt):
            c6(i)
    gw_piece(3, 0, ut_v, dcols(1))
    rs_far(2)
    gw_piece(2, 1, ut_v, dcols(0))
    rs_far(3)
    gw_piece(3, 1, ut_v, dcols(1))
    rs_relay(1)
    rs_near(2)
    def c8(i):
        t = tile_of(i)
        du = mm(dqkv_v[t, :], wqkv_v[...], NT)
        rstd = rstd_v[t, :]
        xhat = (x_v[t, :].astype(F32) - mean_v[t, :]) * rstd
        p = du * xhat
        accumulate(gbacc, 0, jnp.sum(p.reshape(tile // 8, 8, width), axis=0), i == 0)
        accumulate(gbacc, 1, jnp.sum(du.reshape(tile // 8, 8, width), axis=0), i == 0)
        dxh = du * gain_v[...]
        m1 = jnp.mean(dxh, axis=1, keepdims=True)
        m2 = jnp.mean(p * gain_v[...], axis=1, keepdims=True)
        dx = rstd * (dxh - m1 - xhat * m2)
        gtok_v[t, :] = (dy_v[t, :].astype(F32) + dx).astype(BF16)

    with scope('c8a'):
        c8(0)
    rs_near(3)
    with scope('c8b'):
        c8(1)
    with scope('c8c'):
        c8(2)
    rs_relay(2)
    with scope('c8d'):
        c8(3)
        for n in range(2):
            row_sum = jnp.sum(gbacc[n], axis=0, keepdims=True)
            for j in range(width // 128):
                gb_all[me, 4 * n + j:4 * n + j + 1, :] = row_sum[:, 128 * j:128 * j + 128]
        to_all(3, gb_all)
    rs_relay(3)
    with scope('c7b'):
        for i in range(nt // 2, nt):
            c7(i)
    for pc in range(npc):
        rs_final(pc)

    with scope('gb'):
        from_all(3, gb_all)
        gb = gb_all[0]
        for d in range(1, ns):
            gb = gb + gb_all[d]
        for j in range(width // 128):
            ggain_ref[:, 128 * j:128 * j + 128] = gb[j:j + 1]
            gbias_ref[:, 128 * j:128 * j + 128] = gb[4 + j:5 + j]

    with scope('drain'):
        for kind, mid in enumerate((gpre, dpre)):
            wait_bytes(mid, own_s.at[kind, 0])
            wait_bytes(mid.at[1:nchip], own_s.at[kind, 1])
        for kind, buf in enumerate((a_all, e_all, st_all, gb_all)):
            wait_bytes(buf.at[0:ns - 1], all_s.at[kind])
        wait_bytes(pre, pre_s.at[0])
        wait_bytes(opp, opp_s.at[0])
        wait_bytes(fin, fin_s.at[0])


def writer(width, out_v, gtok_v, gwst, gg_v, gb_v, gt_v, out_hbm, gtok_hbm, gwqkv_hbm, gwout_hbm, gg_hbm, gb_hbm, gt_hbm, sem):
    copies = [(gg_v, gg_hbm), (gb_v, gb_hbm), (gt_v, gt_hbm), (gwst.at[0], gwout_hbm)]
    copies += [(gwst.at[pc], gwqkv_hbm.at[:, pl.ds(c * width, width)]) for pc, c in ((1, 2), (2, 0), (3, 1))]
    copies += [(out_v, out_hbm), (gtok_v, gtok_hbm)]
    for i, (src, dst) in enumerate(copies):
        pltpu.make_async_copy(src, dst, sem.at[i]).start()
    for i, (src, dst) in enumerate(copies):
        pltpu.make_async_copy(src, dst, sem.at[i]).wait()


def solution(mesh):
    ns = mesh.shape['sp']
    row_spec = P(('dp', 'sp'), None)
    part_spec = P('dp')

    def local_step(x, dy, gain, bias, w_qkv, w_out, temp):
        rows, width = x.shape
        heads = temp.shape[0]
        hd = width // heads
        tile = 512
        nt = rows // tile
        share = width // ns
        nchip = ns // 2
        ngrp = width // 256
        hbm = pl.BlockSpec(memory_space=pl.ANY)
        vmem = pl.BlockSpec(memory_space=pltpu.VMEM)
        tok = lambda: pltpu.VMEM((rows, width), BF16)
        tok_t = lambda: pltpu.VMEM((width, rows), BF16)
        outs = pl.pallas_call(
            functools.partial(kernel, ns, rows, width, heads, tile),
            out_shape=[pltpu.VMEM((rows, width), BF16), pltpu.VMEM((rows, width), BF16),
                       pltpu.VMEM((4, share, width), F32), pltpu.VMEM((1, width), F32),
                       pltpu.VMEM((1, width), F32), pltpu.VMEM((1, heads), F32)],
            in_specs=[hbm] * 7,
            out_specs=[vmem] * 6,
            scratch_shapes=[
                tok(), tok(), pltpu.VMEM((1, width), F32), pltpu.VMEM((1, width), F32),
                pltpu.VMEM((width, 3 * width), BF16), pltpu.VMEM((width, width), BF16), pltpu.SMEM((heads,), F32),
                tok(), tok(), tok(), tok(), tok(), tok_t(), tok_t(), tok_t(), pltpu.VMEM((rows, 3 * width), BF16),
                pltpu.VMEM((rows, 1), F32), pltpu.VMEM((rows, 1), F32),
                pltpu.VMEM((ngrp, 256, 256), F32), pltpu.VMEM((ngrp, 256, 256), F32),
                pltpu.VMEM((8, width), F32), pltpu.VMEM((8, width), F32),
                pltpu.VMEM((nchip, 2, hd // 2 + 8, 2 * hd), F32), pltpu.VMEM((nchip, hd // 2 + 8, 2 * hd), F32),
                pltpu.VMEM((nchip, hd // 2 + 8, 2 * hd), F32),
                pltpu.VMEM((nchip, 2, hd // 2, 2 * hd), F32), pltpu.VMEM((nchip, hd // 2, 2 * hd), F32),
                pltpu.VMEM((nchip, hd // 2, 2 * hd), F32),
                pltpu.VMEM((heads, hd // 2, 2 * hd), BF16), pltpu.VMEM((heads, hd // 2, 2 * hd), BF16),
                pltpu.VMEM((heads, 8, 2 * hd), F32),
                pltpu.VMEM((ngrp, 256, 256), BF16), pltpu.VMEM((ngrp, 256, 256), BF16),
                pltpu.VMEM((4, nchip, 2, share, width), F32), pltpu.VMEM((4, nchip, share, width), F32),
                pltpu.VMEM((4, 2, share // 2, width), F32), pltpu.VMEM((4, 4, share // 2, width), F32),
                pltpu.VMEM((2, 8, width), F32), pltpu.VMEM((ns, 8, 128), F32),
                pltpu.SemaphoreType.DMA((nt + 9,)),
                pltpu.SemaphoreType.DMA((2, 2)), pltpu.SemaphoreType.DMA((2, 2)),
                pltpu.SemaphoreType.DMA((4,)), pltpu.SemaphoreType.DMA((4,)),
                pltpu.SemaphoreType.DMA((1,)), pltpu.SemaphoreType.DMA((4, 2)),
                pltpu.SemaphoreType.DMA((1,)), pltpu.SemaphoreType.DMA((4,)),
                pltpu.SemaphoreType.DMA((1,)), pltpu.SemaphoreType.DMA((4,)),
            ],
            compiler_params=pltpu.CompilerParams(collective_id=0, has_side_effects=True,
                                                 vmem_limit_bytes=52 * 1024 * 1024),
        )(x, dy, gain.reshape(1, -1), bias.reshape(1, -1), w_qkv, w_out, temp)
        out, gtok, gwqkv, gwout, ggain, gbias, gtemp = pl.pallas_call(
            functools.partial(writer, width),
            out_shape=[jax.ShapeDtypeStruct((rows, width), BF16),
                       jax.ShapeDtypeStruct((rows, width), BF16),
                       jax.ShapeDtypeStruct((share, 3 * width), F32),
                       jax.ShapeDtypeStruct((share, width), F32),
                       jax.ShapeDtypeStruct((1, width), F32),
                       jax.ShapeDtypeStruct((1, width), F32),
                       jax.ShapeDtypeStruct((1, heads), F32)],
            in_specs=[vmem] * 6,
            out_specs=[hbm] * 7,
            scratch_shapes=[pltpu.SemaphoreType.DMA((9,))],
            compiler_params=pltpu.CompilerParams(vmem_limit_bytes=1024 * 1024),
        )(*outs)
        return out, gtok, gwqkv, gwout, ggain.reshape(-1), gbias.reshape(-1), gtemp.reshape(-1)

    full = P()
    return jax.shard_map(local_step, mesh=mesh,
                         in_specs=(row_spec, row_spec, full, full, full, full, full),
                         out_specs=(row_spec, row_spec, row_spec, row_spec, part_spec, part_spec, part_spec),
                         check_vma=False)
```

```python
import functools

import jax
import jax.numpy as jnp
from jax import lax
from jax.experimental import pallas as pl
from jax.experimental.pallas import tpu as pltpu
from jax.sharding import PartitionSpec as P

F32 = jnp.float32
BF16 = jnp.bfloat16
NN = (((1,), (0,)), ((), ()))
NT = (((1,), (1,)), ((), ()))
TN = (((0,), (0,)), ((), ()))
EPS = 1e-6


def mm(a, b, dims=NN):
    return lax.dot_general(a, b, dims, preferred_element_type=F32)


def kernel(ns, rows, width, heads, tile,
           x_hbm, dy_hbm, gain_hbm, bias_hbm, wqkv_hbm, wout_hbm, temp_hbm,
           out_v, gtok_v, gwst, ggain_ref, gbias_ref, gtemp_ref,
           x_v, dy_v, gain_v, bias_v, wqkv_v, wout_v, temp_ref,
           u_v, q_v, k_v, v_v, do_v, ut_v, vt_v, ot_v, dqkv_v, mean_v, rstd_v,
           gacc, dacc, sqacc, skacc, gsend, gpre, grecv, dsend, dpre, drecv, a_all, e_all, st_all, bd_a, bd_g,
           gw, pre, opp, fin, gbacc, gb_all,
           in_sem, own_s, own_r, all_s, all_r, pre_s, pre_r, opp_s, opp_r, fin_s, fin_r):
    me = lax.axis_index('sp')
    nt = rows // tile
    hd = width // heads
    core = lax.rem(me, 2)
    chip = me // 2
    nchip = ns // 2
    partner = me + 1 - 2 * core
    right = lax.rem(me + 2, ns)
    left = lax.rem(me + ns - 2, ns)
    c_r = lax.rem(chip + 1, nchip)
    c_l = lax.rem(chip + nchip - 1, nchip)
    c_o = lax.rem(chip + 2, nchip)
    scope = jax.named_scope

    def remote(src, dst, ssem, rsem, dev):
        return lambda: pltpu.make_async_remote_copy(src_ref=src, dst_ref=dst, send_sem=ssem, recv_sem=rsem,
                                                    device_id={'sp': dev}, device_id_type=pl.DeviceIdType.MESH)

    def wait_bytes(ref, sem):
        pltpu.make_async_copy(ref, ref, sem).wait()

    far_first = sorted(range(1, nchip), key=lambda s: -min(s, nchip - s))
    peers = [2 * lax.rem(chip + s, nchip) + c for s in far_first for c in (core, 1 - core)] + [partner]

    barrier = pltpu.get_barrier_semaphore()
    def ld(i, src, dst):
        return lambda: pltpu.make_async_copy(src, dst, in_sem.at[i])

    def tile_of(i):
        return slice(i * tile, (i + 1) * tile)

    def x_copy(i):
        return ld(i, x_hbm.at[tile_of(i)], x_v.at[tile_of(i)])

    dy_copy = ld(nt, dy_hbm, dy_v)
    gain_copy = ld(nt + 1, gain_hbm, gain_v)
    bias_copy = ld(nt + 2, bias_hbm, bias_v)
    wq_copy = ld(nt + 3, wqkv_hbm.at[:, 0:width], wqkv_v.at[:, 0:width])
    wk_copy = ld(nt + 7, wqkv_hbm.at[:, width:2 * width], wqkv_v.at[:, width:2 * width])
    wv_copy = ld(nt + 4, wqkv_hbm.at[:, 2 * width:3 * width], wqkv_v.at[:, 2 * width:3 * width])
    wout_copy = ld(nt + 5, wout_hbm, wout_v)
    temp_copy = ld(nt + 6, temp_hbm, temp_ref)
    head = slice(0, tile // 2)
    rest = slice(tile // 2, tile)
    x_head = ld(0, x_hbm.at[head], x_v.at[head])
    x_rest = ld(nt + 8, x_hbm.at[rest], x_v.at[rest])
    x_head().start()
    gain_copy().start()
    bias_copy().start()
    wq_copy().start()
    x_rest().start()
    wk_copy().start()
    x_copy(1)().start()
    for dev in peers:
        pl.semaphore_signal(barrier, inc=1, device_id={'sp': dev}, device_id_type=pl.DeviceIdType.MESH)

    with scope('init'):
        bd_a[...] = jnp.zeros_like(bd_a)
        bd_g[...] = jnp.zeros_like(bd_g)

    ngrp = width // 256
    hpg = heads // ngrp

    def cols(g):
        return slice(256 * g, 256 * g + 256)

    def ln(t):
        x = x_v[t, :].astype(F32)
        mean = jnp.mean(x, axis=1, keepdims=True)
        cent = x - mean
        var = jnp.mean(cent * cent, axis=1, keepdims=True)
        rstd = lax.rsqrt(var + EPS)
        mean_v[t, :] = mean
        rstd_v[t, :] = rstd
        u_v[t, :] = (cent * rstd * gain_v[...] + bias_v[...]).astype(BF16)

    def accumulate(ref, idx, val, first):
        if first:
            ref[idx] = val
        else:
            ref[idx] += val

    def square_sum(ref, c, val, first):
        v32 = val.astype(F32)
        part = jnp.sum((v32 * v32).reshape(tile // 8, 8, 256), axis=0)
        ref[:, c] = part if first else ref[:, c] + part

    with scope('wx0'):
        x_head().wait()
        for i in range(2, nt):
            x_copy(i)().start()
        gain_copy().wait()
        bias_copy().wait()
    with scope('ln0'):
        ln(head)
    with scope('ww'):
        wq_copy().wait()
        x_rest().wait()
    with scope('c1h'):
        ln(rest)
        q_v[head, :] = mm(u_v[head, :], wqkv_v[:, 0:width]).astype(BF16)
    with scope('ww2'):
        wk_copy().wait()
        x_copy(1)().wait()
        wv_copy().start()
        wout_copy().start()
        dy_copy().start()
        temp_copy().start()
    with scope('c1'):
        for i in range(nt):
            t = tile_of(i)
            if i == 1:
                for j in range(2, nt):
                    x_copy(j)().wait()
            if i + 1 < nt:
                ln(tile_of(i + 1))
            if i == 0:
                q_v[rest, :] = mm(u_v[rest, :], wqkv_v[:, 0:width]).astype(BF16)
                q = q_v[t, :]
            else:
                q = mm(u_v[t, :], wqkv_v[:, 0:width]).astype(BF16)
                q_v[t, :] = q
            k = mm(u_v[t, :], wqkv_v[:, width:2 * width]).astype(BF16)
            k_v[t, :] = k
            for g in range(ngrp):
                c = cols(g)
                square_sum(sqacc, c, q[:, c], i == 0)
                square_sum(skacc, c, k[:, c], i == 0)
                if i == nt - 2:
                    done = slice(0, (nt - 1) * tile)
                    gacc[g] = mm(q_v[done, c], k_v[done, c], TN)
                elif i == nt - 1:
                    gacc[g] += mm(q[:, c], k[:, c], TN)

    lane32 = lax.broadcasted_iota(jnp.int32, (hd // 2, 2 * hd), 1)

    def pack_block(blk, odd):
        top, bot = blk[0:hd // 2], blk[hd // 2:hd]
        if odd:
            top = pltpu.roll(top, hd, axis=1)
        else:
            bot = pltpu.roll(bot, hd, axis=1)
        return jnp.where(lane32 < hd, top, bot)

    def pack(acc, h):
        g, hh = h // hpg, h % hpg
        return pack_block(acc[g, hh * hd:hh * hd + hd, (hh // 2) * 128:(hh // 2) * 128 + 128], h % 2 == 1)

    with scope('packg'):
        sq_row = jnp.sum(sqacc[...], axis=0, keepdims=True)
        sk_row = jnp.sum(skacc[...], axis=0, keepdims=True)
        for h in range(heads):
            gsend[h // 2, h % 2, 0:hd // 2, :] = pack(gacc, h)
            c = slice((h // 2) * 128, (h // 2) * 128 + 128)
            gsend[h // 2, h % 2, hd // 2:hd // 2 + 1, :] = sq_row[:, c]
            gsend[h // 2, h % 2, hd // 2 + 1:hd // 2 + 2, :] = sk_row[:, c]

    def to_partner(kind, src, dst):
        return remote(src.at[:, 1 - core], dst, own_s.at[kind, 0], own_r.at[kind, 0], partner)

    def chip_sum(kind, src, mid, dst):
        wait_bytes(mid, own_r.at[kind, 0])
        n = mid.shape[1] if kind else hd // 2 + 2
        for c in range(nchip):
            mid[c, 0:n] = mid[c, 0:n] + src[c, core, 0:n]
        for s in far_first:
            c = lax.rem(chip + s, nchip)
            remote(mid.at[c], dst.at[s], own_s.at[kind, 1], own_r.at[kind, 1], 2 * c + core)().start()

    def image_sum(kind, mid, dst):
        n = mid.shape[1] if kind else hd // 2 + 2
        wait_bytes(dst.at[1:nchip], own_r.at[kind, 1])
        tot = mid[chip, 0:n]
        for s in range(1, nchip):
            tot = tot + dst[s, 0:n]
        return tot

    def to_all(kind, buf):
        for dev in peers:
            remote(buf.at[me], buf.at[me], all_s.at[kind], all_r.at[kind], dev)().start()

    def from_all(kind, buf):
        wait_bytes(buf.at[0:ns - 1], all_r.at[kind])

    with scope('sendg'):
        pl.semaphore_wait(barrier, ns - 1)
        to_partner(0, gsend, gpre)().start()

    def v_rows(t):
        v_v[t, :] = mm(u_v[t, :], wqkv_v[:, 2 * width:3 * width]).astype(BF16)

    cut = rows // 2
    with scope('c2a'):
        wv_copy().wait()
        v_rows(slice(0, cut))
    with scope('chipg'):
        chip_sum(0, gsend, gpre, grecv)
    with scope('c2b'):
        wout_copy().wait()
        dy_copy().wait()
        v_rows(slice(cut, rows))
        for i in range(nt):
            t = tile_of(i)
            do_v[t, :] = mm(dy_v[t, :], wout_v[...], NT).astype(BF16)
        for g in range(ngrp):
            dacc[g] = mm(do_v[:, cols(g)], v_v[:, cols(g)], TN)
    with scope('sendd'):
        for h in range(heads):
            dsend[h // 2, h % 2] = pack(dacc, h)
        to_partner(1, dsend, dpre)().start()

    row = lax.broadcasted_iota(jnp.int32, (hd, 2 * hd), 0)
    lanep = lax.broadcasted_iota(jnp.int32, (hd, 2 * hd), 1) - hd * core
    half = (lanep >= 0) & (lanep < hd)
    diag = lanep == row
    half1 = half[0:1]
    even = core == 0

    def unpack(p):
        rolled = pltpu.roll(p, hd, axis=1)
        full = jnp.concatenate([jnp.where(even, p, rolled), jnp.where(even, rolled, p)], axis=0)
        return jnp.where(half, full, 0.0)

    def pack_mine(blk):
        rolled = pltpu.roll(blk, hd, axis=1)
        low, high = jnp.where(even, blk, rolled), jnp.where(even, rolled, blk)
        return jnp.where(lane32 < hd, low[0:hd // 2], high[hd // 2:hd])

    with scope('waitg'):
        tot = image_sum(0, gpre, grecv)
    with scope('soft'):
        gram = unpack(tot[0:hd // 2])
        sq_r = tot[hd // 2:hd // 2 + 1]
        sk_r = jnp.where(half1, tot[hd // 2 + 1:hd // 2 + 2], 1.0)
        sq_c = jnp.sum(jnp.where(diag, sq_r, 0.0), axis=1, keepdims=True)
        den = jnp.sqrt(sq_c) * jnp.sqrt(sk_r)
        cosine = gram / den
        temp_copy().wait()
        temp = temp_ref[me]
        logits = jnp.where(half, temp * cosine, -jnp.inf)
        ex = jnp.exp(logits - jnp.max(logits, axis=1, keepdims=True))
        attn = ex / jnp.sum(ex, axis=1, keepdims=True)
        a_all[me] = pack_mine(attn).astype(BF16)
        to_all(0, a_all)
    with scope('chipd'):
        chip_sum(1, dsend, dpre, drecv)

    def vjp_gram():
        d_a = unpack(image_sum(1, dpre, drecv))
        inner = jnp.sum(d_a * attn, axis=1, keepdims=True)
        d_s = attn * (d_a - inner)
        d_cos = temp * d_s
        e_all[me] = pack_mine(d_cos / den).astype(BF16)
        return d_s, d_cos * cosine

    def vjp_rest(d_s, ec):
        d_t = jnp.sum(jnp.sum(d_s * cosine, axis=1, keepdims=True), axis=0, keepdims=True)
        dsq_c = -0.5 * jnp.sum(ec, axis=1, keepdims=True) / sq_c
        dsk_r = -0.5 * jnp.sum(ec, axis=0, keepdims=True) / sk_r
        st_all[me, 0:1, :] = jnp.sum(jnp.where(diag, dsq_c, 0.0), axis=0, keepdims=True)
        st_all[me, 1:2, :] = dsk_r
        st_all[me, 2:3, :] = jnp.broadcast_to(d_t, (1, 2 * hd))

    def fill(bd, blocks):
        for h in range(heads):
            g, hh = h // hpg, h % hpg
            p = blocks[h].astype(F32)
            rolled = pltpu.roll(p, hd, axis=1)
            mine = (lane32 < hd) if h % 2 == 0 else (lane32 >= hd)
            top, bot = (p, rolled) if h % 2 == 0 else (rolled, p)
            c = slice((hh // 2) * 128, (hh // 2) * 128 + 128)
            bd[g, hh * hd:hh * hd + hd // 2, c] = jnp.where(mine, top, 0.0).astype(BF16)
            bd[g, hh * hd + hd // 2:hh * hd + hd, c] = jnp.where(mine, bot, 0.0).astype(BF16)

    hr = gw.shape[3] // 2
    lo, hi = slice(0, hr), slice(hr, 2 * hr)
    npc = gw.shape[0]

    nhalf = nchip // 2
    half_rows = nhalf * 2 * gw.shape[3]
    near_half = lax.rem(c_o // nhalf + 1, 2)
    far_half = 1 - near_half

    def put(pc, n, lhs, rhs):
        first = (far_half, near_half)[n]
        val = mm(lhs[pl.ds(pl.multiple_of(first * half_rows, half_rows), half_rows), :], rhs)
        c = pl.ds(first * nhalf, nhalf)
        gw[pc, c] = val.reshape(nhalf, *gw.shape[2:])
        remote(gw.at[pc, c, 1 - core], pre.at[pc, c], pre_s.at[0], pre_r.at[pc, n], partner)().start()

    def add_half(pc, n):
        wait_bytes(pre.at[pc, 0:nhalf], pre_r.at[pc, n])
        c = pl.ds((far_half, near_half)[n] * nhalf, nhalf)
        pre[pc, c] = pre[pc, c] + gw[pc, c, core]

    def rs_far(pc):
        with scope('far%d' % pc):
            add_half(pc, 0)
            remote(pre.at[pc, c_o, lo], opp.at[pc, 0], opp_s.at[0], opp_r.at[pc], right)().start()
            remote(pre.at[pc, c_o, hi], opp.at[pc, 1], opp_s.at[0], opp_r.at[pc], left)().start()

    def rs_near(pc):
        with scope('near%d' % pc):
            add_half(pc, 1)
            remote(pre.at[pc, c_r, hi], fin.at[pc, 0], fin_s.at[0], fin_r.at[pc], right)().start()
            remote(pre.at[pc, c_l, lo], fin.at[pc, 1], fin_s.at[0], fin_r.at[pc], left)().start()

    def rs_relay(pc):
        with scope('relay%d' % pc):
            wait_bytes(opp.at[pc], opp_r.at[pc])
            pre[pc, c_r, lo] = pre[pc, c_r, lo] + opp[pc, 0]
            remote(pre.at[pc, c_r, lo], fin.at[pc, 2], fin_s.at[0], fin_r.at[pc], right)().start()
            pre[pc, c_l, hi] = pre[pc, c_l, hi] + opp[pc, 1]
            remote(pre.at[pc, c_l, hi], fin.at[pc, 3], fin_s.at[0], fin_r.at[pc], left)().start()

    def rs_final(pc):
        with scope('final%d' % pc):
            wait_bytes(fin.at[pc], fin_r.at[pc])
            gwst[pc, lo] = pre[pc, chip, lo] + fin[pc, 2] + fin[pc, 1]
            gwst[pc, hi] = pre[pc, chip, hi] + fin[pc, 0] + fin[pc, 3]

    def c3(g):
        with scope('c3'):
            c = pl.ds(pl.multiple_of(g * 256, 256), 256)
            ot_v[c, :] = mm(bd_a[g], vt_v[c, :]).astype(BF16)

    def c4(i):
        t = tile_of(i)
        for g in range(ngrp):
            dqkv_v[t, 2 * width + 256 * g:2 * width + 256 * g + 256] = mm(do_v[t, cols(g)], bd_a[g]).astype(BF16)

    with scope('transpose'):
        for i in range(nt):
            t = tile_of(i)
            ut_v[:, t] = u_v[t, :].T
            vt_v[:, t] = v_v[t, :].T
    with scope('waita'):
        from_all(0, a_all)
    with scope('filla'):
        fill(bd_a, a_all)
    def gw_piece(pc, n, lhs, rhs):
        with scope('gw%d%s' % (pc, 'ab'[n])):
            put(pc, n, lhs, rhs)

    def dcols(c):
        return dqkv_v[:, c * width:(c + 1) * width]

    def c7(i):
        t = tile_of(i)
        out_v[t, :] = (x_v[t, :].astype(F32) + mm(ot_v[:, t], wout_v[...], TN)).astype(BF16)

    c3(far_half)
    with scope('gw0a'):
        vjp_rest(*vjp_gram())
        put(0, 0, ot_v, dy_v[...])
        to_all(1, e_all)
        to_all(2, st_all)
    c3(near_half)
    gw_piece(0, 1, ot_v, dy_v[...])
    rs_far(0)

    with scope('c4'):
        for i in range(nt):
            c4(i)
    gw_piece(1, 0, ut_v, dcols(2))
    rs_near(0)
    gw_piece(1, 1, ut_v, dcols(2))
    with scope('c7a'):
        for i in range(nt // 2):
            c7(i)
    rs_far(1)

    with scope('waite'):
        from_all(1, e_all)
        from_all(2, st_all)
    with scope('fillg'):
        fill(bd_g, e_all)
        pair = [st_all[2 * j, 0:2, :] + st_all[2 * j + 1, 0:2, :] for j in range(heads // 2)]
        dsq2 = jnp.concatenate([2.0 * p[0:1] for p in pair], axis=1)
        dsk2 = jnp.concatenate([2.0 * p[1:2] for p in pair], axis=1)
        lane1 = lax.broadcasted_iota(jnp.int32, (1, 2 * hd), 1)
        gt = jnp.zeros((1, 2 * hd), F32)
        for h in range(heads):
            gt = jnp.where(lane1 == h, st_all[h, 2:3, :], gt)
        gtemp_ref[...] = gt[:, 0:heads]

    def c5(i):
        t = tile_of(i)
        for g in range(ngrp):
            c = cols(g)
            dqkv_v[t, c] = (mm(k_v[t, c], bd_g[g], NT) + q_v[t, c].astype(F32) * dsq2[:, c]).astype(BF16)

    def c6(i):
        t = tile_of(i)
        for g in range(ngrp):
            c = cols(g)
            dqkv_v[t, width + 256 * g:width + 256 * g + 256] = (
                mm(q_v[t, c], bd_g[g]) + k_v[t, c].astype(F32) * dsk2[:, c]).astype(BF16)

    with scope('c5'):
        for i in range(nt):
            c5(i)
    rs_near(1)
    gw_piece(2, 0, ut_v, dcols(0))
    rs_relay(0)
    with scope('c6'):
        for i in range(nt):
            c6(i)
    gw_piece(3, 0, ut_v, dcols(1))
    @pl.when(core == 0)
    def _():
        rs_far(2)

    gw_piece(2, 1, ut_v, dcols(0))

    @pl.when(core == 0)
    def _():
        rs_far(3)

    gw_piece(3, 1, ut_v, dcols(1))

    @pl.when(core == 1)
    def _():
        rs_far(2)
        rs_far(3)

    rs_relay(1)
    rs_near(2)
    def c8(i):
        t = tile_of(i)
        du = mm(dqkv_v[t, :], wqkv_v[...], NT)
        rstd = rstd_v[t, :]
        xhat = (x_v[t, :].astype(F32) - mean_v[t, :]) * rstd
        p = du * xhat
        accumulate(gbacc, 0, jnp.sum(p.reshape(tile // 8, 8, width), axis=0), i == 0)
        accumulate(gbacc, 1, jnp.sum(du.reshape(tile // 8, 8, width), axis=0), i == 0)
        dxh = du * gain_v[...]
        m1 = jnp.mean(dxh, axis=1, keepdims=True)
        m2 = jnp.mean(p * gain_v[...], axis=1, keepdims=True)
        dx = rstd * (dxh - m1 - xhat * m2)
        gtok_v[t, :] = (dy_v[t, :].astype(F32) + dx).astype(BF16)

    with scope('c8a'):
        c8(0)
    rs_near(3)
    with scope('c8b'):
        c8(1)
    with scope('c8c'):
        c8(2)
    rs_relay(2)
    with scope('c8d'):
        c8(3)
        for n in range(2):
            row_sum = jnp.sum(gbacc[n], axis=0, keepdims=True)
            for j in range(width // 128):
                gb_all[me, 4 * n + j:4 * n + j + 1, :] = row_sum[:, 128 * j:128 * j + 128]
        to_all(3, gb_all)
    rs_relay(3)
    with scope('c7b'):
        for i in range(nt // 2, nt):
            c7(i)
    for pc in range(npc):
        rs_final(pc)

    with scope('gb'):
        from_all(3, gb_all)
        gb = gb_all[0]
        for d in range(1, ns):
            gb = gb + gb_all[d]
        for j in range(width // 128):
            ggain_ref[:, 128 * j:128 * j + 128] = gb[j:j + 1]
            gbias_ref[:, 128 * j:128 * j + 128] = gb[4 + j:5 + j]

    with scope('drain'):
        for kind, mid in enumerate((gpre, dpre)):
            wait_bytes(mid, own_s.at[kind, 0])
            wait_bytes(mid.at[1:nchip], own_s.at[kind, 1])
        for kind, buf in enumerate((a_all, e_all, st_all, gb_all)):
            wait_bytes(buf.at[0:ns - 1], all_s.at[kind])
        wait_bytes(pre, pre_s.at[0])
        wait_bytes(opp, opp_s.at[0])
        wait_bytes(fin, fin_s.at[0])


def writer(width, out_v, gtok_v, gwst, gg_v, gb_v, gt_v, out_hbm, gtok_hbm, gwqkv_hbm, gwout_hbm, gg_hbm, gb_hbm, gt_hbm, sem):
    copies = [(gg_v, gg_hbm), (gb_v, gb_hbm), (gt_v, gt_hbm), (gwst.at[0], gwout_hbm)]
    copies += [(gwst.at[pc], gwqkv_hbm.at[:, pl.ds(c * width, width)]) for pc, c in ((1, 2), (2, 0), (3, 1))]
    copies += [(out_v, out_hbm), (gtok_v, gtok_hbm)]
    for i, (src, dst) in enumerate(copies):
        pltpu.make_async_copy(src, dst, sem.at[i]).start()
    for i, (src, dst) in enumerate(copies):
        pltpu.make_async_copy(src, dst, sem.at[i]).wait()


def solution(mesh):
    ns = mesh.shape['sp']
    row_spec = P(('dp', 'sp'), None)
    part_spec = P('dp')

    def local_step(x, dy, gain, bias, w_qkv, w_out, temp):
        rows, width = x.shape
        heads = temp.shape[0]
        hd = width // heads
        tile = 512
        nt = rows // tile
        share = width // ns
        nchip = ns // 2
        ngrp = width // 256
        hbm = pl.BlockSpec(memory_space=pl.ANY)
        vmem = pl.BlockSpec(memory_space=pltpu.VMEM)
        tok = lambda: pltpu.VMEM((rows, width), BF16)
        tok_t = lambda: pltpu.VMEM((width, rows), BF16)
        outs = pl.pallas_call(
            functools.partial(kernel, ns, rows, width, heads, tile),
            out_shape=[pltpu.VMEM((rows, width), BF16), pltpu.VMEM((rows, width), BF16),
                       pltpu.VMEM((4, share, width), F32), pltpu.VMEM((1, width), F32),
                       pltpu.VMEM((1, width), F32), pltpu.VMEM((1, heads), F32)],
            in_specs=[hbm] * 7,
            out_specs=[vmem] * 6,
            scratch_shapes=[
                tok(), tok(), pltpu.VMEM((1, width), F32), pltpu.VMEM((1, width), F32),
                pltpu.VMEM((width, 3 * width), BF16), pltpu.VMEM((width, width), BF16), pltpu.SMEM((heads,), F32),
                tok(), tok(), tok(), tok(), tok(), tok_t(), tok_t(), tok_t(), pltpu.VMEM((rows, 3 * width), BF16),
                pltpu.VMEM((rows, 1), F32), pltpu.VMEM((rows, 1), F32),
                pltpu.VMEM((ngrp, 256, 256), F32), pltpu.VMEM((ngrp, 256, 256), F32),
                pltpu.VMEM((8, width), F32), pltpu.VMEM((8, width), F32),
                pltpu.VMEM((nchip, 2, hd // 2 + 8, 2 * hd), F32), pltpu.VMEM((nchip, hd // 2 + 8, 2 * hd), F32),
                pltpu.VMEM((nchip, hd // 2 + 8, 2 * hd), F32),
                pltpu.VMEM((nchip, 2, hd // 2, 2 * hd), F32), pltpu.VMEM((nchip, hd // 2, 2 * hd), F32),
                pltpu.VMEM((nchip, hd // 2, 2 * hd), F32),
                pltpu.VMEM((heads, hd // 2, 2 * hd), BF16), pltpu.VMEM((heads, hd // 2, 2 * hd), BF16),
                pltpu.VMEM((heads, 8, 2 * hd), F32),
                pltpu.VMEM((ngrp, 256, 256), BF16), pltpu.VMEM((ngrp, 256, 256), BF16),
                pltpu.VMEM((4, nchip, 2, share, width), F32), pltpu.VMEM((4, nchip, share, width), F32),
                pltpu.VMEM((4, 2, share // 2, width), F32), pltpu.VMEM((4, 4, share // 2, width), F32),
                pltpu.VMEM((2, 8, width), F32), pltpu.VMEM((ns, 8, 128), F32),
                pltpu.SemaphoreType.DMA((nt + 9,)),
                pltpu.SemaphoreType.DMA((2, 2)), pltpu.SemaphoreType.DMA((2, 2)),
                pltpu.SemaphoreType.DMA((4,)), pltpu.SemaphoreType.DMA((4,)),
                pltpu.SemaphoreType.DMA((1,)), pltpu.SemaphoreType.DMA((4, 2)),
                pltpu.SemaphoreType.DMA((1,)), pltpu.SemaphoreType.DMA((4,)),
                pltpu.SemaphoreType.DMA((1,)), pltpu.SemaphoreType.DMA((4,)),
            ],
            compiler_params=pltpu.CompilerParams(collective_id=0, has_side_effects=True,
                                                 vmem_limit_bytes=52 * 1024 * 1024),
        )(x, dy, gain.reshape(1, -1), bias.reshape(1, -1), w_qkv, w_out, temp)
        out, gtok, gwqkv, gwout, ggain, gbias, gtemp = pl.pallas_call(
            functools.partial(writer, width),
            out_shape=[jax.ShapeDtypeStruct((rows, width), BF16),
                       jax.ShapeDtypeStruct((rows, width), BF16),
                       jax.ShapeDtypeStruct((share, 3 * width), F32),
                       jax.ShapeDtypeStruct((share, width), F32),
                       jax.ShapeDtypeStruct((1, width), F32),
                       jax.ShapeDtypeStruct((1, width), F32),
                       jax.ShapeDtypeStruct((1, heads), F32)],
            in_specs=[vmem] * 6,
            out_specs=[hbm] * 7,
            scratch_shapes=[pltpu.SemaphoreType.DMA((9,))],
            compiler_params=pltpu.CompilerParams(vmem_limit_bytes=1024 * 1024),
        )(*outs)
        return out, gtok, gwqkv, gwout, ggain.reshape(-1), gbias.reshape(-1), gtemp.reshape(-1)

    full = P()
    return jax.shard_map(local_step, mesh=mesh,
                         in_specs=(row_spec, row_spec, full, full, full, full, full),
                         out_specs=(row_spec, row_spec, row_spec, row_spec, part_spec, part_spec, part_spec),
                         check_vma=False)
```

```python
import functools

import jax
import jax.numpy as jnp
from jax import lax
from jax.experimental import pallas as pl
from jax.experimental.pallas import tpu as pltpu
from jax.sharding import PartitionSpec as P

F32 = jnp.float32
BF16 = jnp.bfloat16
NN = (((1,), (0,)), ((), ()))
NT = (((1,), (1,)), ((), ()))
TN = (((0,), (0,)), ((), ()))
EPS = 1e-6


def mm(a, b, dims=NN):
    return lax.dot_general(a, b, dims, preferred_element_type=F32)


def kernel(ns, rows, width, heads, tile,
           x_hbm, dy_hbm, gain_hbm, bias_hbm, wqkv_hbm, wout_hbm, temp_hbm,
           out_v, gtok_v, gwst, ggain_ref, gbias_ref, gtemp_ref,
           x_v, dy_v, gain_v, bias_v, wqkv_v, wout_v, temp_ref,
           u_v, q_v, k_v, v_v, do_v, ut_v, vt_v, ot_v, dqkv_v, mean_v, rstd_v,
           gacc, dacc, sqacc, skacc, gsend, gpre, grecv, dsend, dpre, drecv, a_all, e_all, st_all, bd_a, bd_g,
           gw, pre, opp, fin, gbacc, gb_mine, gb_mate, gb_all,
           in_sem, own_s, own_r, all_s, all_r, pre_s, pre_r, opp_s, opp_r, fin_s, fin_r):
    me = lax.axis_index('sp')
    nt = rows // tile
    hd = width // heads
    core = lax.rem(me, 2)
    chip = me // 2
    nchip = ns // 2
    partner = me + 1 - 2 * core
    right = lax.rem(me + 2, ns)
    left = lax.rem(me + ns - 2, ns)
    c_r = lax.rem(chip + 1, nchip)
    c_l = lax.rem(chip + nchip - 1, nchip)
    c_o = lax.rem(chip + 2, nchip)
    scope = jax.named_scope

    def remote(src, dst, ssem, rsem, dev):
        return lambda: pltpu.make_async_remote_copy(src_ref=src, dst_ref=dst, send_sem=ssem, recv_sem=rsem,
                                                    device_id={'sp': dev}, device_id_type=pl.DeviceIdType.MESH)

    def wait_bytes(ref, sem):
        pltpu.make_async_copy(ref, ref, sem).wait()

    far_first = sorted(range(1, nchip), key=lambda s: -min(s, nchip - s))
    peers = [2 * lax.rem(chip + s, nchip) + c for s in far_first for c in (1, 0)] + [partner]

    barrier = pltpu.get_barrier_semaphore()
    def ld(i, src, dst):
        return lambda: pltpu.make_async_copy(src, dst, in_sem.at[i])

    def tile_of(i):
        return slice(i * tile, (i + 1) * tile)

    def x_copy(i):
        return ld(i, x_hbm.at[tile_of(i)], x_v.at[tile_of(i)])

    dy_copy = ld(nt, dy_hbm, dy_v)
    gain_copy = ld(nt + 1, gain_hbm, gain_v)
    bias_copy = ld(nt + 2, bias_hbm, bias_v)
    wq_copy = ld(nt + 3, wqkv_hbm.at[:, 0:width], wqkv_v.at[:, 0:width])
    wk_copy = ld(nt + 7, wqkv_hbm.at[:, width:2 * width], wqkv_v.at[:, width:2 * width])
    wv_copy = ld(nt + 4, wqkv_hbm.at[:, 2 * width:3 * width], wqkv_v.at[:, 2 * width:3 * width])
    wout_copy = ld(nt + 5, wout_hbm, wout_v)
    temp_copy = ld(nt + 6, temp_hbm, temp_ref)
    head = slice(0, tile // 2)
    rest = slice(tile // 2, tile)
    x_head = ld(0, x_hbm.at[head], x_v.at[head])
    x_rest = ld(nt + 8, x_hbm.at[rest], x_v.at[rest])
    x_head().start()
    gain_copy().start()
    bias_copy().start()
    wq_copy().start()
    x_rest().start()
    wk_copy().start()
    x_copy(1)().start()
    for dev in peers:
        pl.semaphore_signal(barrier, inc=1, device_id={'sp': dev}, device_id_type=pl.DeviceIdType.MESH)

    with scope('init'):
        bd_a[...] = jnp.zeros_like(bd_a)
        bd_g[...] = jnp.zeros_like(bd_g)

    ngrp = width // 256
    hpg = heads // ngrp

    def cols(g):
        return slice(256 * g, 256 * g + 256)

    def ln(t):
        x = x_v[t, :].astype(F32)
        mean = jnp.mean(x, axis=1, keepdims=True)
        cent = x - mean
        var = jnp.mean(cent * cent, axis=1, keepdims=True)
        rstd = lax.rsqrt(var + EPS)
        mean_v[t, :] = mean
        rstd_v[t, :] = rstd
        u_v[t, :] = (cent * rstd * gain_v[...] + bias_v[...]).astype(BF16)

    def accumulate(ref, idx, val, first):
        if first:
            ref[idx] = val
        else:
            ref[idx] += val

    def square_sum(ref, c, val, first):
        v32 = val.astype(F32)
        part = jnp.sum((v32 * v32).reshape(tile // 8, 8, 256), axis=0)
        ref[:, c] = part if first else ref[:, c] + part

    with scope('wx0'):
        x_head().wait()
        for i in range(2, nt):
            x_copy(i)().start()
        gain_copy().wait()
        bias_copy().wait()
    with scope('ln0'):
        ln(head)
    with scope('ww'):
        wq_copy().wait()
        x_rest().wait()
    with scope('c1h'):
        ln(rest)
        q_v[head, :] = mm(u_v[head, :], wqkv_v[:, 0:width]).astype(BF16)
    with scope('ww2'):
        wk_copy().wait()
        x_copy(1)().wait()
        wv_copy().start()
        wout_copy().start()
        dy_copy().start()
        temp_copy().start()
    with scope('c1'):
        for i in range(nt):
            t = tile_of(i)
            if i == 1:
                for j in range(2, nt):
                    x_copy(j)().wait()
            if i + 1 < nt:
                ln(tile_of(i + 1))
            if i == 0:
                q_v[rest, :] = mm(u_v[rest, :], wqkv_v[:, 0:width]).astype(BF16)
                q = q_v[t, :]
            else:
                q = mm(u_v[t, :], wqkv_v[:, 0:width]).astype(BF16)
                q_v[t, :] = q
            k = mm(u_v[t, :], wqkv_v[:, width:2 * width]).astype(BF16)
            k_v[t, :] = k
            for g in range(ngrp):
                c = cols(g)
                square_sum(sqacc, c, q[:, c], i == 0)
                square_sum(skacc, c, k[:, c], i == 0)
                if i == nt - 2:
                    done = slice(0, (nt - 1) * tile)
                    gacc[g] = mm(q_v[done, c], k_v[done, c], TN)
                elif i == nt - 1:
                    gacc[g] += mm(q[:, c], k[:, c], TN)

    lane32 = lax.broadcasted_iota(jnp.int32, (hd // 2, 2 * hd), 1)

    def pack_block(blk, odd):
        top, bot = blk[0:hd // 2], blk[hd // 2:hd]
        if odd:
            top = pltpu.roll(top, hd, axis=1)
        else:
            bot = pltpu.roll(bot, hd, axis=1)
        return jnp.where(lane32 < hd, top, bot)

    def pack(acc, h):
        g, hh = h // hpg, h % hpg
        return pack_block(acc[g, hh * hd:hh * hd + hd, (hh // 2) * 128:(hh // 2) * 128 + 128], h % 2 == 1)

    with scope('packg'):
        sq_row = jnp.sum(sqacc[...], axis=0, keepdims=True)
        sk_row = jnp.sum(skacc[...], axis=0, keepdims=True)
        for h in range(heads):
            gsend[h // 2, h % 2, 0:hd // 2, :] = pack(gacc, h)
            c = slice((h // 2) * 128, (h // 2) * 128 + 128)
            gsend[h // 2, h % 2, hd // 2:hd // 2 + 1, :] = sq_row[:, c]
            gsend[h // 2, h % 2, hd // 2 + 1:hd // 2 + 2, :] = sk_row[:, c]

    def to_partner(kind, src, dst):
        return remote(src.at[:, 1 - core], dst, own_s.at[kind, 0], own_r.at[kind, 0], partner)

    def chip_sum(kind, src, mid, dst):
        wait_bytes(mid, own_r.at[kind, 0])
        n = mid.shape[1] if kind else hd // 2 + 2
        for c in range(nchip):
            mid[c, 0:n] = mid[c, 0:n] + src[c, core, 0:n]
        for s in far_first:
            c = lax.rem(chip + s, nchip)
            remote(mid.at[c, 0:n], dst.at[s, 0:n], own_s.at[kind, 1], own_r.at[kind, 1], 2 * c + core)().start()

    def image_sum(kind, mid, dst):
        n = mid.shape[1] if kind else hd // 2 + 2
        wait_bytes(dst.at[1:nchip, 0:n], own_r.at[kind, 1])
        tot = mid[chip, 0:n]
        for s in range(1, nchip):
            tot = tot + dst[s, 0:n]
        return tot

    def to_all(kind, buf):
        for dev in peers:
            remote(buf.at[me], buf.at[me], all_s.at[kind], all_r.at[kind], dev)().start()

    def from_all(kind, buf):
        wait_bytes(buf.at[0:ns - 1], all_r.at[kind])

    with scope('sendg'):
        pl.semaphore_wait(barrier, ns - 1)
        to_partner(0, gsend, gpre)().start()

    def v_rows(t):
        v_v[t, :] = mm(u_v[t, :], wqkv_v[:, 2 * width:3 * width]).astype(BF16)

    cut = rows // 2
    with scope('c2a'):
        wv_copy().wait()
        v_rows(slice(0, cut))
    with scope('chipg'):
        chip_sum(0, gsend, gpre, grecv)
    with scope('c2b'):
        wout_copy().wait()
        dy_copy().wait()
        v_rows(slice(cut, rows))
        for i in range(nt):
            t = tile_of(i)
            do_v[t, :] = mm(dy_v[t, :], wout_v[...], NT).astype(BF16)
        for g in range(ngrp):
            dacc[g] = mm(do_v[:, cols(g)], v_v[:, cols(g)], TN)
    with scope('sendd'):
        for h in range(heads):
            dsend[h // 2, h % 2] = pack(dacc, h)
        to_partner(1, dsend, dpre)().start()

    row = lax.broadcasted_iota(jnp.int32, (hd, 2 * hd), 0)
    lanep = lax.broadcasted_iota(jnp.int32, (hd, 2 * hd), 1) - hd * core
    half = (lanep >= 0) & (lanep < hd)
    diag = lanep == row
    half1 = half[0:1]
    even = core == 0

    def unpack(p):
        rolled = pltpu.roll(p, hd, axis=1)
        full = jnp.concatenate([jnp.where(even, p, rolled), jnp.where(even, rolled, p)], axis=0)
        return jnp.where(half, full, 0.0)

    def pack_mine(blk):
        rolled = pltpu.roll(blk, hd, axis=1)
        low, high = jnp.where(even, blk, rolled), jnp.where(even, rolled, blk)
        return jnp.where(lane32 < hd, low[0:hd // 2], high[hd // 2:hd])

    with scope('waitg'):
        tot = image_sum(0, gpre, grecv)
    with scope('soft'):
        gram = unpack(tot[0:hd // 2])
        sq_r = tot[hd // 2:hd // 2 + 1]
        sk_r = jnp.where(half1, tot[hd // 2 + 1:hd // 2 + 2], 1.0)
        sq_c = jnp.sum(jnp.where(diag, sq_r, 0.0), axis=1, keepdims=True)
        den = jnp.sqrt(sq_c) * jnp.sqrt(sk_r)
        cosine = gram / den
        temp_copy().wait()
        temp = temp_ref[me]
        logits = jnp.where(half, temp * cosine, -jnp.inf)
        ex = jnp.exp(logits - jnp.max(logits, axis=1, keepdims=True))
        attn = ex / jnp.sum(ex, axis=1, keepdims=True)
        a_all[me] = pack_mine(attn).astype(BF16)
        to_all(0, a_all)
    with scope('chipd'):
        chip_sum(1, dsend, dpre, drecv)

    def vjp_gram():
        d_a = unpack(image_sum(1, dpre, drecv))
        inner = jnp.sum(d_a * attn, axis=1, keepdims=True)
        d_s = attn * (d_a - inner)
        d_cos = temp * d_s
        e_all[me] = pack_mine(d_cos / den).astype(BF16)
        return d_s, d_cos * cosine

    def vjp_rest(d_s, ec):
        d_t = jnp.sum(jnp.sum(d_s * cosine, axis=1, keepdims=True), axis=0, keepdims=True)
        dsq_c = -0.5 * jnp.sum(ec, axis=1, keepdims=True) / sq_c
        dsk_r = -0.5 * jnp.sum(ec, axis=0, keepdims=True) / sk_r
        st_all[me, 0:1, :] = jnp.sum(jnp.where(diag, dsq_c, 0.0), axis=0, keepdims=True)
        st_all[me, 1:2, :] = dsk_r
        st_all[me, 2:3, :] = jnp.broadcast_to(d_t, (1, 2 * hd))

    def fill(bd, blocks):
        for h in range(heads):
            g, hh = h // hpg, h % hpg
            p = blocks[h].astype(F32)
            rolled = pltpu.roll(p, hd, axis=1)
            mine = (lane32 < hd) if h % 2 == 0 else (lane32 >= hd)
            top, bot = (p, rolled) if h % 2 == 0 else (rolled, p)
            c = slice((hh // 2) * 128, (hh // 2) * 128 + 128)
            bd[g, hh * hd:hh * hd + hd // 2, c] = jnp.where(mine, top, 0.0).astype(BF16)
            bd[g, hh * hd + hd // 2:hh * hd + hd, c] = jnp.where(mine, bot, 0.0).astype(BF16)

    hr = gw.shape[3] // 2
    lo, hi = slice(0, hr), slice(hr, 2 * hr)
    npc = gw.shape[0]

    nhalf = nchip // 2
    half_rows = nhalf * 2 * gw.shape[3]
    near_half = lax.rem(c_o // nhalf + 1, 2)
    far_half = 1 - near_half

    def put(pc, n, lhs, rhs):
        first = (far_half, near_half)[n]
        val = mm(lhs[pl.ds(pl.multiple_of(first * half_rows, half_rows), half_rows), :], rhs)
        c = pl.ds(first * nhalf, nhalf)
        gw[pc, c] = val.reshape(nhalf, *gw.shape[2:])
        remote(gw.at[pc, c, 1 - core], pre.at[pc, c], pre_s.at[0], pre_r.at[pc, n], partner)().start()

    def add_half(pc, n):
        wait_bytes(pre.at[pc, 0:nhalf], pre_r.at[pc, n])
        c = pl.ds((far_half, near_half)[n] * nhalf, nhalf)
        pre[pc, c] = pre[pc, c] + gw[pc, c, core]

    def rs_far(pc):
        with scope('far%d' % pc):
            add_half(pc, 0)
            remote(pre.at[pc, c_o, lo], opp.at[pc, 0], opp_s.at[0], opp_r.at[pc], right)().start()
            remote(pre.at[pc, c_o, hi], opp.at[pc, 1], opp_s.at[0], opp_r.at[pc], left)().start()

    def rs_near(pc):
        with scope('near%d' % pc):
            add_half(pc, 1)
            remote(pre.at[pc, c_r, hi], fin.at[pc, 0], fin_s.at[0], fin_r.at[pc], right)().start()
            remote(pre.at[pc, c_l, lo], fin.at[pc, 1], fin_s.at[0], fin_r.at[pc], left)().start()

    def rs_relay(pc):
        with scope('relay%d' % pc):
            wait_bytes(opp.at[pc], opp_r.at[pc])
            pre[pc, c_r, lo] = pre[pc, c_r, lo] + opp[pc, 0]
            remote(pre.at[pc, c_r, lo], fin.at[pc, 2], fin_s.at[0], fin_r.at[pc], right)().start()
            pre[pc, c_l, hi] = pre[pc, c_l, hi] + opp[pc, 1]
            remote(pre.at[pc, c_l, hi], fin.at[pc, 3], fin_s.at[0], fin_r.at[pc], left)().start()

    def rs_final(pc):
        with scope('final%d' % pc):
            wait_bytes(fin.at[pc], fin_r.at[pc])
            gwst[pc, lo] = pre[pc, chip, lo] + fin[pc, 2] + fin[pc, 1]
            gwst[pc, hi] = pre[pc, chip, hi] + fin[pc, 0] + fin[pc, 3]

    def c3(g):
        with scope('c3'):
            c = pl.ds(pl.multiple_of(g * 256, 256), 256)
            ot_v[c, :] = mm(bd_a[g], vt_v[c, :]).astype(BF16)

    def c4(i):
        t = tile_of(i)
        for g in range(ngrp):
            dqkv_v[t, 2 * width + 256 * g:2 * width + 256 * g + 256] = mm(do_v[t, cols(g)], bd_a[g]).astype(BF16)

    with scope('transpose'):
        for i in range(nt):
            t = tile_of(i)
            ut_v[:, t] = u_v[t, :].T
            vt_v[:, t] = v_v[t, :].T
    with scope('waita'):
        from_all(0, a_all)
    with scope('filla'):
        fill(bd_a, a_all)
    def gw_piece(pc, n, lhs, rhs):
        with scope('gw%d%s' % (pc, 'ab'[n])):
            put(pc, n, lhs, rhs)

    def dcols(c):
        return dqkv_v[:, c * width:(c + 1) * width]

    def c7(i):
        t = tile_of(i)
        out_v[t, :] = (x_v[t, :].astype(F32) + mm(ot_v[:, t], wout_v[...], TN)).astype(BF16)

    c3(far_half)
    with scope('gw0a'):
        vjp_rest(*vjp_gram())
        put(0, 0, ot_v, dy_v[...])
        to_all(1, e_all)
        for dev in peers:
            st = st_all.at[me, 0:3]
            remote(st, st, all_s.at[2], all_r.at[2], dev)().start()
    c3(near_half)
    gw_piece(0, 1, ot_v, dy_v[...])
    rs_far(0)

    with scope('c4'):
        for i in range(nt):
            c4(i)
    gw_piece(1, 0, ut_v, dcols(2))
    rs_near(0)
    gw_piece(1, 1, ut_v, dcols(2))
    with scope('c7a'):
        for i in range(nt // 2):
            c7(i)
    rs_far(1)

    with scope('waite'):
        from_all(1, e_all)
        wait_bytes(st_all.at[0:ns - 1, 0:3], all_r.at[2])
    with scope('fillg'):
        fill(bd_g, e_all)
        pair = [st_all[2 * j, 0:2, :] + st_all[2 * j + 1, 0:2, :] for j in range(heads // 2)]
        dsq2 = jnp.concatenate([2.0 * p[0:1] for p in pair], axis=1)
        dsk2 = jnp.concatenate([2.0 * p[1:2] for p in pair], axis=1)
        lane1 = lax.broadcasted_iota(jnp.int32, (1, 2 * hd), 1)
        gt = jnp.zeros((1, 2 * hd), F32)
        for h in range(heads):
            gt = jnp.where(lane1 == h, st_all[h, 2:3, :], gt)
        gtemp_ref[...] = gt[:, 0:heads]

    def c5(i):
        t = tile_of(i)
        for g in range(ngrp):
            c = cols(g)
            dqkv_v[t, c] = (mm(k_v[t, c], bd_g[g], NT) + q_v[t, c].astype(F32) * dsq2[:, c]).astype(BF16)

    def c6(i):
        t = tile_of(i)
        for g in range(ngrp):
            c = cols(g)
            dqkv_v[t, width + 256 * g:width + 256 * g + 256] = (
                mm(q_v[t, c], bd_g[g]) + k_v[t, c].astype(F32) * dsk2[:, c]).astype(BF16)

    with scope('c5'):
        for i in range(nt):
            c5(i)
    rs_near(1)
    gw_piece(2, 0, ut_v, dcols(0))
    rs_relay(0)
    with scope('c6'):
        for i in range(nt):
            c6(i)
    gw_piece(3, 0, ut_v, dcols(1))
    @pl.when(core == 0)
    def _():
        rs_far(2)

    gw_piece(2, 1, ut_v, dcols(0))

    @pl.when(core == 0)
    def _():
        rs_far(3)

    gw_piece(3, 1, ut_v, dcols(1))

    @pl.when(core == 1)
    def _():
        rs_far(2)
        rs_far(3)

    rs_relay(1)
    rs_near(2)
    def c8(i):
        t = tile_of(i)
        du = mm(dqkv_v[t, :], wqkv_v[...], NT)
        rstd = rstd_v[t, :]
        xhat = (x_v[t, :].astype(F32) - mean_v[t, :]) * rstd
        p = du * xhat
        accumulate(gbacc, 0, jnp.sum(p.reshape(tile // 8, 8, width), axis=0), i == 0)
        accumulate(gbacc, 1, jnp.sum(du.reshape(tile // 8, 8, width), axis=0), i == 0)
        dxh = du * gain_v[...]
        m1 = jnp.mean(dxh, axis=1, keepdims=True)
        m2 = jnp.mean(p * gain_v[...], axis=1, keepdims=True)
        dx = rstd * (dxh - m1 - xhat * m2)
        gtok_v[t, :] = (dy_v[t, :].astype(F32) + dx).astype(BF16)

    with scope('c8a'):
        c8(0)
    rs_near(3)
    with scope('c8b'):
        c8(1)
    with scope('c8c'):
        c8(2)
    rs_relay(2)
    with scope('c8d'):
        c8(3)
        for n in range(2):
            row_sum = jnp.sum(gbacc[n], axis=0, keepdims=True)
            for j in range(width // 128):
                gb_mine[4 * n + j:4 * n + j + 1, :] = row_sum[:, 128 * j:128 * j + 128]
        remote(gb_mine, gb_mate, own_s.at[2, 0], own_r.at[2, 0], partner)().start()
    rs_relay(3)
    with scope('c7b'):
        for i in range(nt // 2, nt):
            c7(i)
    with scope('gbchip'):
        wait_bytes(gb_mate, own_r.at[2, 0])
        gb_all[chip] = gb_mine[...] + gb_mate[...]
        for n in far_first:
            remote(gb_all.at[chip], gb_all.at[chip], own_s.at[2, 1], own_r.at[2, 1], 2 * lax.rem(chip + n, nchip) + core)().start()
    for pc in range(npc):
        rs_final(pc)

    with scope('gb'):
        wait_bytes(gb_all.at[1:nchip], own_r.at[2, 1])
        gb = gb_all[0]
        for d in range(1, nchip):
            gb = gb + gb_all[d]
        for j in range(width // 128):
            ggain_ref[:, 128 * j:128 * j + 128] = gb[j:j + 1]
            gbias_ref[:, 128 * j:128 * j + 128] = gb[4 + j:5 + j]

    with scope('drain'):
        for kind, mid in enumerate((gpre, dpre)):
            wait_bytes(mid, own_s.at[kind, 0])
            wait_bytes(mid.at[1:nchip, 0:mid.shape[1] if kind else hd // 2 + 2], own_s.at[kind, 1])
        wait_bytes(gb_mate, own_s.at[2, 0])
        wait_bytes(gb_all.at[1:nchip], own_s.at[2, 1])
        for kind, buf in enumerate((a_all, e_all)):
            wait_bytes(buf.at[0:ns - 1], all_s.at[kind])
        wait_bytes(st_all.at[0:ns - 1, 0:3], all_s.at[2])
        wait_bytes(pre, pre_s.at[0])
        wait_bytes(opp, opp_s.at[0])
        wait_bytes(fin, fin_s.at[0])


def writer(width, out_v, gtok_v, gwst, gg_v, gb_v, gt_v, out_hbm, gtok_hbm, gwqkv_hbm, gwout_hbm, gg_hbm, gb_hbm, gt_hbm, sem):
    copies = [(gg_v, gg_hbm), (gb_v, gb_hbm), (gt_v, gt_hbm), (gwst.at[0], gwout_hbm)]
    copies += [(gwst.at[pc], gwqkv_hbm.at[:, pl.ds(c * width, width)]) for pc, c in ((1, 2), (2, 0), (3, 1))]
    copies += [(out_v, out_hbm), (gtok_v, gtok_hbm)]
    for i, (src, dst) in enumerate(copies):
        pltpu.make_async_copy(src, dst, sem.at[i]).start()
    for i, (src, dst) in enumerate(copies):
        pltpu.make_async_copy(src, dst, sem.at[i]).wait()


def solution(mesh):
    ns = mesh.shape['sp']
    row_spec = P(('dp', 'sp'), None)
    part_spec = P('dp')

    def local_step(x, dy, gain, bias, w_qkv, w_out, temp):
        rows, width = x.shape
        heads = temp.shape[0]
        hd = width // heads
        tile = 512
        nt = rows // tile
        share = width // ns
        nchip = ns // 2
        ngrp = width // 256
        hbm = pl.BlockSpec(memory_space=pl.ANY)
        vmem = pl.BlockSpec(memory_space=pltpu.VMEM)
        tok = lambda: pltpu.VMEM((rows, width), BF16)
        tok_t = lambda: pltpu.VMEM((width, rows), BF16)
        outs = pl.pallas_call(
            functools.partial(kernel, ns, rows, width, heads, tile),
            out_shape=[pltpu.VMEM((rows, width), BF16), pltpu.VMEM((rows, width), BF16),
                       pltpu.VMEM((4, share, width), F32), pltpu.VMEM((1, width), F32),
                       pltpu.VMEM((1, width), F32), pltpu.VMEM((1, heads), F32)],
            in_specs=[hbm] * 7,
            out_specs=[vmem] * 6,
            scratch_shapes=[
                tok(), tok(), pltpu.VMEM((1, width), F32), pltpu.VMEM((1, width), F32),
                pltpu.VMEM((width, 3 * width), BF16), pltpu.VMEM((width, width), BF16), pltpu.SMEM((heads,), F32),
                tok(), tok(), tok(), tok(), tok(), tok_t(), tok_t(), tok_t(), pltpu.VMEM((rows, 3 * width), BF16),
                pltpu.VMEM((rows, 1), F32), pltpu.VMEM((rows, 1), F32),
                pltpu.VMEM((ngrp, 256, 256), F32), pltpu.VMEM((ngrp, 256, 256), F32),
                pltpu.VMEM((8, width), F32), pltpu.VMEM((8, width), F32),
                pltpu.VMEM((nchip, 2, hd // 2 + 8, 2 * hd), F32), pltpu.VMEM((nchip, hd // 2 + 8, 2 * hd), F32),
                pltpu.VMEM((nchip, hd // 2 + 8, 2 * hd), F32),
                pltpu.VMEM((nchip, 2, hd // 2, 2 * hd), F32), pltpu.VMEM((nchip, hd // 2, 2 * hd), F32),
                pltpu.VMEM((nchip, hd // 2, 2 * hd), F32),
                pltpu.VMEM((heads, hd // 2, 2 * hd), BF16), pltpu.VMEM((heads, hd // 2, 2 * hd), BF16),
                pltpu.VMEM((heads, 8, 2 * hd), F32),
                pltpu.VMEM((ngrp, 256, 256), BF16), pltpu.VMEM((ngrp, 256, 256), BF16),
                pltpu.VMEM((4, nchip, 2, share, width), F32), pltpu.VMEM((4, nchip, share, width), F32),
                pltpu.VMEM((4, 2, share // 2, width), F32), pltpu.VMEM((4, 4, share // 2, width), F32),
                pltpu.VMEM((2, 8, width), F32), pltpu.VMEM((8, 128), F32), pltpu.VMEM((8, 128), F32), pltpu.VMEM((nchip, 8, 128), F32),
                pltpu.SemaphoreType.DMA((nt + 9,)),
                pltpu.SemaphoreType.DMA((3, 2)), pltpu.SemaphoreType.DMA((3, 2)),
                pltpu.SemaphoreType.DMA((3,)), pltpu.SemaphoreType.DMA((3,)),
                pltpu.SemaphoreType.DMA((1,)), pltpu.SemaphoreType.DMA((4, 2)),
                pltpu.SemaphoreType.DMA((1,)), pltpu.SemaphoreType.DMA((4,)),
                pltpu.SemaphoreType.DMA((1,)), pltpu.SemaphoreType.DMA((4,)),
            ],
            compiler_params=pltpu.CompilerParams(collective_id=0, has_side_effects=True,
                                                 vmem_limit_bytes=52 * 1024 * 1024),
        )(x, dy, gain.reshape(1, -1), bias.reshape(1, -1), w_qkv, w_out, temp)
        out, gtok, gwqkv, gwout, ggain, gbias, gtemp = pl.pallas_call(
            functools.partial(writer, width),
            out_shape=[jax.ShapeDtypeStruct((rows, width), BF16),
                       jax.ShapeDtypeStruct((rows, width), BF16),
                       jax.ShapeDtypeStruct((share, 3 * width), F32),
                       jax.ShapeDtypeStruct((share, width), F32),
                       jax.ShapeDtypeStruct((1, width), F32),
                       jax.ShapeDtypeStruct((1, width), F32),
                       jax.ShapeDtypeStruct((1, heads), F32)],
            in_specs=[vmem] * 6,
            out_specs=[hbm] * 7,
            scratch_shapes=[pltpu.SemaphoreType.DMA((9,))],
            compiler_params=pltpu.CompilerParams(vmem_limit_bytes=1024 * 1024),
        )(*outs)
        return out, gtok, gwqkv, gwout, ggain.reshape(-1), gbias.reshape(-1), gtemp.reshape(-1)

    full = P()
    return jax.shard_map(local_step, mesh=mesh,
                         in_specs=(row_spec, row_spec, full, full, full, full, full),
                         out_specs=(row_spec, row_spec, row_spec, row_spec, part_spec, part_spec, part_spec),
                         check_vma=False)
```

```python
import functools

import jax
import jax.numpy as jnp
from jax import lax
from jax.experimental import pallas as pl
from jax.experimental.pallas import tpu as pltpu
from jax.sharding import PartitionSpec as P

F32 = jnp.float32
BF16 = jnp.bfloat16
NN = (((1,), (0,)), ((), ()))
NT = (((1,), (1,)), ((), ()))
TN = (((0,), (0,)), ((), ()))
EPS = 1e-6


def mm(a, b, dims=NN):
    return lax.dot_general(a, b, dims, preferred_element_type=F32)


def kernel(ns, rows, width, heads, tile,
           x_hbm, dy_hbm, gain_hbm, bias_hbm, wqkv_hbm, wout_hbm, temp_hbm,
           out_v, gtok_v, gwst, ggain_ref, gbias_ref, gtemp_ref,
           x_v, dy_v, gain_v, bias_v, wqkv_v, wout_v, temp_ref,
           u_v, q_v, k_v, v_v, do_v, ut_v, vt_v, ot_v, dqkv_v, mean_v, rstd_v,
           gacc, dacc, sqacc, skacc, gsend, gpre, grecv, dsend, dpre, drecv, a_all, e_all, st_all, bd_a, bd_g,
           gw, pre, opp, fin, gbacc, gb_mine, gb_mate, gb_all,
           in_sem, own_s, own_r, all_s, all_r, pre_s, pre_r, opp_s, opp_r, fin_s, fin_r):
    me = lax.axis_index('sp')
    nt = rows // tile
    hd = width // heads
    keep = True
    hf, wide, w2, w3 = hd // 2, 2 * hd, 2 * width, 3 * width
    core = lax.rem(me, 2)
    chip = me // 2
    nchip = ns // 2
    partner = me + 1 - 2 * core
    right = lax.rem(me + 2, ns)
    left = lax.rem(me + ns - 2, ns)
    c_r = lax.rem(chip + 1, nchip)
    c_l = lax.rem(chip + nchip - 1, nchip)
    c_o = lax.rem(chip + 2, nchip)
    scope = jax.named_scope

    def remote(src, dst, ssem, rsem, dev):
        return lambda: pltpu.make_async_remote_copy(src_ref=src, dst_ref=dst, send_sem=ssem, recv_sem=rsem,
                                                    device_id={'sp': dev}, device_id_type=pl.DeviceIdType.MESH)

    def wait_bytes(ref, sem):
        pltpu.make_async_copy(ref, ref, sem).wait()

    far_first = sorted(range(1, nchip), key=lambda s: -min(s, nchip - s))
    peers = [2 * lax.rem(chip + s, nchip) + c for s in far_first for c in (1, 0)] + [partner]

    barrier = pltpu.get_barrier_semaphore()
    def ld(i, src, dst):
        return lambda: pltpu.make_async_copy(src, dst, in_sem.at[i])

    def tile_of(i):
        return slice(i * tile, (i + 1) * tile)

    def x_copy(i):
        return ld(i, x_hbm.at[tile_of(i)], x_v.at[tile_of(i)])

    dy_copy = ld(nt, dy_hbm, dy_v)
    gain_copy = ld(nt + 1, gain_hbm, gain_v)
    bias_copy = ld(nt + 2, bias_hbm, bias_v)
    wq_copy = ld(nt + 3, wqkv_hbm.at[:, 0:width], wqkv_v.at[:, 0:width])
    wk_copy = ld(nt + 7, wqkv_hbm.at[:, width:w2], wqkv_v.at[:, width:w2])
    wv_copy = ld(nt + 4, wqkv_hbm.at[:, w2:w3], wqkv_v.at[:, w2:w3])
    wout_copy = ld(nt + 5, wout_hbm, wout_v)
    temp_copy = ld(nt + 6, temp_hbm, temp_ref)
    head = slice(0, tile // 2)
    rest = slice(tile // 2, tile)
    x_head = ld(0, x_hbm.at[head], x_v.at[head])
    x_rest = ld(nt + 8, x_hbm.at[rest], x_v.at[rest])
    x_head().start()
    gain_copy().start()
    bias_copy().start()
    wq_copy().start()
    x_rest().start()
    wk_copy().start()
    x_copy(1)().start()
    for dev in peers:
        pl.semaphore_signal(barrier, inc=1, device_id={'sp': dev}, device_id_type=pl.DeviceIdType.MESH)

    with scope('init'):
        bd_a[...] = jnp.zeros_like(bd_a)
        bd_g[...] = jnp.zeros_like(bd_g)

    ngrp = width // 256
    hpg = heads // ngrp

    def cols(g):
        return slice(256 * g, 256 * g + 256)

    def ln(t):
        x = x_v[t, :].astype(F32)
        mean = jnp.mean(x, axis=1, keepdims=keep)
        cent = x - mean
        var = jnp.mean(cent * cent, axis=1, keepdims=keep)
        rstd = lax.rsqrt(var + EPS)
        mean_v[t, :] = mean
        rstd_v[t, :] = rstd
        u_v[t, :] = (cent * rstd * gain_v[...] + bias_v[...]).astype(BF16)

    def accumulate(ref, idx, val, first):
        if first:
            ref[idx] = val
        else:
            ref[idx] += val

    def square_sum(ref, c, val, first):
        v32 = val.astype(F32)
        part = jnp.sum((v32 * v32).reshape(tile // 8, 8, 256), axis=0)
        ref[:, c] = part if first else ref[:, c] + part

    with scope('wx0'):
        x_head().wait()
        for i in range(2, nt):
            x_copy(i)().start()
        gain_copy().wait()
        bias_copy().wait()
    with scope('ln0'):
        ln(head)
    with scope('ww'):
        wq_copy().wait()
        x_rest().wait()
    with scope('c1h'):
        ln(rest)
        q_v[head, :] = mm(u_v[head, :], wqkv_v[:, 0:width]).astype(BF16)
    with scope('ww2'):
        wk_copy().wait()
        x_copy(1)().wait()
        wv_copy().start()
        wout_copy().start()
        dy_copy().start()
        temp_copy().start()
    with scope('c1'):
        for i in range(nt):
            t = tile_of(i)
            if i == 1:
                for j in range(2, nt):
                    x_copy(j)().wait()
            if i + 1 < nt:
                ln(tile_of(i + 1))
            if i == 0:
                q_v[rest, :] = mm(u_v[rest, :], wqkv_v[:, 0:width]).astype(BF16)
                q = q_v[t, :]
            else:
                q = mm(u_v[t, :], wqkv_v[:, 0:width]).astype(BF16)
                q_v[t, :] = q
            k = mm(u_v[t, :], wqkv_v[:, width:w2]).astype(BF16)
            k_v[t, :] = k
            for g in range(ngrp):
                c = cols(g)
                square_sum(sqacc, c, q[:, c], i == 0)
                square_sum(skacc, c, k[:, c], i == 0)
                if i == nt - 2:
                    done = slice(0, (nt - 1) * tile)
                    gacc[g] = mm(q_v[done, c], k_v[done, c], TN)
                elif i == nt - 1:
                    gacc[g] += mm(q[:, c], k[:, c], TN)

    lane32 = lax.broadcasted_iota(jnp.int32, (hf, wide), 1)

    def pack_block(blk, odd):
        top, bot = blk[0:hf], blk[hf:hd]
        if odd:
            top = pltpu.roll(top, hd, axis=1)
        else:
            bot = pltpu.roll(bot, hd, axis=1)
        return jnp.where(lane32 < hd, top, bot)

    def pack(acc, h):
        g, hh = h // hpg, h % hpg
        return pack_block(acc[g, hh * hd:hh * hd + hd, (hh // 2) * 128:(hh // 2) * 128 + 128], h % 2 == 1)

    with scope('packg'):
        sq_row = jnp.sum(sqacc[...], axis=0, keepdims=keep)
        sk_row = jnp.sum(skacc[...], axis=0, keepdims=keep)
        for h in range(heads):
            gsend[h // 2, h % 2, 0:hf, :] = pack(gacc, h)
            c = slice((h // 2) * 128, (h // 2) * 128 + 128)
            gsend[h // 2, h % 2, hf:hf + 1, :] = sq_row[:, c]
            gsend[h // 2, h % 2, hf + 1:hf + 2, :] = sk_row[:, c]

    def to_partner(kind, src, dst):
        return remote(src.at[:, 1 - core], dst, own_s.at[kind, 0], own_r.at[kind, 0], partner)

    def chip_sum(kind, src, mid, dst):
        wait_bytes(mid, own_r.at[kind, 0])
        n = mid.shape[1] if kind else hf + 2
        for c in range(nchip):
            mid[c, 0:n] = mid[c, 0:n] + src[c, core, 0:n]
        for s in far_first:
            c = lax.rem(chip + s, nchip)
            remote(mid.at[c, 0:n], dst.at[s, 0:n], own_s.at[kind, 1], own_r.at[kind, 1], 2 * c + core)().start()

    def image_sum(kind, mid, dst):
        n = mid.shape[1] if kind else hf + 2
        wait_bytes(dst.at[1:nchip, 0:n], own_r.at[kind, 1])
        tot = mid[chip, 0:n]
        for s in range(1, nchip):
            tot = tot + dst[s, 0:n]
        return tot

    def to_all(kind, buf):
        for dev in peers:
            remote(buf.at[me], buf.at[me], all_s.at[kind], all_r.at[kind], dev)().start()

    def from_all(kind, buf):
        wait_bytes(buf.at[0:ns - 1], all_r.at[kind])

    with scope('sendg'):
        pl.semaphore_wait(barrier, ns - 1)
        to_partner(0, gsend, gpre)().start()

    def v_rows(t):
        v_v[t, :] = mm(u_v[t, :], wqkv_v[:, w2:w3]).astype(BF16)

    cut = rows // 2
    with scope('c2a'):
        wv_copy().wait()
        v_rows(slice(0, cut))
    with scope('chipg'):
        chip_sum(0, gsend, gpre, grecv)
    with scope('c2b'):
        wout_copy().wait()
        dy_copy().wait()
        v_rows(slice(cut, rows))
        for i in range(nt):
            t = tile_of(i)
            do_v[t, :] = mm(dy_v[t, :], wout_v[...], NT).astype(BF16)
        for g in range(ngrp):
            dacc[g] = mm(do_v[:, cols(g)], v_v[:, cols(g)], TN)
    with scope('sendd'):
        for h in range(heads):
            dsend[h // 2, h % 2] = pack(dacc, h)
        to_partner(1, dsend, dpre)().start()

    row = lax.broadcasted_iota(jnp.int32, (hd, wide), 0)
    lanep = lax.broadcasted_iota(jnp.int32, (hd, wide), 1) - hd * core
    half = (lanep >= 0) & (lanep < hd)
    diag = lanep == row
    half1 = half[0:1]
    even = core == 0

    def unpack(p):
        rolled = pltpu.roll(p, hd, axis=1)
        full = jnp.concatenate([jnp.where(even, p, rolled), jnp.where(even, rolled, p)], axis=0)
        return jnp.where(half, full, 0.0)

    def pack_mine(blk):
        rolled = pltpu.roll(blk, hd, axis=1)
        low, high = jnp.where(even, blk, rolled), jnp.where(even, rolled, blk)
        return jnp.where(lane32 < hd, low[0:hf], high[hf:hd])

    with scope('waitg'):
        tot = image_sum(0, gpre, grecv)
    with scope('soft'):
        gram = unpack(tot[0:hf])
        sq_r = tot[hf:hf + 1]
        sk_r = jnp.where(half1, tot[hf + 1:hf + 2], 1.0)
        sq_c = jnp.sum(jnp.where(diag, sq_r, 0.0), axis=1, keepdims=keep)
        den = jnp.sqrt(sq_c) * jnp.sqrt(sk_r)
        cosine = gram / den
        temp_copy().wait()
        temp = temp_ref[me]
        logits = jnp.where(half, temp * cosine, -jnp.inf)
        ex = jnp.exp(logits - jnp.max(logits, axis=1, keepdims=keep))
        attn = ex / jnp.sum(ex, axis=1, keepdims=keep)
        a_all[me] = pack_mine(attn).astype(BF16)
        to_all(0, a_all)
    with scope('chipd'):
        chip_sum(1, dsend, dpre, drecv)

    def vjp_gram():
        d_a = unpack(image_sum(1, dpre, drecv))
        inner = jnp.sum(d_a * attn, axis=1, keepdims=keep)
        d_s = attn * (d_a - inner)
        d_cos = temp * d_s
        e_all[me] = pack_mine(d_cos / den).astype(BF16)
        return d_s, d_cos * cosine

    def vjp_rest(d_s, ec):
        d_t = jnp.sum(jnp.sum(d_s * cosine, axis=1, keepdims=keep), axis=0, keepdims=keep)
        dsq_c = -0.5 * jnp.sum(ec, axis=1, keepdims=keep) / sq_c
        dsk_r = -0.5 * jnp.sum(ec, axis=0, keepdims=keep) / sk_r
        st_all[me, 0:1, :] = jnp.sum(jnp.where(diag, dsq_c, 0.0), axis=0, keepdims=keep)
        st_all[me, 1:2, :] = dsk_r
        st_all[me, 2:3, :] = jnp.broadcast_to(d_t, (1, wide))

    def fill(bd, blocks):
        for h in range(heads):
            g, hh = h // hpg, h % hpg
            p = blocks[h].astype(F32)
            rolled = pltpu.roll(p, hd, axis=1)
            mine = (lane32 < hd) if h % 2 == 0 else (lane32 >= hd)
            top, bot = (p, rolled) if h % 2 == 0 else (rolled, p)
            c = slice((hh // 2) * 128, (hh // 2) * 128 + 128)
            bd[g, hh * hd:hh * hd + hf, c] = jnp.where(mine, top, 0.0).astype(BF16)
            bd[g, hh * hd + hf:hh * hd + hd, c] = jnp.where(mine, bot, 0.0).astype(BF16)

    hr = gw.shape[3] // 2
    lo, hi = slice(0, hr), slice(hr, 2 * hr)
    npc = gw.shape[0]

    nhalf = nchip // 2
    half_rows = nhalf * 2 * gw.shape[3]
    near_half = lax.rem(c_o // nhalf + 1, 2)
    far_half = 1 - near_half

    def put(pc, n, lhs, rhs):
        first = (far_half, near_half)[n]
        val = mm(lhs[pl.ds(pl.multiple_of(first * half_rows, half_rows), half_rows), :], rhs)
        c = pl.ds(first * nhalf, nhalf)
        gw[pc, c] = val.reshape(nhalf, *gw.shape[2:])
        remote(gw.at[pc, c, 1 - core], pre.at[pc, c], pre_s, pre_r.at[pc, n], partner)().start()

    def add_half(pc, n):
        wait_bytes(pre.at[pc, 0:nhalf], pre_r.at[pc, n])
        c = pl.ds((far_half, near_half)[n] * nhalf, nhalf)
        pre[pc, c] = pre[pc, c] + gw[pc, c, core]

    def rs_far(pc):
        with scope('far%d' % pc):
            add_half(pc, 0)
            remote(pre.at[pc, c_o, lo], opp.at[pc, 0], opp_s, opp_r.at[pc], right)().start()
            remote(pre.at[pc, c_o, hi], opp.at[pc, 1], opp_s, opp_r.at[pc], left)().start()

    def rs_near(pc):
        with scope('near%d' % pc):
            add_half(pc, 1)
            remote(pre.at[pc, c_r, hi], fin.at[pc, 0], fin_s, fin_r.at[pc], right)().start()
            remote(pre.at[pc, c_l, lo], fin.at[pc, 1], fin_s, fin_r.at[pc], left)().start()

    def rs_relay(pc):
        with scope('relay%d' % pc):
            wait_bytes(opp.at[pc], opp_r.at[pc])
            pre[pc, c_r, lo] = pre[pc, c_r, lo] + opp[pc, 0]
            remote(pre.at[pc, c_r, lo], fin.at[pc, 2], fin_s, fin_r.at[pc], right)().start()
            pre[pc, c_l, hi] = pre[pc, c_l, hi] + opp[pc, 1]
            remote(pre.at[pc, c_l, hi], fin.at[pc, 3], fin_s, fin_r.at[pc], left)().start()

    def rs_final(pc):
        with scope('final%d' % pc):
            wait_bytes(fin.at[pc], fin_r.at[pc])
            gwst[pc, lo] = pre[pc, chip, lo] + fin[pc, 2] + fin[pc, 1]
            gwst[pc, hi] = pre[pc, chip, hi] + fin[pc, 0] + fin[pc, 3]

    def c3(g):
        with scope('c3'):
            c = pl.ds(pl.multiple_of(g * 256, 256), 256)
            ot_v[c, :] = mm(bd_a[g], vt_v[c, :]).astype(BF16)

    def c4(i):
        t = tile_of(i)
        for g in range(ngrp):
            dqkv_v[t, w2 + 256 * g:w2 + 256 * g + 256] = mm(do_v[t, cols(g)], bd_a[g]).astype(BF16)

    with scope('transpose'):
        for i in range(nt):
            t = tile_of(i)
            ut_v[:, t] = u_v[t, :].T
            vt_v[:, t] = v_v[t, :].T
    with scope('waita'):
        from_all(0, a_all)
    with scope('filla'):
        fill(bd_a, a_all)
    def gw_piece(pc, n, lhs, rhs):
        with scope('gw%d%s' % (pc, 'ab'[n])):
            put(pc, n, lhs, rhs)

    def dcols(c):
        return dqkv_v[:, c * width:(c + 1) * width]

    def c7(i):
        t = tile_of(i)
        out_v[t, :] = (x_v[t, :].astype(F32) + mm(ot_v[:, t], wout_v[...], TN)).astype(BF16)

    c3(far_half)
    with scope('gw0a'):
        vjp_rest(*vjp_gram())
        put(0, 0, ot_v, dy_v[...])
        to_all(1, e_all)
        for dev in peers:
            st = st_all.at[me, 0:3]
            remote(st, st, all_s.at[2], all_r.at[2], dev)().start()
    c3(near_half)
    gw_piece(0, 1, ot_v, dy_v[...])
    rs_far(0)

    with scope('c4'):
        for i in range(nt):
            c4(i)
    gw_piece(1, 0, ut_v, dcols(2))
    rs_near(0)
    gw_piece(1, 1, ut_v, dcols(2))
    with scope('c7a'):
        for i in range(nt // 2):
            c7(i)
    rs_far(1)

    with scope('waite'):
        from_all(1, e_all)
        wait_bytes(st_all.at[0:ns - 1, 0:3], all_r.at[2])
    with scope('fillg'):
        fill(bd_g, e_all)
        pair = [st_all[2 * j, 0:2, :] + st_all[2 * j + 1, 0:2, :] for j in range(heads // 2)]
        dsq2 = jnp.concatenate([2.0 * p[0:1] for p in pair], axis=1)
        dsk2 = jnp.concatenate([2.0 * p[1:2] for p in pair], axis=1)
        lane1 = lax.broadcasted_iota(jnp.int32, (1, wide), 1)
        gt = jnp.zeros((1, wide), F32)
        for h in range(heads):
            gt = jnp.where(lane1 == h, st_all[h, 2:3, :], gt)
        gtemp_ref[...] = gt[:, 0:heads]

    def c5(i):
        t = tile_of(i)
        for g in range(ngrp):
            c = cols(g)
            dqkv_v[t, c] = (mm(k_v[t, c], bd_g[g], NT) + q_v[t, c].astype(F32) * dsq2[:, c]).astype(BF16)

    def c6(i):
        t = tile_of(i)
        for g in range(ngrp):
            c = cols(g)
            dqkv_v[t, width + 256 * g:width + 256 * g + 256] = (
                mm(q_v[t, c], bd_g[g]) + k_v[t, c].astype(F32) * dsk2[:, c]).astype(BF16)

    with scope('c5'):
        for i in range(nt):
            c5(i)
    rs_near(1)
    gw_piece(2, 0, ut_v, dcols(0))
    rs_relay(0)
    with scope('c6'):
        for i in range(nt):
            c6(i)
    gw_piece(3, 0, ut_v, dcols(1))
    @pl.when(core == 0)
    def _():
        rs_far(2)

    gw_piece(2, 1, ut_v, dcols(0))

    @pl.when(core == 0)
    def _():
        rs_far(3)

    gw_piece(3, 1, ut_v, dcols(1))

    @pl.when(core == 1)
    def _():
        rs_far(2)
        rs_far(3)

    rs_relay(1)
    rs_near(2)
    def c8(i):
        t = tile_of(i)
        du = mm(dqkv_v[t, :], wqkv_v[...], NT)
        rstd = rstd_v[t, :]
        xhat = (x_v[t, :].astype(F32) - mean_v[t, :]) * rstd
        p = du * xhat
        accumulate(gbacc, 0, jnp.sum(p.reshape(tile // 8, 8, width), axis=0), i == 0)
        accumulate(gbacc, 1, jnp.sum(du.reshape(tile // 8, 8, width), axis=0), i == 0)
        dxh = du * gain_v[...]
        m1 = jnp.mean(dxh, axis=1, keepdims=keep)
        m2 = jnp.mean(p * gain_v[...], axis=1, keepdims=keep)
        dx = rstd * (dxh - m1 - xhat * m2)
        gtok_v[t, :] = (dy_v[t, :].astype(F32) + dx).astype(BF16)

    with scope('c8a'):
        c8(0)
    rs_near(3)
    with scope('c8b'):
        c8(1)
    with scope('c8c'):
        c8(2)
    rs_relay(2)
    with scope('c8d'):
        c8(3)
        for n in range(2):
            row_sum = jnp.sum(gbacc[n], axis=0, keepdims=keep)
            for j in range(width // 128):
                gb_mine[4 * n + j:4 * n + j + 1, :] = row_sum[:, 128 * j:128 * j + 128]
        remote(gb_mine, gb_mate, own_s.at[2, 0], own_r.at[2, 0], partner)().start()
    rs_relay(3)
    with scope('c7b'):
        for i in range(nt // 2, nt):
            c7(i)
    with scope('gbchip'):
        wait_bytes(gb_mate, own_r.at[2, 0])
        gb_all[chip] = gb_mine[...] + gb_mate[...]
        for n in far_first:
            remote(gb_all.at[chip], gb_all.at[chip], own_s.at[2, 1], own_r.at[2, 1], 2 * lax.rem(chip + n, nchip) + core)().start()
    for pc in range(npc):
        rs_final(pc)

    with scope('gb'):
        wait_bytes(gb_all.at[1:nchip], own_r.at[2, 1])
        gb = gb_all[0]
        for d in range(1, nchip):
            gb = gb + gb_all[d]
        for j in range(width // 128):
            ggain_ref[:, 128 * j:128 * j + 128] = gb[j:j + 1]
            gbias_ref[:, 128 * j:128 * j + 128] = gb[4 + j:5 + j]

    with scope('drain'):
        for kind, mid in enumerate((gpre, dpre)):
            wait_bytes(mid, own_s.at[kind, 0])
            wait_bytes(mid.at[1:nchip, 0:mid.shape[1] if kind else hf + 2], own_s.at[kind, 1])
        wait_bytes(gb_mate, own_s.at[2, 0])
        wait_bytes(gb_all.at[1:nchip], own_s.at[2, 1])
        for kind, buf in enumerate((a_all, e_all)):
            wait_bytes(buf.at[0:ns - 1], all_s.at[kind])
        wait_bytes(st_all.at[0:ns - 1, 0:3], all_s.at[2])
        wait_bytes(pre, pre_s)
        wait_bytes(opp, opp_s)
        wait_bytes(fin, fin_s)


def writer(width, out_v, gtok_v, gwst, gg_v, gb_v, gt_v, out_hbm, gtok_hbm, gwqkv_hbm, gwout_hbm, gg_hbm, gb_hbm, gt_hbm, sem):
    copies = [(gg_v, gg_hbm), (gb_v, gb_hbm), (gt_v, gt_hbm), (gwst.at[0], gwout_hbm)]
    copies += [(gwst.at[pc], gwqkv_hbm.at[:, pl.ds(c * width, width)]) for pc, c in ((1, 2), (2, 0), (3, 1))]
    copies += [(out_v, out_hbm), (gtok_v, gtok_hbm)]
    for i, (src, dst) in enumerate(copies):
        pltpu.make_async_copy(src, dst, sem.at[i]).start()
    for i, (src, dst) in enumerate(copies):
        pltpu.make_async_copy(src, dst, sem.at[i]).wait()


def solution(mesh):
    ns = mesh.shape['sp']
    row_spec = P(('dp', 'sp'), None)
    part_spec = P('dp')

    def local_step(x, dy, gain, bias, w_qkv, w_out, temp):
        rows, width = x.shape
        heads = temp.shape[0]
        hd = width // heads
        tile = 512
        nt = rows // tile
        share = width // ns
        nchip = ns // 2
        ngrp = width // 256
        hf, wide = hd // 2, 2 * hd
        f32 = lambda *shape: pltpu.VMEM(shape, F32)
        b16 = lambda *shape: pltpu.VMEM(shape, BF16)
        sems = lambda *shape: pltpu.SemaphoreType.DMA(shape)
        hbm = pl.BlockSpec(memory_space=pl.ANY)
        vmem = pl.BlockSpec(memory_space=pltpu.VMEM)
        tok = lambda: pltpu.VMEM((rows, width), BF16)
        tok_t = lambda: pltpu.VMEM((width, rows), BF16)
        outs = pl.pallas_call(
            functools.partial(kernel, ns, rows, width, heads, tile),
            out_shape=[pltpu.VMEM((rows, width), BF16), pltpu.VMEM((rows, width), BF16),
                       pltpu.VMEM((4, share, width), F32), pltpu.VMEM((1, width), F32),
                       pltpu.VMEM((1, width), F32), pltpu.VMEM((1, heads), F32)],
            in_specs=[hbm] * 7,
            out_specs=[vmem] * 6,
            scratch_shapes=[
                tok(), tok(), f32(1, width), f32(1, width), b16(width, 3 * width), b16(width, width), pltpu.SMEM((heads,), F32),
                tok(), tok(), tok(), tok(), tok(), tok_t(), tok_t(), tok_t(), b16(rows, 3 * width), f32(rows, 1), f32(rows, 1),
                f32(ngrp, 256, 256), f32(ngrp, 256, 256), f32(8, width), f32(8, width),
                f32(nchip, 2, hf + 8, wide), f32(nchip, hf + 8, wide), f32(nchip, hf + 8, wide),
                f32(nchip, 2, hf, wide), f32(nchip, hf, wide), f32(nchip, hf, wide),
                b16(heads, hf, wide), b16(heads, hf, wide), f32(heads, 8, wide),
                b16(ngrp, 256, 256), b16(ngrp, 256, 256),
                f32(4, nchip, 2, share, width), f32(4, nchip, share, width),
                f32(4, 2, share // 2, width), f32(4, 4, share // 2, width),
                f32(2, 8, width), f32(8, 128), f32(8, 128), f32(nchip, 8, 128),
                sems(nt + 9), sems(3, 2), sems(3, 2), sems(3), sems(3), sems(), sems(4, 2), sems(), sems(4), sems(), sems(4),
            ],
            compiler_params=pltpu.CompilerParams(collective_id=0, has_side_effects=True,
                                                 vmem_limit_bytes=52 * 1024 * 1024),
        )(x, dy, gain.reshape(1, -1), bias.reshape(1, -1), w_qkv, w_out, temp)
        out, gtok, gwqkv, gwout, ggain, gbias, gtemp = pl.pallas_call(
            functools.partial(writer, width),
            out_shape=[jax.ShapeDtypeStruct((rows, width), BF16),
                       jax.ShapeDtypeStruct((rows, width), BF16),
                       jax.ShapeDtypeStruct((share, 3 * width), F32),
                       jax.ShapeDtypeStruct((share, width), F32),
                       jax.ShapeDtypeStruct((1, width), F32),
                       jax.ShapeDtypeStruct((1, width), F32),
                       jax.ShapeDtypeStruct((1, heads), F32)],
            in_specs=[vmem] * 6,
            out_specs=[hbm] * 7,
            scratch_shapes=[pltpu.SemaphoreType.DMA((9,))],
            compiler_params=pltpu.CompilerParams(vmem_limit_bytes=1024 * 1024),
        )(*outs)
        return out, gtok, gwqkv, gwout, ggain.reshape(-1), gbias.reshape(-1), gtemp.reshape(-1)

    full = P()
    return jax.shard_map(local_step, mesh=mesh,
                         in_specs=(row_spec, row_spec, full, full, full, full, full),
                         out_specs=(row_spec, row_spec, row_spec, row_spec, part_spec, part_spec, part_spec),
                         check_vma=False)
```
